32 devices in a mesh: ctx: 8 (over z, y), fsdp: 4 (over x, core).
Axes of the slice: x: 2, y: 2, z: 4, core: 2. Of those that a mesh axis runs over, the one named last changes fastest.
Arguments:
- tokens: bfloat16 [4, 1024, 1600], P('fsdp', 'ctx'), may hold values from -6 to 6
- block_order: int32 [4, 16], P('fsdp'), may hold values from 0 to 15, each once within a row
- qkv_weight: bfloat16 [1600, 4800], P('fsdp'), may hold values from -0.15625 to 0.15625
- query_bias: float32 [1600], replicated, may hold values from -3 to 3
- value_bias: float32 [1600], replicated, may hold values from -0.18 to 0.18
- out_weight: bfloat16 [1600, 1600], P('fsdp'), may hold values from -2.5 to 2.5
- out_bias: float32 [1600], replicated, may hold values from -1.8 to 1.8
- expand_weight: bfloat16 [1600, 6400], P('fsdp'), may hold values from -0.15625 to 0.15625
- expand_bias: float32 [6400], replicated, may hold values from -3 to 3
- shrink_weight: bfloat16 [6400, 1600], P('fsdp'), may hold values from -0.078125 to 0.078125
- shrink_bias: float32 [1600], replicated, may hold values from -1.8 to 1.8
- first_gain: float32 [1600], replicated, may hold values from 0.5 to 1.5
- first_shift: float32 [1600], replicated, may hold values from -1.8 to 1.8
- second_gain: float32 [1600], replicated, may hold values from 0.5 to 1.5
- second_shift: float32 [1600], replicated, may hold values from -1.8 to 1.8
- cotangent: bfloat16 [4, 1024, 1600], P('fsdp', 'ctx'), may hold values from -6 to 6
Outputs:
- result: bfloat16 [4, 1024, 1600], P('fsdp', 'ctx')
- grad_tokens: float32 [4, 1024, 1600], P('fsdp', 'ctx')
- grad_qkv: float32 [1600, 4800], P('fsdp', 'ctx')
- grad_outw: float32 [1600, 1600], P('fsdp', 'ctx')
- grad_expand: float32 [1600, 6400], P('fsdp', 'ctx')
- grad_shrink: float32 [6400, 1600], P('fsdp', 'ctx')
- grad_query_bias: float32 [1600], replicated
- grad_value_bias: float32 [1600], replicated
- grad_out_bias: float32 [1600], replicated
- grad_expand_bias: float32 [6400], replicated
- grad_shrink_bias: float32 [1600], replicated
- grad_first_gain: float32 [1600], replicated
- grad_first_shift: float32 [1600], replicated
- grad_second_gain: float32 [1600], replicated
- grad_second_shift: float32 [1600], replicated
The draws below stay inside these ranges and needn't reach their ends.
Inputs may be any that keep to these rules, and one draw needn't show every extreme that they name: Each row of block_order names every block of its sequence once.
All inputs are finite; a program needn't handle non-finite values.
Results may differ from the reference program's by a relative error of at most 0.015.
Values may be sent and summed in bfloat16 or wider, within the bound.
A program may use at most 384 MiB of HBM per device.

```python
import jax
import jax.numpy as jnp
from jax import lax

D = 1600
HEADS = 25
HEAD_DIM = 64
FF = 6400
SEQS = 4
LEN = 1024
N_CTX = 8


def block_scale(key, dims, cuts, least, high):
    factor_of = 1.0
    for dim, parts in cuts:
        steps = jax.random.uniform(jax.random.fold_in(jax.random.fold_in(key, 6), dim), (parts,), jnp.float32, least / len(cuts), high / len(cuts))
        factor_of = factor_of * jnp.repeat(jnp.exp(steps), dims[dim] // parts).reshape((-1,) + (1,) * (len(dims) - 1 - dim))
    return factor_of


def normal_values(stream_key, extent, deviation, reach, pieces=(), kind=jnp.bfloat16):
    level = block_scale(stream_key, extent, pieces, -0.22, 0.18) if pieces else 1.0
    values = jax.random.normal(stream_key, extent, jnp.float32) * deviation * level
    return jnp.minimum(jnp.maximum(values, -reach), reach).astype(kind)


def setup_inputs(seed: int = 0) -> dict:
    seeds = jax.random.split(jax.random.key(seed), 17)
    tokens = normal_values(seeds[0], (SEQS, LEN, D), 1.0, 6.0, ((0, 4), (1, 8)))
    block_order = jax.vmap(lambda own: jax.random.permutation(own, 2 * N_CTX))(jax.random.split(seeds[1], SEQS)).reshape((SEQS, 2 * N_CTX)).astype(jnp.int32)
    qkv_weight = normal_values(seeds[2], (D, 3 * D), D ** -0.5, 0.15625, ((0, 4),))
    query_bias = normal_values(seeds[3], (D,), 0.5, 3.0, (), jnp.float32)
    value_bias = normal_values(seeds[4], (D,), 0.03, 0.18, (), jnp.float32)
    out_weight = normal_values(seeds[5], (D, D), (max(1, D // 256)) ** -0.5, 2.5, ((0, 4),))
    out_bias = normal_values(seeds[6], (D,), 0.3, 1.8, (), jnp.float32)
    expand_weight = normal_values(seeds[7], (D, FF), D ** -0.5, 0.15625, ((0, 4),))
    expand_bias = normal_values(seeds[8], (FF,), 0.5, 3.0, (), jnp.float32)
    shrink_weight = normal_values(seeds[9], (FF, D), FF ** -0.5, 0.078125, ((0, 4),))
    shrink_bias = normal_values(seeds[10], (D,), 0.3, 1.8, (), jnp.float32)
    first_gain = jnp.clip(1.0 + 0.1 * jax.random.normal(seeds[11], (D,), jnp.float32), 0.5, 1.5)
    first_shift = normal_values(seeds[12], (D,), 0.3, 1.8, (), jnp.float32)
    second_gain = jnp.clip(1.0 + 0.1 * jax.random.normal(seeds[13], (D,), jnp.float32), 0.5, 1.5)
    second_shift = normal_values(seeds[14], (D,), 0.3, 1.8, (), jnp.float32)
    cotangent = normal_values(seeds[15], (SEQS, LEN, D), 1.0, 6.0, ((0, 4), (1, 8)))
    return {"tokens": tokens, "block_order": block_order, "qkv_weight": qkv_weight, "query_bias": query_bias, "value_bias": value_bias, "out_weight": out_weight, "out_bias": out_bias, "expand_weight": expand_weight, "expand_bias": expand_bias, "shrink_weight": shrink_weight, "shrink_bias": shrink_bias, "first_gain": first_gain, "first_shift": first_shift, "second_gain": second_gain, "second_shift": second_shift, "cotangent": cotangent}


@jax.custom_vjp
def low(v):
    return lax.optimization_barrier(v.astype(jnp.bfloat16)).astype(jnp.float32)

@jax.custom_vjp
def low_back(v):
    return v

def low_keep(v):
    return (low(v), None)

def low_pass(kept, grad):
    return (grad,)

def back_keep(v):
    return (v, None)

def back_low(kept, grad):
    return (low(grad),)
low.defvjp(low_keep, low_pass)
low_back.defvjp(back_keep, back_low)
HIGH = lax.Precision.HIGHEST
EPSILON = 1e-05

def layer_norm(values, gain, shift):
    center = lax.optimization_barrier(jnp.mean(values, axis=-1, keepdims=True))
    centred = values - center
    spread = lax.optimization_barrier(jnp.mean(centred * centred, axis=-1, keepdims=True))
    return centred * lax.rsqrt(spread + EPSILON) * gain + shift

def smooth_gelu(values):
    return 0.5 * values * (1.0 + jnp.tanh(0.7978845608028654 * (values + 0.044715 * values * values * values)))

def sequence(params, inputs, order):
    qkv_full, query_bias, value_bias, out_full, out_bias, expand_full, expand_bias, shrink_full, shrink_bias, first_gain, first_shift, second_gain, second_shift = params
    length = inputs.shape[0]
    width = inputs.shape[1]
    half = length // (2 * N_CTX)
    positions = (order[:, None] * half + jnp.arange(half, dtype=jnp.int32)[None, :]).reshape(-1)
    normed_one = low(layer_norm(inputs, first_gain, first_shift))
    project = jnp.dot(normed_one, qkv_full, precision=HIGH)
    queries = low(low_back(project[:, :width] + query_bias))
    keys = low(low_back(project[:, width:2 * width]))
    values = low(low_back(project[:, 2 * width:] + value_bias))
    factor = HEAD_DIM ** (-0.5)
    block = min(512, length)
    count = length // block
    query_blocks = queries.reshape(count, block, HEADS, HEAD_DIM)
    key_heads = keys.reshape(length, HEADS, HEAD_DIM)
    value_heads = values.reshape(length, HEADS, HEAD_DIM)
    position_blocks = positions.reshape(count, block)

    def attend(pair):
        rows_query, rows_position = pair
        scores = low_back(jnp.einsum('qhd,khd->hqk', rows_query, key_heads, precision=HIGH) * factor)
        allowed = (positions[None, :] <= rows_position[:, None])[None]
        scores = jnp.where(allowed, scores, -jnp.inf)
        highest = lax.optimization_barrier(jnp.max(scores, axis=-1, keepdims=True))
        weights = jnp.exp(scores - highest)
        probs = weights / lax.optimization_barrier(jnp.sum(weights, axis=-1, keepdims=True))
        return jnp.einsum('hqk,khd->qhd', low(probs), value_heads, precision=HIGH)
    attended = lax.map(jax.checkpoint(attend), (query_blocks, position_blocks)).reshape(length, width)
    attended = low(low_back(attended))
    middle = inputs + low_back(jnp.dot(attended, out_full, precision=HIGH) + out_bias)
    normed_two = low(layer_norm(middle, second_gain, second_shift))
    expanded = low_back(jnp.dot(normed_two, expand_full, precision=HIGH) + expand_bias)
    hidden = low(smooth_gelu(expanded))
    return middle + low_back(jnp.dot(hidden, shrink_full, precision=HIGH) + shrink_bias)

def reference(tokens, block_order, qkv_weight, query_bias, value_bias, out_weight, out_bias, expand_weight, expand_bias, shrink_weight, shrink_bias, first_gain, first_shift, second_gain, second_shift, cotangent):
    params = (qkv_weight.astype(jnp.float32), query_bias, value_bias, out_weight.astype(jnp.float32), out_bias, expand_weight.astype(jnp.float32), expand_bias, shrink_weight.astype(jnp.float32), shrink_bias, first_gain, first_shift, second_gain, second_shift)
    inputs = tokens.astype(jnp.float32)

    def forward(params, inputs):

        def one_sequence(pair):
            return sequence(params, pair[0], pair[1])
        return lax.map(one_sequence, (inputs, block_order))
    result, pullback = jax.vjp(forward, params, inputs)
    grad_params, grad_inputs = pullback(cotangent.astype(jnp.float32))
    return (result.astype(jnp.bfloat16), grad_inputs, grad_params[0], grad_params[3], grad_params[5], grad_params[7], grad_params[1], grad_params[2], grad_params[4], grad_params[6], grad_params[8], grad_params[9], grad_params[10], grad_params[11], grad_params[12])
```

```python
import functools
import itertools

import jax
import jax.numpy as jnp
from jax import lax
from jax.experimental import pallas as pl
from jax.experimental.pallas import tpu as pltpu
from jax.sharding import Mesh
from jax.sharding import PartitionSpec as P

HEADS = 25
HEAD_DIM = 64
EPSILON = 1e-05
MESH = pl.DeviceIdType.MESH
F32 = jnp.float32
BF16 = jnp.bfloat16
ANY = pl.BlockSpec(memory_space=pl.ANY)
VMEM = pl.BlockSpec(memory_space=pltpu.VMEM)


def offsets(sizes):
    return [o for o in itertools.product(*(range(s) for s in sizes)) if any(o)]


def moved(axes, sizes, offset, sign=1):
    return {
        a: lax.rem(lax.axis_index(a) + (o if sign > 0 else s - o), s)
        for a, s, o in zip(axes, sizes, offset)
    }


def flat(place, axes, sizes):
    index = 0
    for a, s in zip(axes, sizes):
        index = index * s + place[a]
    return index


def own_place(axes):
    return {a: lax.axis_index(a) for a in axes}


def greet(peers):
    barrier = pltpu.get_barrier_semaphore()
    for peer in peers:
        pl.semaphore_signal(barrier, inc=1, device_id=peer, device_id_type=MESH)
    pl.semaphore_wait(barrier, len(peers))


def remote(src, dst, send, recv, peer):
    return pltpu.make_async_remote_copy(
        src_ref=src,
        dst_ref=dst,
        send_sem=send,
        recv_sem=recv,
        device_id=peer,
        device_id_type=MESH,
    )


def gather_kernel(specs, *refs):
    count = len(specs)
    ins, outs = refs[:count], refs[count : 2 * count]
    scratch = refs[2 * count :]
    plans = []
    peers = []
    for index, (axes, sizes, pair) in enumerate(specs):
        offs = offsets(sizes)
        send, recv, local = scratch[3 * index : 3 * index + 3]
        side = lax.axis_index(pair)
        mate = {pair: 1 - side}
        plans.append((axes, sizes, offs, side, mate, ins[index], outs[index], send, recv, local))
        peers += [moved(axes, sizes, o) for o in offs] + [mate]
    greet(peers)
    started = []
    for axes, sizes, offs, side, mate, source, out, send, recv, local in plans:
        me = flat(own_place(axes), axes, sizes)
        here = pltpu.make_async_copy(source, out.at[me, side], local)
        here.start()
        for t, off in enumerate(offs):
            copy = remote(
                source, out.at[me, side], send.at[t], recv.at[t], moved(axes, sizes, off)
            )
            copy.start()
            started.append(copy)
        last = len(offs)
        copy = remote(source, out.at[me, side], send.at[last], recv.at[last], mate)
        copy.start()
        started.append(copy)
    for axes, sizes, offs, side, mate, source, out, send, recv, local in plans:
        last = len(offs)
        for t, off in enumerate(offs):
            came = flat(moved(axes, sizes, off, -1), axes, sizes)
            block = out.at[came, side]
            remote(source, block, send.at[t], recv.at[t], mate).wait_recv()
            copy = remote(block, block, send.at[last + 1 + t], recv.at[last + 1 + t], mate)
            copy.start()
            started.append(copy)
    for axes, sizes, offs, side, mate, source, out, send, recv, local in plans:
        last = len(offs)
        me = flat(own_place(axes), axes, sizes)
        pltpu.make_async_copy(source, out.at[me, side], local).wait()
        remote(source, out.at[me, 1 - side], send.at[last], recv.at[last], mate).wait_recv()
        for t, off in enumerate(offs):
            came = flat(moved(axes, sizes, off, -1), axes, sizes)
            remote(
                source, out.at[came, 1 - side], send.at[last + 1 + t], recv.at[last + 1 + t], mate
            ).wait_recv()
    for copy in started:
        copy.wait_send()


def gather(blocks, specs, ident):
    shapes, scratch, moved_bytes = [], [], 0
    for block, (axes, sizes, pair) in zip(blocks, specs):
        group = 1
        for s in sizes:
            group *= s
        shapes.append(jax.ShapeDtypeStruct((group, 2) + block.shape, block.dtype))
        scratch += [
            pltpu.SemaphoreType.DMA((2 * group,)),
            pltpu.SemaphoreType.DMA((2 * group,)),
            pltpu.SemaphoreType.DMA,
        ]
        moved_bytes += 2 * group * block.size * 2
    return pl.pallas_call(
        functools.partial(gather_kernel, specs),
        out_shape=shapes,
        in_specs=[VMEM] * len(blocks),
        out_specs=[ANY] * len(blocks),
        scratch_shapes=scratch,
        name="gather%d" % ident,
        compiler_params=pltpu.CompilerParams(collective_id=ident, has_side_effects=True),
        cost_estimate=pl.CostEstimate(
            flops=0, bytes_accessed=10 * moved_bytes, transcendentals=0
        ),
    )(*blocks)


def exchange_kernel(axes, sizes, source, out, send, recv, local):
    offs = offsets(sizes)
    greet([moved(axes, sizes, o) for o in offs])
    me = flat(own_place(axes), axes, sizes)
    here = pltpu.make_async_copy(source.at[me], out.at[me], local)
    here.start()
    started = []
    for t, off in enumerate(offs):
        peer = moved(axes, sizes, off)
        copy = remote(
            source.at[flat(peer, axes, sizes)], out.at[me], send.at[t], recv.at[t], peer
        )
        copy.start()
        started.append(copy)
    here.wait()
    for t, off in enumerate(offs):
        peer = moved(axes, sizes, off, -1)
        came = flat(peer, axes, sizes)
        remote(source.at[came], out.at[came], send.at[t], recv.at[t], peer).wait_recv()
    for copy in started:
        copy.wait_send()


def exchange(pieces, axes, sizes, ident):
    group = pieces.shape[0]
    return pl.pallas_call(
        functools.partial(exchange_kernel, axes, sizes),
        out_shape=jax.ShapeDtypeStruct(pieces.shape, pieces.dtype),
        in_specs=[VMEM],
        out_specs=VMEM,
        scratch_shapes=[
            pltpu.SemaphoreType.DMA((group,)),
            pltpu.SemaphoreType.DMA((group,)),
            pltpu.SemaphoreType.DMA,
        ],
        name="exchange%d" % ident,
        compiler_params=pltpu.CompilerParams(collective_id=ident, has_side_effects=True),
        cost_estimate=pl.CostEstimate(
            flops=0, bytes_accessed=20 * pieces.size, transcendentals=0
        ),
    )(pieces)


def scatter_kernel(axes, sizes, pair, source, out, first, summed, last, send, recv):
    offs = offsets(sizes)
    side = lax.axis_index(pair)
    mate = {pair: 1 - side}
    greet([moved(axes, sizes, o) for o in offs] + [mate])
    me = flat(own_place(axes), axes, sizes)
    count = len(offs)
    started = []
    for t, off in enumerate(offs + [(0,) * len(sizes)]):
        there = flat(moved(axes, sizes, off), axes, sizes)
        copy = remote(source.at[there, 1 - side], first.at[t], send.at[t], recv.at[t], mate)
        copy.start()
        started.append(copy)
    for t, off in enumerate(offs):
        peer = moved(axes, sizes, off)
        there = flat(peer, axes, sizes)
        started[t].wait_recv()
        summed[t] = (source[there, side].astype(F32) + first[t].astype(F32)).astype(BF16)
        slot = count + 1 + t
        copy = remote(summed.at[t], last.at[t], send.at[slot], recv.at[slot], peer)
        copy.start()
        started.append(copy)
    started[count].wait_recv()
    out[...] = source[me, side].astype(F32) + first[count].astype(F32)
    for t in range(count):
        started[count + 1 + t].wait_recv()
        out[...] += last[t].astype(F32)
    for copy in started:
        copy.wait_send()


def scatter(partial, axes, sizes, pair, ident):
    group = partial.shape[0]
    block = partial.shape[2:]
    return pl.pallas_call(
        functools.partial(scatter_kernel, axes, sizes, pair),
        out_shape=jax.ShapeDtypeStruct(block, F32),
        in_specs=[VMEM],
        out_specs=VMEM,
        scratch_shapes=[
            pltpu.VMEM((group,) + block, BF16),
            pltpu.VMEM((group - 1,) + block, BF16),
            pltpu.VMEM((group - 1,) + block, BF16),
            pltpu.SemaphoreType.DMA((2 * group,)),
            pltpu.SemaphoreType.DMA((2 * group,)),
        ],
        name="scatter%d" % ident,
        compiler_params=pltpu.CompilerParams(collective_id=ident, has_side_effects=True),
        cost_estimate=pl.CostEstimate(
            flops=0, bytes_accessed=20 * partial.size, transcendentals=0
        ),
    )(partial)


def total_kernel(axes, sizes, source, out, came, send, recv):
    offs = offsets(sizes)
    greet([moved(axes, sizes, o) for o in offs])
    me = flat(own_place(axes), axes, sizes)
    count = len(offs)
    started = []
    for t, off in enumerate(offs):
        peer = moved(axes, sizes, off)
        copy = remote(
            source.at[flat(peer, axes, sizes)], came.at[t], send.at[t], recv.at[t], peer
        )
        copy.start()
        started.append(copy)
    for copy in started:
        copy.wait_recv()
    out[me] = source[me] + jnp.sum(came[...], axis=0)
    second = []
    for t, off in enumerate(offs):
        peer = moved(axes, sizes, off)
        copy = remote(out.at[me], out.at[me], send.at[count + t], recv.at[count + t], peer)
        copy.start()
        second.append(copy)
    for t, off in enumerate(offs):
        peer = moved(axes, sizes, off, -1)
        block = out.at[flat(peer, axes, sizes)]
        remote(block, block, send.at[count + t], recv.at[count + t], peer).wait_recv()
    for copy in started + second:
        copy.wait_send()


def total(parts, axes, sizes, ident):
    group = parts.shape[0]
    return pl.pallas_call(
        functools.partial(total_kernel, axes, sizes),
        out_shape=jax.ShapeDtypeStruct(parts.shape, F32),
        in_specs=[VMEM],
        out_specs=VMEM,
        scratch_shapes=[
            pltpu.VMEM((group - 1,) + parts.shape[1:], F32),
            pltpu.SemaphoreType.DMA((2 * group,)),
            pltpu.SemaphoreType.DMA((2 * group,)),
        ],
        name="total%d" % ident,
        compiler_params=pltpu.CompilerParams(collective_id=ident, has_side_effects=True),
    )(parts)


def nt(left, right):
    return lax.dot_general(left, right, (((1,), (1,)), ((), ())), preferred_element_type=F32)


def nn(left, right):
    return lax.dot_general(left, right, (((1,), (0,)), ((), ())), preferred_element_type=F32)


def rows_of(inv, ref, pair, low, high):
    first = pl.multiple_of(inv[2 * pair] * HEAD_DIM, HEAD_DIM)
    second = pl.multiple_of(inv[2 * pair + 1] * HEAD_DIM, HEAD_DIM)
    return jnp.concatenate(
        [ref[pl.ds(first, 64), low:high], ref[pl.ds(second, 64), low:high]], axis=0
    )


def put_rows(inv, ref, pair, low, high, values):
    first = pl.multiple_of(inv[2 * pair] * HEAD_DIM, HEAD_DIM)
    second = pl.multiple_of(inv[2 * pair + 1] * HEAD_DIM, HEAD_DIM)
    ref[pl.ds(first, 64), low:high] = values[:64]
    ref[pl.ds(second, 64), low:high] = values[64:]


def head_slice(values, part, heads, head):
    low = (part * heads + head) * HEAD_DIM
    return values[:, low : low + HEAD_DIM]


def diagonal(block):
    return lax.broadcasted_iota(jnp.int32, (block, block), 0) <= lax.broadcasted_iota(
        jnp.int32, (block, block), 1
    )


def attend_kernel(heads, block, inv, qkv, out, lse, qs, ks, vt, ot):
    length = qkv.shape[0]
    width = heads * HEAD_DIM

    def sort(pair, unused):
        at = pl.multiple_of(pair * 128, 128)
        values = rows_of(inv, qkv, pair, 0, 3 * width)
        for h in range(heads):
            qs[h, pl.ds(at, 128), :] = head_slice(values, 0, heads, h) * BF16(0.125)
            ks[h, pl.ds(at, 128), :] = head_slice(values, 1, heads, h)
            vt[h, :, pl.ds(at, 128)] = head_slice(values, 2, heads, h).astype(F32).T.astype(BF16)
        return unused

    lax.fori_loop(0, length // 128, sort, 0)
    allowed = diagonal(block)

    def row(qi, unused):
        q_at = pl.multiple_of(qi * block, block)

        def first(h):
            scores = nt(ks[h, pl.ds(q_at, block), :], qs[h, pl.ds(q_at, block), :])
            scores = jnp.where(allowed, scores, -1e30)
            high = jnp.max(scores, axis=0, keepdims=True)
            probs = jnp.exp(scores - high)
            return (
                high,
                jnp.sum(probs, axis=0, keepdims=True),
                nn(vt[h, :, pl.ds(q_at, block)], probs.astype(BF16)),
            )

        def column(kj, state):
            k_at = pl.multiple_of(kj * block, block)
            fresh_state = []
            for h in range(heads):
                high, weight, acc = state[h]
                scores = nt(ks[h, pl.ds(k_at, block), :], qs[h, pl.ds(q_at, block), :])
                fresh = jnp.maximum(high, jnp.max(scores, axis=0, keepdims=True))
                probs = jnp.exp(scores - fresh)
                fade = jnp.exp(high - fresh)
                fresh_state.append(
                    (
                        fresh,
                        weight * fade + jnp.sum(probs, axis=0, keepdims=True),
                        acc * fade + nn(vt[h, :, pl.ds(k_at, block)], probs.astype(BF16)),
                    )
                )
            return tuple(fresh_state)

        state = lax.fori_loop(0, qi, column, tuple(first(h) for h in range(heads)))
        for h in range(heads):
            high, weight, acc = state[h]
            ot[h, :, pl.ds(q_at, block)] = acc / weight
            lse[h : h + 1, pl.ds(q_at, block)] = high + jnp.log(weight)
        return unused

    lax.fori_loop(0, length // block, row, 0)

    def unsort(pair, unused):
        at = pl.multiple_of(pair * 128, 128)
        values = [ot[h, :, pl.ds(at, 128)].T for h in range(heads)]
        put_rows(inv, out, pair, 0, width, jnp.concatenate(values, axis=1))
        return unused

    lax.fori_loop(0, length // 128, unsort, 0)


def attend(inv, qkv, heads):
    length = qkv.shape[0]
    width = heads * HEAD_DIM
    block = min(256, length)
    pairs = length * (length + block) // 2
    return pl.pallas_call(
        functools.partial(attend_kernel, heads, block),
        out_shape=(
            jax.ShapeDtypeStruct((length, width), F32),
            jax.ShapeDtypeStruct((heads, length), F32),
        ),
        grid_spec=pltpu.PrefetchScalarGridSpec(
            num_scalar_prefetch=1,
            grid=(1,),
            in_specs=[pl.BlockSpec((length, 3 * width), lambda i, inv: (0, 0))],
            out_specs=(
                pl.BlockSpec((length, width), lambda i, inv: (0, 0)),
                pl.BlockSpec((heads, length), lambda i, inv: (0, 0)),
            ),
            scratch_shapes=[
                pltpu.VMEM((heads, length, HEAD_DIM), BF16),
                pltpu.VMEM((heads, length, HEAD_DIM), BF16),
                pltpu.VMEM((heads, HEAD_DIM, length), BF16),
                pltpu.VMEM((heads, HEAD_DIM, length), F32),
            ],
        ),
        name="attend",
        cost_estimate=pl.CostEstimate(
            flops=4 * heads * pairs * HEAD_DIM * 4,
            bytes_accessed=length * width * 10,
            transcendentals=heads * pairs,
        ),
    )(inv, qkv)


def attend_back_kernel(
    heads, block, inv, qkv, grads, outs, lse, dqkv, qs, ks, vs, gs, kt, delta, dqt, dks, dvs
):
    length = qkv.shape[0]
    width = heads * HEAD_DIM
    count = length // block

    def sort(pair, unused):
        at = pl.multiple_of(pair * 128, 128)
        values = rows_of(inv, qkv, pair, 0, 3 * width)
        grad = rows_of(inv, grads, pair, 0, width)
        value = rows_of(inv, outs, pair, 0, width)
        product = (grad.astype(F32) * value).T
        for h in range(heads):
            qs[h, pl.ds(at, 128), :] = head_slice(values, 0, heads, h) * BF16(0.125)
            key = head_slice(values, 1, heads, h)
            ks[h, pl.ds(at, 128), :] = key
            kt[h, :, pl.ds(at, 128)] = key.astype(F32).T.astype(BF16)
            vs[h, pl.ds(at, 128), :] = head_slice(values, 2, heads, h)
            gs[h, pl.ds(at, 128), :] = head_slice(grad, 0, heads, h)
            delta[h : h + 1, pl.ds(at, 128)] = jnp.sum(
                product[h * HEAD_DIM : (h + 1) * HEAD_DIM], axis=0, keepdims=True
            )
            dqt[h, :, pl.ds(at, 128)] = jnp.zeros((HEAD_DIM, 128), F32)
        return unused

    lax.fori_loop(0, length // 128, sort, 0)
    allowed = diagonal(block)

    def column(kj, unused):
        k_at = pl.multiple_of(kj * block, block)

        def tile(h, q_at, masked):
            q = qs[h, pl.ds(q_at, block), :]
            g = gs[h, pl.ds(q_at, block), :]
            scores = nt(ks[h, pl.ds(k_at, block), :], q)
            probs = jnp.exp(scores - lse[h : h + 1, pl.ds(q_at, block)])
            if masked:
                probs = jnp.where(allowed, probs, 0.0)
            slopes = nt(vs[h, pl.ds(k_at, block), :], g)
            low = (probs * (slopes - delta[h : h + 1, pl.ds(q_at, block)])).astype(BF16)
            dqt[h, :, pl.ds(q_at, block)] += nn(kt[h, :, pl.ds(k_at, block)], low)
            return nn(low, q), nn(probs.astype(BF16), g)

        def row(qi, state):
            q_at = pl.multiple_of(qi * block, block)
            fresh = []
            for h in range(heads):
                dk, dv = tile(h, q_at, False)
                fresh.append((state[h][0] + dk, state[h][1] + dv))
            return tuple(fresh)

        state = tuple(tile(h, k_at, True) for h in range(heads))
        state = lax.fori_loop(kj + 1, count, row, state)
        for h in range(heads):
            dks[h, pl.ds(k_at, block), :] = state[h][0].astype(BF16)
            dvs[h, pl.ds(k_at, block), :] = state[h][1].astype(BF16)
        return unused

    lax.fori_loop(0, count, column, 0)

    def unsort(pair, unused):
        at = pl.multiple_of(pair * 128, 128)
        values = [(dqt[h, :, pl.ds(at, 128)].T * 0.125).astype(BF16) for h in range(heads)]
        values += [dks[h, pl.ds(at, 128), :] for h in range(heads)]
        values += [dvs[h, pl.ds(at, 128), :] for h in range(heads)]
        put_rows(inv, dqkv, pair, 0, 3 * width, jnp.concatenate(values, axis=1))
        return unused

    lax.fori_loop(0, length // 128, unsort, 0)


def attend_back(inv, qkv, grads, outs, lse, heads):
    length = qkv.shape[0]
    width = heads * HEAD_DIM
    block = min(256, length)
    pairs = length * (length + block) // 2
    row_shape = (heads, length, HEAD_DIM)
    return pl.pallas_call(
        functools.partial(attend_back_kernel, heads, block),
        out_shape=jax.ShapeDtypeStruct((length, 3 * width), BF16),
        grid_spec=pltpu.PrefetchScalarGridSpec(
            num_scalar_prefetch=1,
            grid=(1,),
            in_specs=[
                pl.BlockSpec((length, 3 * width), lambda i, inv: (0, 0)),
                pl.BlockSpec((length, width), lambda i, inv: (0, 0)),
                pl.BlockSpec((length, width), lambda i, inv: (0, 0)),
                pl.BlockSpec((heads, length), lambda i, inv: (0, 0)),
            ],
            out_specs=pl.BlockSpec((length, 3 * width), lambda i, inv: (0, 0)),
            scratch_shapes=[
                pltpu.VMEM(row_shape, BF16),
                pltpu.VMEM(row_shape, BF16),
                pltpu.VMEM(row_shape, BF16),
                pltpu.VMEM(row_shape, BF16),
                pltpu.VMEM((heads, HEAD_DIM, length), BF16),
                pltpu.VMEM((heads, length), F32),
                pltpu.VMEM((heads, HEAD_DIM, length), F32),
                pltpu.VMEM(row_shape, BF16),
                pltpu.VMEM(row_shape, BF16),
            ],
        ),
        name="attend_back",
        cost_estimate=pl.CostEstimate(
            flops=10 * heads * pairs * HEAD_DIM * 4,
            bytes_accessed=length * width * 20,
            transcendentals=heads * pairs,
        ),
    )(inv, qkv, grads, outs, lse)


def layer_norm(values, gain, shift):
    center = jnp.mean(values, axis=-1, keepdims=True)
    centred = values - center
    spread = jnp.mean(centred * centred, axis=-1, keepdims=True)
    return centred * lax.rsqrt(spread + EPSILON) * gain + shift


def smooth_gelu(values):
    return (
        0.5
        * values
        * (1.0 + jnp.tanh(0.7978845608028654 * (values + 0.044715 * values * values * values)))
    )


def matmul(left, right):
    return jnp.dot(left, right, preferred_element_type=F32)


def against(left, weight):
    return lax.dot_general(left, weight, (((1,), (1,)), ((), ())), preferred_element_type=F32)


def onto(left, right):
    return lax.dot_general(left, right, (((0,), (0,)), ((), ())), preferred_element_type=F32)


def body(
    sizes,
    tokens,
    block_order,
    qkv_weight,
    query_bias,
    value_bias,
    out_weight,
    out_bias,
    expand_weight,
    expand_bias,
    shrink_weight,
    shrink_bias,
    first_gain,
    first_shift,
    second_gain,
    second_shift,
    cotangent,
):
    outer, inner, xs, ks = (sizes[a] for a in ("o", "i", "x", "k"))
    spots = outer * inner
    shards = xs * ks
    rows, width = tokens.shape[1:]
    o, i = lax.axis_index("o"), lax.axis_index("i")
    shard = lax.axis_index("x") * ks + lax.axis_index("k")
    place = o * inner + i
    heads = -(-HEADS // spots)
    span = heads * HEAD_DIM
    padded = spots * span
    part = qkv_weight.shape[0]
    hidden = expand_weight.shape[1]
    piece = hidden // (shards * inner)
    ctx = (("o",), (outer,), "i")
    group = (("i", "x"), (inner, xs), "k")
    pair = (("x",), (xs,), "k")
    own = tokens[0]
    own_grad = cotangent[0]

    def columns(values, count):
        wide = values.reshape(values.shape[:-1] + (count, width))
        wide = jnp.pad(wide, [(0, 0)] * (wide.ndim - 1) + [(0, padded - width)])
        return lax.dynamic_slice_in_dim(wide, place * span, span, axis=wide.ndim - 1)

    qkv_own = columns(qkv_weight, 3).reshape(part, 3 * span)
    qkv_bias = jnp.concatenate(
        [columns(query_bias, 1)[0], jnp.zeros((span,), F32), columns(value_bias, 1)[0]]
    )
    gathered, qkv_columns = gather([own, qkv_own], [ctx, pair], 0)
    sequence = gathered.reshape(spots * rows, width)
    qkv_columns = qkv_columns.reshape(width, 3 * span)

    later = lax.optimization_barrier((out_weight, own_grad, gathered[0, 0, :8, :128]))
    out_full = lax.all_gather(later[0], ("x", "k"), axis=0, tiled=True)
    group_grad = lax.all_gather(later[1], ("i", "x", "k"), axis=0, tiled=True)

    expand_pieces = expand_weight.reshape(part, shards, inner, piece)
    expand_pieces = lax.dynamic_index_in_dim(expand_pieces, i, axis=2, keepdims=False)
    expand_pieces = expand_pieces.transpose(1, 0, 2)
    came = [lax.dynamic_index_in_dim(expand_pieces, shard, axis=0, keepdims=False)]
    for step in range(1, shards):
        there = lax.rem(shard + step, shards)
        sent = lax.dynamic_index_in_dim(expand_pieces, there, axis=0, keepdims=False)
        came.append(
            lax.ppermute(sent, ("x", "k"), [(f, (f + step) % shards) for f in range(shards)])
        )
    stacked = jnp.stack(came)
    order = lax.rem(shard - jnp.arange(shards) + shards, shards)
    expand_columns = jnp.take(stacked, order, axis=0).reshape(width, piece)
    shrink_rows = lax.dynamic_slice_in_dim(shrink_weight, i * piece, piece, axis=0)
    expand_own_bias = lax.dynamic_slice_in_dim(
        expand_bias, (shard * inner + i) * piece, piece, axis=0
    )

    order_row = block_order[0]
    blocks = order_row.shape[0]
    inv = jnp.sum(
        jnp.where(
            order_row[:, None] == jnp.arange(blocks, dtype=jnp.int32)[None, :],
            jnp.arange(blocks, dtype=jnp.int32)[:, None],
            0,
        ),
        axis=0,
    ).astype(jnp.int32)
    normed_low = layer_norm(sequence.astype(F32), first_gain, first_shift).astype(BF16)
    qkv = (matmul(normed_low, qkv_columns) + qkv_bias).astype(BF16)
    attended, log_sum = attend(inv, qkv, heads)
    came_out = exchange(
        attended.astype(BF16).reshape(spots, rows, span), ("o", "i"), (outer, inner), 1
    )
    attended_low = came_out.transpose(1, 0, 2).reshape(rows, padded)[:, :width]

    inputs = own.astype(F32)
    middle = inputs + matmul(attended_low, out_full) + out_bias
    lowered_two = layer_norm(middle, second_gain, second_shift).astype(BF16)

    (group_low,) = gather([lowered_two], [group], 2)
    group_low = group_low.reshape(-1, width)
    expanded = matmul(group_low, expand_columns) + expand_own_bias
    hidden_low = smooth_gelu(expanded).astype(BF16)
    grad_hidden = against(group_grad, shrink_rows)
    unused, gelu_back = jax.vjp(smooth_gelu, expanded)
    (grad_expanded,) = gelu_back(grad_hidden)
    expanded_low = grad_expanded.astype(BF16)
    grad_partial = against(expanded_low, expand_columns).astype(BF16)
    shape = (inner * xs, ks, rows, width)
    grad_normed_two = scatter(grad_partial.reshape(shape), *group, 3)
    result_partial = matmul(hidden_low, shrink_rows).astype(BF16)
    shrunk = scatter(result_partial.reshape(shape), *group, 4)
    result = middle + shrunk + shrink_bias

    grad_result = own_grad.astype(F32)
    unused, second_back = jax.vjp(layer_norm, middle, second_gain, second_shift)
    grad_middle_norm, grad_second_gain, grad_second_shift = second_back(grad_normed_two)
    grad_middle = grad_result + grad_middle_norm
    middle_low = grad_middle.astype(BF16)
    grad_att_low = against(middle_low, out_full).astype(BF16)
    grad_att_padded = jnp.pad(grad_att_low, ((0, 0), (0, padded - width)))
    grad_heads = exchange(
        grad_att_padded.reshape(rows, spots, span).transpose(1, 0, 2),
        ("o", "i"),
        (outer, inner),
        5,
    ).reshape(spots * rows, span)

    dqkv = attend_back(inv, qkv, grad_heads, attended, log_sum, heads)
    norm_partial = against(dqkv, qkv_columns).astype(BF16)
    grad_normed_one = scatter(norm_partial.reshape(outer, inner, rows, width), *ctx, 6)
    unused, first_back = jax.vjp(layer_norm, inputs, first_gain, first_shift)
    grad_first_input, grad_first_gain, grad_first_shift = first_back(grad_normed_one)
    grad_inputs = grad_middle + grad_first_input

    axes = ("o", "i", "x", "k")
    out_rows = width // (shards * inner)
    att_pieces = attended_low.reshape(rows, shards, inner, out_rows).transpose(2, 1, 0, 3)
    att_group = lax.all_to_all(
        att_pieces.reshape(inner * shards, rows, out_rows),
        ("i", "x", "k"),
        split_axis=0,
        concat_axis=0,
        tiled=True,
    ).reshape(-1, out_rows)
    middle_group = lax.all_gather(middle_low, ("i", "x", "k"), axis=0, tiled=True)
    both = jnp.concatenate(
        [onto(hidden_low, group_grad).astype(BF16), onto(att_group, middle_group).astype(BF16)],
        axis=0,
    )
    both = lax.psum_scatter(both, "o", scatter_dimension=1, tiled=True)
    cell = both.shape[1] // inner
    both = lax.all_to_all(
        both.reshape(piece + out_rows, inner, cell), "i", split_axis=1, concat_axis=1
    )
    grad_shrink = both[:piece].transpose(1, 0, 2).reshape(inner * piece, cell).astype(F32)
    grad_outw = both[piece:].transpose(1, 0, 2).reshape(inner * out_rows, cell).astype(F32)

    cuts = outer // shards
    expand_partial = onto(group_low, expanded_low).astype(BF16)
    expand_partial = expand_partial.reshape(shards, part, cuts, piece // cuts).transpose(0, 2, 1, 3)
    expand_partial = lax.psum_scatter(
        expand_partial.reshape(outer, part, piece // cuts), "o", scatter_dimension=0, tiled=True
    )[0]
    routes = []
    for so in range(outer):
        for si in range(inner):
            for sf in range(shards):
                spot = sf * (spots // shards) + si * (spots // (shards * inner)) + so % cuts
                routes.append(
                    (
                        (so * inner + si) * shards + sf,
                        spot * shards + so // cuts,
                    )
                )
    grad_expand = lax.ppermute(expand_partial, axes, routes).astype(F32)

    qkv_partial = onto(normed_low, dqkv).astype(BF16)
    qkv_partial = lax.psum_scatter(qkv_partial, ("x", "k"), scatter_dimension=0, tiled=True)
    qkv_all = lax.all_gather(qkv_partial, ("o", "i"), axis=0, tiled=False)
    qkv_all = qkv_all.reshape(spots, part, 3, span).transpose(1, 2, 0, 3)
    qkv_all = qkv_all.reshape(part, 3, padded)[:, :, :width].reshape(part, 3 * width)
    share = 3 * width // spots
    grad_qkv = lax.dynamic_slice_in_dim(qkv_all, place * share, share, axis=1).astype(F32)

    def placed(values, start, size):
        return lax.dynamic_update_slice_in_dim(jnp.zeros((size,), F32), values, start, axis=0)

    dqkv_sums = jnp.sum(dqkv.astype(F32), axis=0)
    small = [
        placed(dqkv_sums[:span], place * span, padded),
        placed(dqkv_sums[2 * span :], place * span, padded),
        jnp.sum(middle_low.astype(F32), axis=0),
        placed(
            jnp.sum(expanded_low.astype(F32), axis=0), (shard * inner + i) * piece, hidden
        ),
        jnp.sum(grad_result, axis=0),
        grad_first_gain,
        grad_first_shift,
        grad_second_gain,
        grad_second_shift,
    ]
    lengths = [s.shape[0] for s in small]
    devices = spots * shards
    lanes = 128 * (-(-sum(lengths) // (devices * 1024)))
    line = jnp.concatenate(small)
    line = jnp.pad(line, (0, devices * 8 * lanes - line.shape[0])).reshape(devices, 8, lanes)
    line = total(line, axes, (outer, inner, xs, ks), 7).reshape(-1)
    summed = []
    start = 0
    for length in lengths:
        summed.append(line[start : start + length])
        start += length
    summed[0] = summed[0][:width]
    summed[1] = summed[1][:width]
    return (
        result.astype(BF16)[None],
        grad_inputs[None],
        grad_qkv,
        grad_outw,
        grad_expand,
        grad_shrink,
        *summed,
    )


def solution(mesh):
    spots, shards = mesh.shape["ctx"], mesh.shape["fsdp"]
    sizes = {"o": spots // 2, "i": 2, "x": shards // 2, "k": 2}
    fine = Mesh(mesh.devices.reshape(tuple(sizes.values())), tuple(sizes))
    seq, pos = ("x", "k"), ("o", "i")
    weight = P(seq, None)
    placed = (
        P(seq, pos, None),
        P(seq, None),
        weight,
        P(),
        P(),
        weight,
        P(),
        weight,
        P(),
        weight,
        P(),
        P(),
        P(),
        P(),
        P(),
        P(seq, pos, None),
    )
    given = (P(seq, pos, None),) * 2 + (P(seq, pos),) * 4 + (P(),) * 9
    return jax.shard_map(
        functools.partial(body, sizes),
        mesh=fine,
        in_specs=placed,
        out_specs=given,
        check_vma=False,
    )
```

```python
import functools
import itertools

import jax
import jax.numpy as jnp
from jax import lax
from jax.experimental import pallas as pl
from jax.experimental.pallas import tpu as pltpu
from jax.sharding import Mesh
from jax.sharding import PartitionSpec as P

HEADS = 25
HEAD_DIM = 64
EPSILON = 1e-05
MESH = pl.DeviceIdType.MESH
F32 = jnp.float32
BF16 = jnp.bfloat16
ANY = pl.BlockSpec(memory_space=pl.ANY)
VMEM = pl.BlockSpec(memory_space=pltpu.VMEM)


def offsets(sizes):
    return [o for o in itertools.product(*(range(s) for s in sizes)) if any(o)]


def moved(axes, sizes, offset, sign=1):
    return {
        a: lax.rem(lax.axis_index(a) + (o if sign > 0 else s - o), s)
        for a, s, o in zip(axes, sizes, offset)
    }


def flat(place, axes, sizes):
    index = 0
    for a, s in zip(axes, sizes):
        index = index * s + place[a]
    return index


def own_place(axes):
    return {a: lax.axis_index(a) for a in axes}


def greet(peers):
    barrier = pltpu.get_barrier_semaphore()
    for peer in peers:
        pl.semaphore_signal(barrier, inc=1, device_id=peer, device_id_type=MESH)
    pl.semaphore_wait(barrier, len(peers))


def remote(src, dst, send, recv, peer):
    return pltpu.make_async_remote_copy(
        src_ref=src,
        dst_ref=dst,
        send_sem=send,
        recv_sem=recv,
        device_id=peer,
        device_id_type=MESH,
    )


class Gather:
    def __init__(self, axes, sizes, pair, source, out, send, recv, local):
        self.axes, self.sizes = axes, sizes
        self.offs = offsets(sizes)
        self.side = lax.axis_index(pair)
        self.mate = {pair: 1 - self.side}
        self.source, self.out, self.send, self.recv, self.local = source, out, send, recv, local
        self.started = []

    def peers(self):
        return [moved(self.axes, self.sizes, o) for o in self.offs] + [self.mate]

    def mine(self):
        return self.out.at[flat(own_place(self.axes), self.axes, self.sizes), self.side]

    def start(self):
        pltpu.make_async_copy(self.source, self.mine(), self.local).start()
        last = len(self.offs)
        for t, peer in enumerate(self.peers()):
            copy = remote(self.source, self.mine(), self.send.at[t], self.recv.at[t], peer)
            copy.start()
            self.started.append(copy)

    def hand_on(self):
        last = len(self.offs)
        for t, off in enumerate(self.offs):
            came = flat(moved(self.axes, self.sizes, off, -1), self.axes, self.sizes)
            block = self.out.at[came, self.side]
            remote(self.source, block, self.send.at[t], self.recv.at[t], self.mate).wait_recv()
            slot = last + 1 + t
            copy = remote(block, block, self.send.at[slot], self.recv.at[slot], self.mate)
            copy.start()
            self.started.append(copy)

    def finish(self):
        last = len(self.offs)
        me = flat(own_place(self.axes), self.axes, self.sizes)
        pltpu.make_async_copy(self.source, self.mine(), self.local).wait()
        block = self.out.at[me, 1 - self.side]
        remote(self.source, block, self.send.at[last], self.recv.at[last], self.mate).wait_recv()
        for t, off in enumerate(self.offs):
            came = flat(moved(self.axes, self.sizes, off, -1), self.axes, self.sizes)
            slot = last + 1 + t
            block = self.out.at[came, 1 - self.side]
            remote(
                self.source, block, self.send.at[slot], self.recv.at[slot], self.mate
            ).wait_recv()
        for copy in self.started:
            copy.wait_send()


def gather_shape(block, spec):
    group = 1
    for s in spec[1]:
        group *= s
    return jax.ShapeDtypeStruct((group, 2) + block.shape, block.dtype)


def gather_scratch(spec):
    group = 1
    for s in spec[1]:
        group *= s
    return [
        pltpu.SemaphoreType.DMA((2 * group,)),
        pltpu.SemaphoreType.DMA((2 * group,)),
        pltpu.SemaphoreType.DMA,
    ]


def sent_estimate(size):
    return pl.CostEstimate(flops=0, bytes_accessed=20 * size, transcendentals=0)


def gather_kernel(specs, *refs):
    count = len(specs)
    gathers = [
        Gather(*spec, refs[n], refs[count + n], *refs[2 * count + 3 * n : 2 * count + 3 * n + 3])
        for n, spec in enumerate(specs)
    ]
    greet([peer for g in gathers for peer in g.peers()])
    for g in gathers:
        g.start()
    for g in gathers:
        g.hand_on()
    for g in gathers:
        g.finish()


def gather(blocks, specs, ident):
    shapes = [gather_shape(block, spec) for block, spec in zip(blocks, specs)]
    return pl.pallas_call(
        functools.partial(gather_kernel, specs),
        out_shape=shapes,
        in_specs=[VMEM] * len(blocks),
        out_specs=[ANY] * len(blocks),
        scratch_shapes=[s for spec in specs for s in gather_scratch(spec)],
        name="gather%d" % ident,
        compiler_params=pltpu.CompilerParams(collective_id=ident, has_side_effects=True),
        cost_estimate=sent_estimate(sum(s.size for s in shapes)),
    )(*blocks)


def first_kernel(
    specs, shard_sizes, own, columns, weight, all_tokens, all_columns, pieces, whole, cut, *sems
):
    axes = ("x", "k")
    offs = offsets(shard_sizes)
    tokens = Gather(*specs[0], own, all_tokens, *sems[0:3])
    heads = Gather(*specs[1], columns, all_columns, *sems[3:6])
    read, send, recv, local = sems[6:10]
    fetch = pltpu.make_async_copy(weight, whole, read)
    fetch.start()
    greet(tokens.peers() + heads.peers() + [moved(axes, shard_sizes, o) for o in offs])
    tokens.start()
    heads.start()
    fetch.wait()
    width = cut.shape[2]
    inner = lax.axis_index("i")
    for half in range(2):

        @pl.when(inner == half)
        def _():
            for f in range(cut.shape[0]):
                low = (2 * f + half) * width
                cut[f] = whole[:, low : low + width]

    me = flat(own_place(axes), axes, shard_sizes)
    here = pltpu.make_async_copy(cut.at[me], pieces.at[me], local)
    here.start()
    started = []
    for t, off in enumerate(offs):
        peer = moved(axes, shard_sizes, off)
        there = flat(peer, axes, shard_sizes)
        copy = remote(cut.at[there], pieces.at[me], send.at[t], recv.at[t], peer)
        copy.start()
        started.append(copy)
    heads.hand_on()
    tokens.hand_on()
    here.wait()
    for t, off in enumerate(offs):
        peer = moved(axes, shard_sizes, off, -1)
        came = flat(peer, axes, shard_sizes)
        remote(cut.at[came], pieces.at[came], send.at[t], recv.at[t], peer).wait_recv()
    for copy in started:
        copy.wait_send()
    heads.finish()
    tokens.finish()


def first_gather(own, columns, weight, specs, shard_sizes, piece, ident):
    shards = shard_sizes[0] * shard_sizes[1]
    part = weight.shape[0]
    shapes = [
        gather_shape(own, specs[0]),
        gather_shape(columns, specs[1]),
        jax.ShapeDtypeStruct((shards, part, piece), BF16),
    ]
    return pl.pallas_call(
        functools.partial(first_kernel, specs, shard_sizes),
        out_shape=shapes,
        in_specs=[VMEM, VMEM, ANY],
        out_specs=[ANY] * 3,
        scratch_shapes=[
            pltpu.VMEM(weight.shape, BF16),
            pltpu.VMEM((shards, part, piece), BF16),
            *gather_scratch(specs[0]),
            *gather_scratch(specs[1]),
            pltpu.SemaphoreType.DMA,
            pltpu.SemaphoreType.DMA((shards,)),
            pltpu.SemaphoreType.DMA((shards,)),
            pltpu.SemaphoreType.DMA,
        ],
        name="first%d" % ident,
        compiler_params=pltpu.CompilerParams(collective_id=ident, has_side_effects=True),
        cost_estimate=sent_estimate(sum(s.size for s in shapes)),
    )(own, columns, weight)


def pieces_out(axes, sizes, source, out, send, recv):
    me = flat(own_place(axes), axes, sizes)
    started = []
    for t, off in enumerate(offsets(sizes)):
        peer = moved(axes, sizes, off)
        copy = remote(
            source.at[flat(peer, axes, sizes)], out.at[me], send.at[t], recv.at[t], peer
        )
        copy.start()
        started.append(copy)
    return started


def pieces_in(axes, sizes, source, out, send, recv, started):
    for t, off in enumerate(offsets(sizes)):
        peer = moved(axes, sizes, off, -1)
        came = flat(peer, axes, sizes)
        remote(source.at[came], out.at[came], send.at[t], recv.at[t], peer).wait_recv()
    for copy in started:
        copy.wait_send()


def to_tokens_kernel(
    axes, sizes, spec, source, block, out, everyone, came, send, recv, *gather_sems
):
    beside = Gather(*spec, block, everyone, *gather_sems)
    greet([moved(axes, sizes, o) for o in offsets(sizes)] + beside.peers())
    started = pieces_out(axes, sizes, source, came, send, recv)
    beside.start()
    me = flat(own_place(axes), axes, sizes)
    came[me] = source[me]
    pieces_in(axes, sizes, source, came, send, recv, started)
    span, width = came.shape[2], out.shape[1]
    for d in range(came.shape[0]):
        low, high = d * span, min((d + 1) * span, width)
        if low < high:
            out[:, low:high] = came[d, :, : high - low]
    beside.hand_on()
    beside.finish()


def to_tokens(pieces, block, width, axes, sizes, spec, ident):
    group, rows, span = pieces.shape
    return pl.pallas_call(
        functools.partial(to_tokens_kernel, axes, sizes, spec),
        out_shape=[
            jax.ShapeDtypeStruct((rows, width), pieces.dtype),
            gather_shape(block, spec),
        ],
        in_specs=[VMEM, VMEM],
        out_specs=[VMEM, ANY],
        scratch_shapes=[
            pltpu.VMEM(pieces.shape, pieces.dtype),
            pltpu.SemaphoreType.DMA((group,)),
            pltpu.SemaphoreType.DMA((group,)),
            *gather_scratch(spec),
        ],
        name="to_tokens%d" % ident,
        compiler_params=pltpu.CompilerParams(collective_id=ident, has_side_effects=True),
        cost_estimate=sent_estimate(3 * pieces.size),
    )(pieces, block)


def to_heads_kernel(
    axes,
    sizes,
    spec,
    group_axes,
    group_sizes,
    source,
    block,
    att,
    out,
    everyone,
    att_out,
    cut,
    att_cut,
    send,
    recv,
    att_send,
    att_recv,
    *gather_sems,
):
    beside = Gather(*spec, block, everyone, *gather_sems)
    greet(
        [moved(axes, sizes, o) for o in offsets(sizes)]
        + [moved(group_axes, group_sizes, o) for o in offsets(group_sizes)]
    )
    span, width = cut.shape[2], source.shape[1]
    for d in range(cut.shape[0]):
        low, high = d * span, min((d + 1) * span, width)
        if high - low < span:
            cut[d] = jnp.zeros(cut.shape[1:], cut.dtype)
        if low < high:
            cut[d, :, : high - low] = source[:, low:high]
    cell = att_cut.shape[2]
    inner, shards = group_sizes[0], group_sizes[1] * group_sizes[2]
    for half in range(inner):
        for f in range(shards):
            low = (f * inner + half) * cell
            att_cut[half * shards + f] = att[:, low : low + cell]
    started = pieces_out(axes, sizes, cut, out, send, recv)
    att_started = pieces_out(group_axes, group_sizes, att_cut, att_out, att_send, att_recv)
    beside.start()
    me = flat(own_place(axes), axes, sizes)
    out[me] = cut[me]
    me = flat(own_place(group_axes), group_axes, group_sizes)
    att_out[me] = att_cut[me]
    pieces_in(axes, sizes, cut, out, send, recv, started)
    beside.hand_on()
    pieces_in(group_axes, group_sizes, att_cut, att_out, att_send, att_recv, att_started)
    beside.finish()


def to_heads(source, block, att, span, axes, sizes, spec, group_axes, group_sizes, ident):
    rows, width = source.shape
    count, group = 1, 1
    for s in sizes:
        count *= s
    for s in group_sizes:
        group *= s
    cell = width // group
    return pl.pallas_call(
        functools.partial(to_heads_kernel, axes, sizes, spec, group_axes, group_sizes),
        out_shape=[
            jax.ShapeDtypeStruct((count, rows, span), source.dtype),
            gather_shape(block, spec),
            jax.ShapeDtypeStruct((group, rows, cell), att.dtype),
        ],
        in_specs=[VMEM, VMEM, VMEM],
        out_specs=[VMEM, ANY, VMEM],
        scratch_shapes=[
            pltpu.VMEM((count, rows, span), source.dtype),
            pltpu.VMEM((group, rows, cell), att.dtype),
            pltpu.SemaphoreType.DMA((count,)),
            pltpu.SemaphoreType.DMA((count,)),
            pltpu.SemaphoreType.DMA((group,)),
            pltpu.SemaphoreType.DMA((group,)),
            *gather_scratch(spec),
        ],
        name="to_heads%d" % ident,
        compiler_params=pltpu.CompilerParams(collective_id=ident, has_side_effects=True),
        cost_estimate=sent_estimate(8 * source.size),
    )(source, block, att)


class Scatter:
    def __init__(self, axes, sizes, pair, source, out, first, summed, last, send, recv):
        self.axes, self.sizes = axes, sizes
        self.offs = offsets(sizes)
        self.side = lax.axis_index(pair)
        self.mate = {pair: 1 - self.side}
        self.source, self.out = source, out
        self.first, self.summed, self.last = first, summed, last
        self.send, self.recv = send, recv
        self.started = []

    def peers(self):
        return [moved(self.axes, self.sizes, o) for o in self.offs] + [self.mate]

    def start(self):
        for t, off in enumerate(self.offs + [(0,) * len(self.sizes)]):
            there = flat(moved(self.axes, self.sizes, off), self.axes, self.sizes)
            copy = remote(
                self.source.at[there, 1 - self.side],
                self.first.at[t],
                self.send.at[t],
                self.recv.at[t],
                self.mate,
            )
            copy.start()
            self.started.append(copy)

    def add(self):
        count = len(self.offs)
        for t, off in enumerate(self.offs):
            peer = moved(self.axes, self.sizes, off)
            there = flat(peer, self.axes, self.sizes)
            self.started[t].wait_recv()
            self.summed[t] = (
                self.source[there, self.side].astype(F32) + self.first[t].astype(F32)
            ).astype(BF16)
            slot = count + 1 + t
            copy = remote(
                self.summed.at[t], self.last.at[t], self.send.at[slot], self.recv.at[slot], peer
            )
            copy.start()
            self.started.append(copy)

    def finish(self):
        count = len(self.offs)
        me = flat(own_place(self.axes), self.axes, self.sizes)
        self.started[count].wait_recv()
        self.out[...] = self.source[me, self.side].astype(F32) + self.first[count].astype(F32)
        for t in range(count):
            self.started[count + 1 + t].wait_recv()
            self.out[...] += self.last[t].astype(F32)
        for copy in self.started:
            copy.wait_send()


def scatter_kernel(specs, *refs):
    count = len(specs)
    scatters = [
        Scatter(*spec, refs[n], refs[count + n], *refs[2 * count + 5 * n : 2 * count + 5 * n + 5])
        for n, spec in enumerate(specs)
    ]
    greet([peer for s in scatters for peer in s.peers()])
    for s in scatters:
        s.start()
    for s in scatters:
        s.add()
    for s in scatters:
        s.finish()


def scatter(partials, specs, ident):
    scratch = []
    for partial in partials:
        group, block = partial.shape[0], partial.shape[2:]
        scratch += [
            pltpu.VMEM((group,) + block, BF16),
            pltpu.VMEM((group - 1,) + block, BF16),
            pltpu.VMEM((group - 1,) + block, BF16),
            pltpu.SemaphoreType.DMA((2 * group,)),
            pltpu.SemaphoreType.DMA((2 * group,)),
        ]
    return pl.pallas_call(
        functools.partial(scatter_kernel, specs),
        out_shape=[jax.ShapeDtypeStruct(p.shape[2:], F32) for p in partials],
        in_specs=[VMEM] * len(partials),
        out_specs=[VMEM] * len(partials),
        scratch_shapes=scratch,
        name="scatter%d" % ident,
        compiler_params=pltpu.CompilerParams(collective_id=ident, has_side_effects=True),
        cost_estimate=sent_estimate(sum(p.size for p in partials)),
    )(*partials)


def last_kernel(
    axes, sizes, spots, heads, share, source, blocks, out, routed, came, send, recv, hop, land
):
    offs = offsets(sizes)
    greet([moved(axes, sizes, o) for o in offs])
    me = flat(own_place(axes), axes, sizes)
    count = len(offs)
    started = []
    for t, off in enumerate(offs):
        peer = moved(axes, sizes, off)
        copy = remote(
            source.at[flat(peer, axes, sizes)], came.at[t], send.at[t], recv.at[t], peer
        )
        copy.start()
        started.append(copy)

    ctx_axes, ctx_sizes = axes[:3], sizes[:3]
    place = flat(own_place(ctx_axes), ctx_axes, ctx_sizes)

    def where(spot):
        return {
            ctx_axes[0]: spot // (ctx_sizes[1] * ctx_sizes[2]),
            ctx_axes[1]: (spot // ctx_sizes[2]) % ctx_sizes[1],
            ctx_axes[2]: spot % ctx_sizes[2],
        }

    def each_sent(act):
        for part in range(3):
            for h in range(heads):
                head = place * heads + h
                block = part * HEADS + head
                low = (block * HEAD_DIM) // share
                high = (block * HEAD_DIM + HEAD_DIM - 1) // share
                index = part * heads + h
                for which, owner, needed in (
                    (0, low, head < HEADS),
                    (1, high, (head < HEADS) & (high != low)),
                ):

                    @pl.when(needed)
                    def _(which=which, owner=owner, block=block, index=index):
                        act(index, 2 * index + which, owner, block - (share * owner) // HEAD_DIM)

    def send_block(index, slot, owner, target):
        @pl.when(owner != place)
        def _():
            remote(
                blocks.at[index], routed.at[target], hop.at[slot], land.at[target], where(owner)
            ).start()

        @pl.when(owner == place)
        def _():
            routed[target] = blocks[index]

    def sent_block(index, slot, owner, target):
        @pl.when(owner != place)
        def _():
            remote(
                blocks.at[index], routed.at[target], hop.at[slot], land.at[target], where(owner)
            ).wait_send()

    each_sent(send_block)
    for copy in started:
        copy.wait_recv()
    out[me] = source[me] + jnp.sum(came[...], axis=0)
    second = []
    for t, off in enumerate(offs):
        peer = moved(axes, sizes, off)
        copy = remote(out.at[me], out.at[me], send.at[count + t], recv.at[count + t], peer)
        copy.start()
        second.append(copy)

    base = (share * place) // HEAD_DIM
    for slot in range(routed.shape[0]):
        block = base + slot
        owner = (block % HEADS) // heads

        @pl.when((block * HEAD_DIM < share * (place + 1)) & (owner != place))
        def _(slot=slot):
            remote(
                blocks.at[0], routed.at[slot], hop.at[0], land.at[slot], where(place)
            ).wait_recv()

    each_sent(sent_block)
    for t, off in enumerate(offs):
        peer = moved(axes, sizes, off, -1)
        block = out.at[flat(peer, axes, sizes)]
        remote(block, block, send.at[count + t], recv.at[count + t], peer).wait_recv()
    for copy in started + second:
        copy.wait_send()


def last_exchange(parts, blocks, axes, sizes, spots, heads, share, ident):
    group = parts.shape[0]
    slots = max(
        (share * (c + 1) - 1) // HEAD_DIM - (share * c) // HEAD_DIM + 1 for c in range(spots)
    )
    return pl.pallas_call(
        functools.partial(last_kernel, axes, sizes, spots, heads, share),
        out_shape=[
            jax.ShapeDtypeStruct(parts.shape, F32),
            jax.ShapeDtypeStruct((slots,) + blocks.shape[1:], BF16),
        ],
        in_specs=[VMEM, VMEM],
        out_specs=[VMEM, VMEM],
        scratch_shapes=[
            pltpu.VMEM((group - 1,) + parts.shape[1:], F32),
            pltpu.SemaphoreType.DMA((2 * group,)),
            pltpu.SemaphoreType.DMA((2 * group,)),
            pltpu.SemaphoreType.DMA((6 * heads,)),
            pltpu.SemaphoreType.DMA((slots,)),
        ],
        name="last%d" % ident,
        compiler_params=pltpu.CompilerParams(collective_id=ident, has_side_effects=True),
    )(parts, blocks)


def nt(left, right):
    return lax.dot_general(left, right, (((1,), (1,)), ((), ())), preferred_element_type=F32)


def nn(left, right):
    return lax.dot_general(left, right, (((1,), (0,)), ((), ())), preferred_element_type=F32)


def rows_of(inv, ref, pair, low, high):
    first = pl.multiple_of(inv[2 * pair] * HEAD_DIM, HEAD_DIM)
    second = pl.multiple_of(inv[2 * pair + 1] * HEAD_DIM, HEAD_DIM)
    return jnp.concatenate(
        [ref[pl.ds(first, 64), low:high], ref[pl.ds(second, 64), low:high]], axis=0
    )


def put_rows(inv, ref, pair, low, high, values):
    first = pl.multiple_of(inv[2 * pair] * HEAD_DIM, HEAD_DIM)
    second = pl.multiple_of(inv[2 * pair + 1] * HEAD_DIM, HEAD_DIM)
    ref[pl.ds(first, 64), low:high] = values[:64]
    ref[pl.ds(second, 64), low:high] = values[64:]


def head_slice(values, part, heads, head):
    low = (part * heads + head) * HEAD_DIM
    return values[:, low : low + HEAD_DIM]


def diagonal(block):
    return lax.broadcasted_iota(jnp.int32, (block, block), 0) <= lax.broadcasted_iota(
        jnp.int32, (block, block), 1
    )


def attend_kernel(heads, block, inv, qkv, out, out_low, lse, qs, ks, vt, ot):
    length = qkv.shape[0]
    width = heads * HEAD_DIM

    def sort(pair, unused):
        at = pl.multiple_of(pair * 128, 128)
        values = rows_of(inv, qkv, pair, 0, 3 * width)
        for h in range(heads):
            qs[h, pl.ds(at, 128), :] = head_slice(values, 0, heads, h) * BF16(0.125)
            ks[h, pl.ds(at, 128), :] = head_slice(values, 1, heads, h)
            vt[h, :, pl.ds(at, 128)] = head_slice(values, 2, heads, h).astype(F32).T.astype(BF16)
        return unused

    lax.fori_loop(0, length // 128, sort, 0)
    allowed = diagonal(block)

    def row(qi, unused):
        q_at = pl.multiple_of(qi * block, block)

        def first(h):
            scores = nt(ks[h, pl.ds(q_at, block), :], qs[h, pl.ds(q_at, block), :])
            scores = jnp.where(allowed, scores, -1e30)
            high = jnp.max(scores, axis=0, keepdims=True)
            probs = jnp.exp(scores - high)
            return (
                high,
                jnp.sum(probs, axis=0, keepdims=True),
                nn(vt[h, :, pl.ds(q_at, block)], probs.astype(BF16)),
            )

        def column(kj, state):
            k_at = pl.multiple_of(kj * block, block)
            fresh_state = []
            for h in range(heads):
                high, weight, acc = state[h]
                scores = nt(ks[h, pl.ds(k_at, block), :], qs[h, pl.ds(q_at, block), :])
                fresh = jnp.maximum(high, jnp.max(scores, axis=0, keepdims=True))
                probs = jnp.exp(scores - fresh)
                fade = jnp.exp(high - fresh)
                fresh_state.append(
                    (
                        fresh,
                        weight * fade + jnp.sum(probs, axis=0, keepdims=True),
                        acc * fade + nn(vt[h, :, pl.ds(k_at, block)], probs.astype(BF16)),
                    )
                )
            return tuple(fresh_state)

        state = lax.fori_loop(0, qi, column, tuple(first(h) for h in range(heads)))
        for h in range(heads):
            high, weight, acc = state[h]
            ot[h, :, pl.ds(q_at, block)] = acc / weight
            lse[h : h + 1, pl.ds(q_at, block)] = high + jnp.log(weight)
        return unused

    lax.fori_loop(0, length // block, row, 0)

    def unsort(pair, unused):
        at = pl.multiple_of(pair * 128, 128)
        values = [ot[h, :, pl.ds(at, 128)].T for h in range(heads)]
        values = jnp.concatenate(values, axis=1)
        put_rows(inv, out, pair, 0, width, values)
        put_rows(inv, out_low, pair, 0, width, values.astype(BF16))
        return unused

    lax.fori_loop(0, length // 128, unsort, 0)


def attend(inv, qkv, heads):
    length = qkv.shape[0]
    width = heads * HEAD_DIM
    block = min(256, length)
    pairs = length * (length + block) // 2
    return pl.pallas_call(
        functools.partial(attend_kernel, heads, block),
        out_shape=(
            jax.ShapeDtypeStruct((length, width), F32),
            jax.ShapeDtypeStruct((length, width), BF16),
            jax.ShapeDtypeStruct((heads, length), F32),
        ),
        grid_spec=pltpu.PrefetchScalarGridSpec(
            num_scalar_prefetch=1,
            grid=(1,),
            in_specs=[pl.BlockSpec((length, 3 * width), lambda i, inv: (0, 0))],
            out_specs=(
                pl.BlockSpec((length, width), lambda i, inv: (0, 0)),
                pl.BlockSpec((length, width), lambda i, inv: (0, 0)),
                pl.BlockSpec((heads, length), lambda i, inv: (0, 0)),
            ),
            scratch_shapes=[
                pltpu.VMEM((heads, length, HEAD_DIM), BF16),
                pltpu.VMEM((heads, length, HEAD_DIM), BF16),
                pltpu.VMEM((heads, HEAD_DIM, length), BF16),
                pltpu.VMEM((heads, HEAD_DIM, length), F32),
            ],
        ),
        name="attend",
        cost_estimate=pl.CostEstimate(
            flops=4 * heads * pairs * HEAD_DIM * 4,
            bytes_accessed=length * width * 10,
            transcendentals=heads * pairs,
        ),
    )(inv, qkv)


def attend_back_kernel(
    heads, block, inv, qkv, grads, outs, lse, dqkv, qs, ks, vs, gs, kt, delta, dqt, dks, dvs
):
    length = qkv.shape[0]
    width = heads * HEAD_DIM
    count = length // block

    def sort(pair, unused):
        at = pl.multiple_of(pair * 128, 128)
        values = rows_of(inv, qkv, pair, 0, 3 * width)
        grad = rows_of(inv, grads, pair, 0, width)
        value = rows_of(inv, outs, pair, 0, width)
        product = (grad.astype(F32) * value).T
        for h in range(heads):
            qs[h, pl.ds(at, 128), :] = head_slice(values, 0, heads, h) * BF16(0.125)
            key = head_slice(values, 1, heads, h)
            ks[h, pl.ds(at, 128), :] = key
            kt[h, :, pl.ds(at, 128)] = key.astype(F32).T.astype(BF16)
            vs[h, pl.ds(at, 128), :] = head_slice(values, 2, heads, h)
            gs[h, pl.ds(at, 128), :] = head_slice(grad, 0, heads, h)
            delta[h : h + 1, pl.ds(at, 128)] = jnp.sum(
                product[h * HEAD_DIM : (h + 1) * HEAD_DIM], axis=0, keepdims=True
            )
            dqt[h, :, pl.ds(at, 128)] = jnp.zeros((HEAD_DIM, 128), F32)
        return unused

    lax.fori_loop(0, length // 128, sort, 0)
    allowed = diagonal(block)

    def column(kj, unused):
        k_at = pl.multiple_of(kj * block, block)

        def tile(h, q_at, masked):
            q = qs[h, pl.ds(q_at, block), :]
            g = gs[h, pl.ds(q_at, block), :]
            scores = nt(ks[h, pl.ds(k_at, block), :], q)
            probs = jnp.exp(scores - lse[h : h + 1, pl.ds(q_at, block)])
            if masked:
                probs = jnp.where(allowed, probs, 0.0)
            slopes = nt(vs[h, pl.ds(k_at, block), :], g)
            low = (probs * (slopes - delta[h : h + 1, pl.ds(q_at, block)])).astype(BF16)
            dqt[h, :, pl.ds(q_at, block)] += nn(kt[h, :, pl.ds(k_at, block)], low)
            return nn(low, q), nn(probs.astype(BF16), g)

        def row(qi, state):
            q_at = pl.multiple_of(qi * block, block)
            fresh = []
            for h in range(heads):
                dk, dv = tile(h, q_at, False)
                fresh.append((state[h][0] + dk, state[h][1] + dv))
            return tuple(fresh)

        state = tuple(tile(h, k_at, True) for h in range(heads))
        state = lax.fori_loop(kj + 1, count, row, state)
        for h in range(heads):
            dks[h, pl.ds(k_at, block), :] = state[h][0].astype(BF16)
            dvs[h, pl.ds(k_at, block), :] = state[h][1].astype(BF16)
        return unused

    lax.fori_loop(0, count, column, 0)

    def unsort(pair, unused):
        at = pl.multiple_of(pair * 128, 128)
        values = [(dqt[h, :, pl.ds(at, 128)].T * 0.125).astype(BF16) for h in range(heads)]
        values += [dks[h, pl.ds(at, 128), :] for h in range(heads)]
        values += [dvs[h, pl.ds(at, 128), :] for h in range(heads)]
        put_rows(inv, dqkv, pair, 0, 3 * width, jnp.concatenate(values, axis=1))
        return unused

    lax.fori_loop(0, length // 128, unsort, 0)


def attend_back(inv, qkv, grads, outs, lse, heads):
    length = qkv.shape[0]
    width = heads * HEAD_DIM
    block = min(256, length)
    pairs = length * (length + block) // 2
    row_shape = (heads, length, HEAD_DIM)
    return pl.pallas_call(
        functools.partial(attend_back_kernel, heads, block),
        out_shape=jax.ShapeDtypeStruct((length, 3 * width), BF16),
        grid_spec=pltpu.PrefetchScalarGridSpec(
            num_scalar_prefetch=1,
            grid=(1,),
            in_specs=[
                pl.BlockSpec((length, 3 * width), lambda i, inv: (0, 0)),
                pl.BlockSpec((length, width), lambda i, inv: (0, 0)),
                pl.BlockSpec((length, width), lambda i, inv: (0, 0)),
                pl.BlockSpec((heads, length), lambda i, inv: (0, 0)),
            ],
            out_specs=pl.BlockSpec((length, 3 * width), lambda i, inv: (0, 0)),
            scratch_shapes=[
                pltpu.VMEM(row_shape, BF16),
                pltpu.VMEM(row_shape, BF16),
                pltpu.VMEM(row_shape, BF16),
                pltpu.VMEM(row_shape, BF16),
                pltpu.VMEM((heads, HEAD_DIM, length), BF16),
                pltpu.VMEM((heads, length), F32),
                pltpu.VMEM((heads, HEAD_DIM, length), F32),
                pltpu.VMEM(row_shape, BF16),
                pltpu.VMEM(row_shape, BF16),
            ],
        ),
        name="attend_back",
        cost_estimate=pl.CostEstimate(
            flops=10 * heads * pairs * HEAD_DIM * 4,
            bytes_accessed=length * width * 20,
            transcendentals=heads * pairs,
        ),
    )(inv, qkv, grads, outs, lse)


def layer_norm(values, gain, shift):
    center = jnp.mean(values, axis=-1, keepdims=True)
    centred = values - center
    spread = jnp.mean(centred * centred, axis=-1, keepdims=True)
    return centred * lax.rsqrt(spread + EPSILON) * gain + shift


def smooth_gelu(values):
    return (
        0.5
        * values
        * (1.0 + jnp.tanh(0.7978845608028654 * (values + 0.044715 * values * values * values)))
    )


def matmul(left, right):
    return jnp.dot(left, right, preferred_element_type=F32)


def against(left, weight):
    return lax.dot_general(left, weight, (((1,), (1,)), ((), ())), preferred_element_type=F32)


def onto(left, right):
    return lax.dot_general(left, right, (((0,), (0,)), ((), ())), preferred_element_type=F32)


def body(
    sizes,
    tokens,
    block_order,
    qkv_weight,
    query_bias,
    value_bias,
    out_weight,
    out_bias,
    expand_weight,
    expand_bias,
    shrink_weight,
    shrink_bias,
    first_gain,
    first_shift,
    second_gain,
    second_shift,
    cotangent,
):
    outer, inner, ys, xs, ks = (sizes[a] for a in ("o", "i", "y", "x", "k"))
    spots = outer * inner * ys
    shards = xs * ks
    rows, width = tokens.shape[1:]
    o, i, y = lax.axis_index("o"), lax.axis_index("i"), lax.axis_index("y")
    shard = lax.axis_index("x") * ks + lax.axis_index("k")
    place = (o * inner + i) * ys + y
    heads = -(-HEADS // spots)
    span = heads * HEAD_DIM
    padded = spots * span
    part = qkv_weight.shape[0]
    hidden = expand_weight.shape[1]
    piece = hidden // (shards * inner)
    every = (("o", "i", "y"), (outer, inner, ys))
    ctx = (("o", "i"), (outer, inner), "y")
    group = (("i", "x"), (inner, xs), "k")
    pair = (("x",), (xs,), "k")
    own = tokens[0]
    own_grad = cotangent[0]

    def columns(values, count):
        wide = values.reshape(values.shape[:-1] + (count, width))
        wide = jnp.pad(wide, [(0, 0)] * (wide.ndim - 1) + [(0, padded - width)])
        return lax.dynamic_slice_in_dim(wide, place * span, span, axis=wide.ndim - 1)

    qkv_own = columns(qkv_weight, 3).reshape(part, 3 * span)
    qkv_bias = jnp.concatenate(
        [columns(query_bias, 1)[0], jnp.zeros((span,), F32), columns(value_bias, 1)[0]]
    )
    gathered, qkv_columns, expand_columns = first_gather(
        own, qkv_own, expand_weight, [ctx, pair], (xs, ks), piece, 0
    )
    sequence = gathered.reshape(spots * rows, width)
    qkv_columns = qkv_columns.reshape(width, 3 * span)
    expand_columns = expand_columns.reshape(width, piece)

    out_own = lax.optimization_barrier((out_weight, gathered[0, 0, :8, :128]))[0]
    x_swap, k_swap, y_swap = ([(0, 1), (1, 0)],) * 3
    out_pair = jnp.stack([out_own, lax.ppermute(out_own, "x", x_swap)])
    out_mate = lax.ppermute(out_pair, "k", k_swap)
    shrink_rows = lax.dynamic_slice_in_dim(shrink_weight, i * piece, piece, axis=0)
    expand_own_bias = lax.dynamic_slice_in_dim(
        expand_bias, (shard * inner + i) * piece, piece, axis=0
    )

    order_row = block_order[0]
    blocks = order_row.shape[0]
    inv = jnp.sum(
        jnp.where(
            order_row[:, None] == jnp.arange(blocks, dtype=jnp.int32)[None, :],
            jnp.arange(blocks, dtype=jnp.int32)[:, None],
            0,
        ),
        axis=0,
    ).astype(jnp.int32)
    normed_low = layer_norm(sequence.astype(F32), first_gain, first_shift).astype(BF16)
    qkv = (matmul(normed_low, qkv_columns) + qkv_bias).astype(BF16)
    attended, attended_bf, log_sum = attend(inv, qkv, heads)
    attended_low, group_grad = to_tokens(
        attended_bf.reshape(spots, rows, span), own_grad, width, *every, group, 1
    )
    group_grad = group_grad.reshape(-1, width)

    out_parts = [out_pair[0], out_mate[0], out_pair[1], out_mate[1]]
    out_spots = [shard, shard ^ 1, shard ^ 2, shard ^ 3]

    def out_project(low):
        terms = [
            matmul(lax.dynamic_slice_in_dim(low, spot * part, part, axis=1), weight)
            for spot, weight in zip(out_spots, out_parts)
        ]
        return terms[0] + terms[1] + terms[2] + terms[3]

    inputs = own.astype(F32)
    middle = inputs + out_project(attended_low) + out_bias
    lowered_two = layer_norm(middle, second_gain, second_shift).astype(BF16)

    (group_low,) = gather([lowered_two], [group], 2)
    group_low = group_low.reshape(-1, width)
    expanded = matmul(group_low, expand_columns) + expand_own_bias
    hidden_low = smooth_gelu(expanded).astype(BF16)
    grad_hidden = against(group_grad, shrink_rows)
    unused, gelu_back = jax.vjp(smooth_gelu, expanded)
    (grad_expanded,) = gelu_back(grad_hidden)
    expanded_low = grad_expanded.astype(BF16)
    grad_partial = against(expanded_low, expand_columns).astype(BF16)
    shape = (inner * xs, ks, rows, width)
    (grad_normed_two,) = scatter([grad_partial.reshape(shape)], [group], 3)

    grad_result = own_grad.astype(F32)
    unused, second_back = jax.vjp(layer_norm, middle, second_gain, second_shift)
    grad_middle_norm, grad_second_gain, grad_second_shift = second_back(grad_normed_two)
    grad_middle = grad_result + grad_middle_norm
    middle_low = grad_middle.astype(BF16)
    turned = jnp.stack([against(middle_low, weight) for weight in out_parts])
    turned = turned.reshape(2, 2, rows, part)
    turned = jnp.where(lax.axis_index("x") == 0, turned, turned[::-1])
    turned = jnp.where(lax.axis_index("k") == 0, turned, turned[:, ::-1])
    grad_att_low = turned.reshape(shards, rows, part).transpose(1, 0, 2).reshape(rows, width)
    grad_att_low = grad_att_low.astype(BF16)
    grad_heads, middle_group, att_group = to_heads(
        grad_att_low,
        middle_low,
        attended_low,
        span,
        *every,
        group,
        ("i", "x", "k"),
        (inner, xs, ks),
        4,
    )
    grad_heads = grad_heads.reshape(spots * rows, span)
    middle_group = middle_group.reshape(-1, width)
    att_group = att_group.reshape(middle_group.shape[0], -1)

    dqkv = attend_back(inv, qkv, grad_heads, attended, log_sum, heads)
    norm_partial = against(dqkv, qkv_columns).astype(BF16)
    qkv_partial = onto(normed_low, dqkv).astype(BF16)
    result_partial = matmul(hidden_low, shrink_rows).astype(BF16)
    grad_normed_one, qkv_cells, shrunk = scatter(
        [
            norm_partial.reshape(outer * inner, ys, rows, width),
            qkv_partial.reshape(xs, ks, part, 3 * span),
            result_partial.reshape(shape),
        ],
        [ctx, pair, group],
        5,
    )
    result = middle + shrunk + shrink_bias
    unused, first_back = jax.vjp(layer_norm, inputs, first_gain, first_shift)
    grad_first_input, grad_first_gain, grad_first_shift = first_back(grad_normed_one)
    grad_inputs = grad_middle + grad_first_input

    def kept_and_sent(values, axis_name, dim):
        index = lax.axis_index(axis_name)
        size = sizes[axis_name]
        kept = lax.dynamic_index_in_dim(values, index, axis=dim, keepdims=False)
        total = kept.astype(F32)
        for step in range(1, size):
            sent = lax.dynamic_index_in_dim(
                values, lax.rem(index + step, size), axis=dim, keepdims=False
            )
            ring = [(d, (d + step) % size) for d in range(size)]
            total = total + lax.ppermute(sent, axis_name, ring).astype(F32)
        return total.astype(BF16)

    def swapped(values, axis_name):
        index = lax.axis_index(axis_name)
        kept = lax.dynamic_index_in_dim(values, index, axis=0, keepdims=False)
        sent = lax.dynamic_index_in_dim(values, 1 - index, axis=0, keepdims=False)
        came = lax.ppermute(sent, axis_name, [(0, 1), (1, 0)])
        return jnp.where(index == 0, jnp.stack([kept, came]), jnp.stack([came, kept]))

    def owned(left, right):
        cell = width // spots
        local = onto(left, right).astype(BF16)
        local = local.reshape(outer, inner, ys, cell, right.shape[1])
        local = kept_and_sent(local, "y", 2)
        local = kept_and_sent(local, "o", 0)
        local = swapped(local, "i")
        return local.transpose(0, 2, 1).reshape(inner * right.shape[1], cell).astype(F32)

    grad_shrink = owned(group_grad, hidden_low)
    grad_outw = owned(middle_group, att_group)

    cuts = spots // (2 * shards)
    local = onto(group_low, expanded_low).astype(BF16)
    local = local.reshape(shards, part, cuts, piece // cuts).transpose(0, 2, 1, 3)
    local = local.reshape(outer, ys, part, piece // cuts)
    local = kept_and_sent(kept_and_sent(local, "y", 1), "o", 0)
    axes = ("o", "i", "y", "x", "k")
    routes = []
    for so, si, sy, sf in itertools.product(*map(range, (outer, inner, ys, shards))):
        index = so * ys + sy
        spot = sf * (spots // shards) + si * cuts + index % cuts
        routes.append((((so * inner + si) * ys + sy) * shards + sf, spot * shards + index // cuts))
    grad_expand = lax.ppermute(local, axes, routes).astype(F32)

    def placed(values, start, size):
        return lax.dynamic_update_slice_in_dim(jnp.zeros((size,), F32), values, start, axis=0)

    dqkv_sums = jnp.sum(dqkv.astype(F32), axis=0)
    small = [
        placed(dqkv_sums[:span], place * span, padded),
        placed(dqkv_sums[2 * span :], place * span, padded),
        jnp.sum(middle_low.astype(F32), axis=0),
        placed(
            jnp.sum(expanded_low.astype(F32), axis=0), (shard * inner + i) * piece, hidden
        ),
        jnp.sum(grad_result, axis=0),
        grad_first_gain,
        grad_first_shift,
        grad_second_gain,
        grad_second_shift,
    ]
    lengths = [s.shape[0] for s in small]
    devices = spots * shards
    lanes = 128 * (-(-sum(lengths) // (devices * 1024)))
    line = jnp.concatenate(small)
    line = jnp.pad(line, (0, devices * 8 * lanes - line.shape[0])).reshape(devices, 8, lanes)
    share = 3 * width // spots
    qkv_blocks = qkv_cells.astype(BF16).T.reshape(3 * heads, HEAD_DIM, part)
    line, routed = last_exchange(
        line, qkv_blocks, axes, (outer, inner, ys, xs, ks), spots, heads, share, 6
    )
    line = line.reshape(-1)
    start = share * place - HEAD_DIM * ((share * place) // HEAD_DIM)
    grad_qkv = lax.dynamic_slice_in_dim(routed.reshape(-1, part), start, share, axis=0)
    grad_qkv = grad_qkv.T.astype(F32)
    summed = []
    start = 0
    for length in lengths:
        summed.append(line[start : start + length])
        start += length
    summed[0] = summed[0][:width]
    summed[1] = summed[1][:width]
    return (
        result.astype(BF16)[None],
        grad_inputs[None],
        grad_qkv,
        grad_outw,
        grad_expand,
        grad_shrink,
        *summed,
    )


def solution(mesh):
    spots, shards = mesh.shape["ctx"], mesh.shape["fsdp"]
    sizes = {"o": spots // 4, "i": 2, "y": 2, "x": shards // 2, "k": 2}
    fine = Mesh(mesh.devices.reshape(tuple(sizes.values())), tuple(sizes))
    seq, pos = ("x", "k"), ("o", "i", "y")
    weight = P(seq, None)
    placed = (
        P(seq, pos, None),
        P(seq, None),
        weight,
        P(),
        P(),
        weight,
        P(),
        weight,
        P(),
        weight,
        P(),
        P(),
        P(),
        P(),
        P(),
        P(seq, pos, None),
    )
    given = (P(seq, pos, None),) * 2 + (P(seq, pos),) * 4 + (P(),) * 9
    return jax.shard_map(
        functools.partial(body, sizes),
        mesh=fine,
        in_specs=placed,
        out_specs=given,
        check_vma=False,
    )
```

```python
import functools
import itertools

import jax
import jax.numpy as jnp
from jax import lax
from jax.experimental import pallas as pl
from jax.experimental.pallas import tpu as pltpu
from jax.sharding import Mesh
from jax.sharding import PartitionSpec as P

HEADS = 25
HEAD_DIM = 64
EPSILON = 1e-05
MESH = pl.DeviceIdType.MESH
F32 = jnp.float32
BF16 = jnp.bfloat16
ANY = pl.BlockSpec(memory_space=pl.ANY)
VMEM = pl.BlockSpec(memory_space=pltpu.VMEM)


def offsets(sizes):
    return [o for o in itertools.product(*(range(s) for s in sizes)) if any(o)]


def moved(axes, sizes, offset, sign=1):
    return {
        a: lax.rem(lax.axis_index(a) + (o if sign > 0 else s - o), s)
        for a, s, o in zip(axes, sizes, offset)
    }


def flat(place, axes, sizes):
    index = 0
    for a, s in zip(axes, sizes):
        index = index * s + place[a]
    return index


def own_place(axes):
    return {a: lax.axis_index(a) for a in axes}


def greet(peers):
    barrier = pltpu.get_barrier_semaphore()
    for peer in peers:
        pl.semaphore_signal(barrier, inc=1, device_id=peer, device_id_type=MESH)
    pl.semaphore_wait(barrier, len(peers))


def remote(src, dst, send, recv, peer):
    return pltpu.make_async_remote_copy(
        src_ref=src,
        dst_ref=dst,
        send_sem=send,
        recv_sem=recv,
        device_id=peer,
        device_id_type=MESH,
    )


class Gather:
    def __init__(self, axes, sizes, pair, source, out, send, recv, local):
        self.axes, self.sizes = axes, sizes
        self.offs = offsets(sizes)
        self.side = lax.axis_index(pair)
        self.mate = {pair: 1 - self.side}
        self.source, self.out, self.send, self.recv, self.local = source, out, send, recv, local
        self.started = []

    def peers(self):
        return [moved(self.axes, self.sizes, o) for o in self.offs] + [self.mate]

    def mine(self):
        return self.out.at[flat(own_place(self.axes), self.axes, self.sizes), self.side]

    def start(self):
        pltpu.make_async_copy(self.source, self.mine(), self.local).start()
        last = len(self.offs)
        for t, peer in enumerate(self.peers()):
            copy = remote(self.source, self.mine(), self.send.at[t], self.recv.at[t], peer)
            copy.start()
            self.started.append(copy)

    def hand_on(self):
        last = len(self.offs)
        for t, off in enumerate(self.offs):
            came = flat(moved(self.axes, self.sizes, off, -1), self.axes, self.sizes)
            block = self.out.at[came, self.side]
            remote(self.source, block, self.send.at[t], self.recv.at[t], self.mate).wait_recv()
            slot = last + 1 + t
            copy = remote(block, block, self.send.at[slot], self.recv.at[slot], self.mate)
            copy.start()
            self.started.append(copy)

    def finish(self):
        last = len(self.offs)
        me = flat(own_place(self.axes), self.axes, self.sizes)
        pltpu.make_async_copy(self.source, self.mine(), self.local).wait()
        block = self.out.at[me, 1 - self.side]
        remote(self.source, block, self.send.at[last], self.recv.at[last], self.mate).wait_recv()
        for t, off in enumerate(self.offs):
            came = flat(moved(self.axes, self.sizes, off, -1), self.axes, self.sizes)
            slot = last + 1 + t
            block = self.out.at[came, 1 - self.side]
            remote(
                self.source, block, self.send.at[slot], self.recv.at[slot], self.mate
            ).wait_recv()
        for copy in self.started:
            copy.wait_send()


def gather_shape(block, spec):
    group = 1
    for s in spec[1]:
        group *= s
    return jax.ShapeDtypeStruct((group, 2) + block.shape, block.dtype)


def gather_scratch(spec):
    group = 1
    for s in spec[1]:
        group *= s
    return [
        pltpu.SemaphoreType.DMA((2 * group,)),
        pltpu.SemaphoreType.DMA((2 * group,)),
        pltpu.SemaphoreType.DMA,
    ]


def sent_estimate(size):
    return pl.CostEstimate(flops=0, bytes_accessed=20 * size, transcendentals=0)


def gather_kernel(specs, *refs):
    count = len(specs)
    gathers = [
        Gather(*spec, refs[n], refs[count + n], *refs[2 * count + 3 * n : 2 * count + 3 * n + 3])
        for n, spec in enumerate(specs)
    ]
    greet([peer for g in gathers for peer in g.peers()])
    for g in gathers:
        g.start()
    for g in gathers:
        g.hand_on()
    for g in gathers:
        g.finish()


def gather(blocks, specs, ident):
    shapes = [gather_shape(block, spec) for block, spec in zip(blocks, specs)]
    return pl.pallas_call(
        functools.partial(gather_kernel, specs),
        out_shape=shapes,
        in_specs=[VMEM] * len(blocks),
        out_specs=[ANY] * len(blocks),
        scratch_shapes=[s for spec in specs for s in gather_scratch(spec)],
        name="gather%d" % ident,
        compiler_params=pltpu.CompilerParams(collective_id=ident, has_side_effects=True),
        cost_estimate=sent_estimate(sum(s.size for s in shapes)),
    )(*blocks)


def first_kernel(
    specs,
    shard_sizes,
    ctx_axes,
    ctx_sizes,
    own,
    qkv_weight,
    weight,
    all_tokens,
    all_columns,
    pieces,
    qkv_whole,
    columns,
    whole,
    cut,
    *sems,
):
    axes = ("x", "k")
    offs = offsets(shard_sizes)
    tokens = Gather(*specs[0], own, all_tokens, *sems[0:3])
    heads = Gather(*specs[1], columns, all_columns, *sems[3:6])
    read, qkv_read, send, recv, local = sems[6:11]
    qkv_fetch = pltpu.make_async_copy(qkv_weight, qkv_whole, qkv_read)
    qkv_fetch.start()
    fetch = pltpu.make_async_copy(weight, whole, read)
    fetch.start()
    greet(tokens.peers() + heads.peers() + [moved(axes, shard_sizes, o) for o in offs])
    tokens.start()
    qkv_fetch.wait()
    place = flat(own_place(ctx_axes), ctx_axes, ctx_sizes)
    rows, span = columns.shape[0], columns.shape[1] // 3
    width = qkv_whole.shape[1] // 3
    for spot in range(-(-width // span)):

        @pl.when(place == spot)
        def _(spot=spot):
            size = min(span, width - spot * span)
            for section in range(3):
                low = section * width + spot * span
                if size < span:
                    columns[:, section * span : (section + 1) * span] = jnp.zeros(
                        (rows, span), BF16
                    )
                columns[:, section * span : section * span + size] = qkv_whole[:, low : low + size]

    @pl.when(place * span >= width)
    def _():
        columns[...] = jnp.zeros(columns.shape, BF16)

    heads.start()
    fetch.wait()
    width = cut.shape[2]
    inner = lax.axis_index("i")
    for half in range(2):

        @pl.when(inner == half)
        def _():
            for f in range(cut.shape[0]):
                low = (2 * f + half) * width
                cut[f] = whole[:, low : low + width]

    me = flat(own_place(axes), axes, shard_sizes)
    here = pltpu.make_async_copy(cut.at[me], pieces.at[me], local)
    here.start()
    started = []
    for t, off in enumerate(offs):
        peer = moved(axes, shard_sizes, off)
        there = flat(peer, axes, shard_sizes)
        copy = remote(cut.at[there], pieces.at[me], send.at[t], recv.at[t], peer)
        copy.start()
        started.append(copy)
    heads.hand_on()
    tokens.hand_on()
    here.wait()
    for t, off in enumerate(offs):
        peer = moved(axes, shard_sizes, off, -1)
        came = flat(peer, axes, shard_sizes)
        remote(cut.at[came], pieces.at[came], send.at[t], recv.at[t], peer).wait_recv()
    for copy in started:
        copy.wait_send()
    heads.finish()
    tokens.finish()


def first_gather(own, qkv_weight, weight, span, specs, shard_sizes, every, piece, ident):
    shards = shard_sizes[0] * shard_sizes[1]
    part = weight.shape[0]
    columns = jax.ShapeDtypeStruct((part, 3 * span), BF16)
    shapes = [
        gather_shape(own, specs[0]),
        gather_shape(columns, specs[1]),
        jax.ShapeDtypeStruct((shards, part, piece), BF16),
    ]
    return pl.pallas_call(
        functools.partial(first_kernel, specs, shard_sizes, *every),
        out_shape=shapes,
        in_specs=[VMEM, ANY, ANY],
        out_specs=[ANY] * 3,
        scratch_shapes=[
            pltpu.VMEM(qkv_weight.shape, BF16),
            pltpu.VMEM(columns.shape, BF16),
            pltpu.VMEM(weight.shape, BF16),
            pltpu.VMEM((shards, part, piece), BF16),
            *gather_scratch(specs[0]),
            *gather_scratch(specs[1]),
            pltpu.SemaphoreType.DMA,
            pltpu.SemaphoreType.DMA,
            pltpu.SemaphoreType.DMA((shards,)),
            pltpu.SemaphoreType.DMA((shards,)),
            pltpu.SemaphoreType.DMA,
        ],
        name="first%d" % ident,
        compiler_params=pltpu.CompilerParams(collective_id=ident, has_side_effects=True),
        cost_estimate=sent_estimate(sum(s.size for s in shapes)),
    )(own, qkv_weight, weight)


def pieces_out(axes, sizes, source, out, send, recv):
    me = flat(own_place(axes), axes, sizes)
    started = []
    for t, off in enumerate(offsets(sizes)):
        peer = moved(axes, sizes, off)
        copy = remote(
            source.at[flat(peer, axes, sizes)], out.at[me], send.at[t], recv.at[t], peer
        )
        copy.start()
        started.append(copy)
    return started


def pieces_in(axes, sizes, source, out, send, recv, started):
    for t, off in enumerate(offsets(sizes)):
        peer = moved(axes, sizes, off, -1)
        came = flat(peer, axes, sizes)
        remote(source.at[came], out.at[came], send.at[t], recv.at[t], peer).wait_recv()
    for copy in started:
        copy.wait_send()


def to_tokens_kernel(axes, sizes, source, out, came, send, recv):
    greet([moved(axes, sizes, o) for o in offsets(sizes)])
    started = pieces_out(axes, sizes, source, came, send, recv)
    me = flat(own_place(axes), axes, sizes)
    came[me] = source[me]
    pieces_in(axes, sizes, source, came, send, recv, started)
    span, width = came.shape[2], out.shape[1]
    for d in range(came.shape[0]):
        low, high = d * span, min((d + 1) * span, width)
        if low < high:
            out[:, low:high] = came[d, :, : high - low]


def to_tokens(pieces, width, axes, sizes, ident):
    group, rows, span = pieces.shape
    return pl.pallas_call(
        functools.partial(to_tokens_kernel, axes, sizes),
        out_shape=jax.ShapeDtypeStruct((rows, width), pieces.dtype),
        in_specs=[VMEM],
        out_specs=VMEM,
        scratch_shapes=[
            pltpu.VMEM(pieces.shape, pieces.dtype),
            pltpu.SemaphoreType.DMA((group,)),
            pltpu.SemaphoreType.DMA((group,)),
        ],
        name="to_tokens%d" % ident,
        compiler_params=pltpu.CompilerParams(collective_id=ident, has_side_effects=True),
        cost_estimate=sent_estimate(3 * pieces.size),
    )(pieces)


def to_heads_kernel(
    axes,
    sizes,
    group_axes,
    group_sizes,
    source,
    att,
    out,
    att_out,
    cut,
    att_cut,
    send,
    recv,
    att_send,
    att_recv,
):
    greet(
        [moved(axes, sizes, o) for o in offsets(sizes)]
        + [moved(group_axes, group_sizes, o) for o in offsets(group_sizes)]
    )
    span, width = cut.shape[2], source.shape[1]
    for d in range(cut.shape[0]):
        low, high = d * span, min((d + 1) * span, width)
        if high - low < span:
            cut[d] = jnp.zeros(cut.shape[1:], cut.dtype)
        if low < high:
            cut[d, :, : high - low] = source[:, low:high]
    started = pieces_out(axes, sizes, cut, out, send, recv)
    cell = att_cut.shape[2]
    inner, shards = group_sizes[0], group_sizes[1] * group_sizes[2]
    for half in range(inner):
        for f in range(shards):
            low = (f * inner + half) * cell
            att_cut[half * shards + f] = att[:, low : low + cell]
    att_started = pieces_out(group_axes, group_sizes, att_cut, att_out, att_send, att_recv)
    me = flat(own_place(axes), axes, sizes)
    out[me] = cut[me]
    me = flat(own_place(group_axes), group_axes, group_sizes)
    att_out[me] = att_cut[me]
    pieces_in(axes, sizes, cut, out, send, recv, started)
    pieces_in(group_axes, group_sizes, att_cut, att_out, att_send, att_recv, att_started)


def to_heads(source, att, span, axes, sizes, group_axes, group_sizes, ident):
    rows, width = source.shape
    count, group = 1, 1
    for s in sizes:
        count *= s
    for s in group_sizes:
        group *= s
    cell = width // group
    return pl.pallas_call(
        functools.partial(to_heads_kernel, axes, sizes, group_axes, group_sizes),
        out_shape=[
            jax.ShapeDtypeStruct((count, rows, span), source.dtype),
            jax.ShapeDtypeStruct((group, rows, cell), att.dtype),
        ],
        in_specs=[VMEM, VMEM],
        out_specs=[VMEM, VMEM],
        scratch_shapes=[
            pltpu.VMEM((count, rows, span), source.dtype),
            pltpu.VMEM((group, rows, cell), att.dtype),
            pltpu.SemaphoreType.DMA((count,)),
            pltpu.SemaphoreType.DMA((count,)),
            pltpu.SemaphoreType.DMA((group,)),
            pltpu.SemaphoreType.DMA((group,)),
        ],
        name="to_heads%d" % ident,
        compiler_params=pltpu.CompilerParams(collective_id=ident, has_side_effects=True),
        cost_estimate=sent_estimate(3 * source.size),
    )(source, att)


class Scatter:
    def __init__(self, axes, sizes, pair, source, out, first, summed, last, send, recv):
        self.axes, self.sizes = axes, sizes
        self.offs = offsets(sizes)
        self.side = lax.axis_index(pair)
        self.mate = {pair: 1 - self.side}
        self.source, self.out = source, out
        self.first, self.summed, self.last = first, summed, last
        self.send, self.recv = send, recv
        self.started = []

    def peers(self):
        return [moved(self.axes, self.sizes, o) for o in self.offs] + [self.mate]

    def start(self):
        for t, off in enumerate(self.offs + [(0,) * len(self.sizes)]):
            there = flat(moved(self.axes, self.sizes, off), self.axes, self.sizes)
            copy = remote(
                self.source.at[there, 1 - self.side],
                self.first.at[t],
                self.send.at[t],
                self.recv.at[t],
                self.mate,
            )
            copy.start()
            self.started.append(copy)

    def add(self):
        count = len(self.offs)
        for t, off in enumerate(self.offs):
            peer = moved(self.axes, self.sizes, off)
            there = flat(peer, self.axes, self.sizes)
            self.started[t].wait_recv()
            self.summed[t] = (
                self.source[there, self.side].astype(F32) + self.first[t].astype(F32)
            ).astype(BF16)
            slot = count + 1 + t
            copy = remote(
                self.summed.at[t], self.last.at[t], self.send.at[slot], self.recv.at[slot], peer
            )
            copy.start()
            self.started.append(copy)

    def finish(self):
        count = len(self.offs)
        me = flat(own_place(self.axes), self.axes, self.sizes)
        self.started[count].wait_recv()
        self.out[...] = self.source[me, self.side].astype(F32) + self.first[count].astype(F32)
        for t in range(count):
            self.started[count + 1 + t].wait_recv()
            self.out[...] += self.last[t].astype(F32)
        for copy in self.started:
            copy.wait_send()


def scatter_kernel(specs, *refs):
    count = len(specs)
    scatters = [
        Scatter(*spec, refs[n], refs[count + n], *refs[2 * count + 5 * n : 2 * count + 5 * n + 5])
        for n, spec in enumerate(specs)
    ]
    greet([peer for s in scatters for peer in s.peers()])
    for s in scatters:
        s.start()
    for s in scatters:
        s.add()
    for s in scatters:
        s.finish()


def scatter(partials, specs, ident):
    scratch = []
    for partial in partials:
        group, block = partial.shape[0], partial.shape[2:]
        scratch += [
            pltpu.VMEM((group,) + block, BF16),
            pltpu.VMEM((group - 1,) + block, BF16),
            pltpu.VMEM((group - 1,) + block, BF16),
            pltpu.SemaphoreType.DMA((2 * group,)),
            pltpu.SemaphoreType.DMA((2 * group,)),
        ]
    return pl.pallas_call(
        functools.partial(scatter_kernel, specs),
        out_shape=[jax.ShapeDtypeStruct(p.shape[2:], F32) for p in partials],
        in_specs=[VMEM] * len(partials),
        out_specs=[VMEM] * len(partials),
        scratch_shapes=scratch,
        name="scatter%d" % ident,
        compiler_params=pltpu.CompilerParams(collective_id=ident, has_side_effects=True),
        cost_estimate=sent_estimate(sum(p.size for p in partials)),
    )(*partials)


def last_kernel(
    axes, sizes, spots, heads, share, source, blocks, out, routed, came, send, recv, hop, land
):
    offs = offsets(sizes)
    greet([moved(axes, sizes, o) for o in offs])
    me = flat(own_place(axes), axes, sizes)
    count = len(offs)
    started = []
    for t, off in enumerate(offs):
        peer = moved(axes, sizes, off)
        copy = remote(
            source.at[flat(peer, axes, sizes)], came.at[t], send.at[t], recv.at[t], peer
        )
        copy.start()
        started.append(copy)

    ctx_axes, ctx_sizes = axes[:3], sizes[:3]
    place = flat(own_place(ctx_axes), ctx_axes, ctx_sizes)

    def where(spot):
        return {
            ctx_axes[0]: spot // (ctx_sizes[1] * ctx_sizes[2]),
            ctx_axes[1]: (spot // ctx_sizes[2]) % ctx_sizes[1],
            ctx_axes[2]: spot % ctx_sizes[2],
        }

    def each_sent(act):
        for part in range(3):
            for h in range(heads):
                head = place * heads + h
                block = part * HEADS + head
                low = (block * HEAD_DIM) // share
                high = (block * HEAD_DIM + HEAD_DIM - 1) // share
                index = part * heads + h
                for which, owner, needed in (
                    (0, low, head < HEADS),
                    (1, high, (head < HEADS) & (high != low)),
                ):

                    @pl.when(needed)
                    def _(which=which, owner=owner, block=block, index=index):
                        act(index, 2 * index + which, owner, block - (share * owner) // HEAD_DIM)

    def send_block(index, slot, owner, target):
        @pl.when(owner != place)
        def _():
            remote(
                blocks.at[index], routed.at[target], hop.at[slot], land.at[target], where(owner)
            ).start()

        @pl.when(owner == place)
        def _():
            routed[target] = blocks[index]

    def sent_block(index, slot, owner, target):
        @pl.when(owner != place)
        def _():
            remote(
                blocks.at[index], routed.at[target], hop.at[slot], land.at[target], where(owner)
            ).wait_send()

    each_sent(send_block)
    for copy in started:
        copy.wait_recv()
    out[me] = source[me] + jnp.sum(came[...], axis=0)
    second = []
    for t, off in enumerate(offs):
        peer = moved(axes, sizes, off)
        copy = remote(out.at[me], out.at[me], send.at[count + t], recv.at[count + t], peer)
        copy.start()
        second.append(copy)

    base = (share * place) // HEAD_DIM
    for slot in range(routed.shape[0]):
        block = base + slot
        owner = (block % HEADS) // heads

        @pl.when((block * HEAD_DIM < share * (place + 1)) & (owner != place))
        def _(slot=slot):
            remote(
                blocks.at[0], routed.at[slot], hop.at[0], land.at[slot], where(place)
            ).wait_recv()

    each_sent(sent_block)
    for t, off in enumerate(offs):
        peer = moved(axes, sizes, off, -1)
        block = out.at[flat(peer, axes, sizes)]
        remote(block, block, send.at[count + t], recv.at[count + t], peer).wait_recv()
    for copy in started + second:
        copy.wait_send()


def last_exchange(parts, blocks, axes, sizes, spots, heads, share, ident):
    group = parts.shape[0]
    slots = max(
        (share * (c + 1) - 1) // HEAD_DIM - (share * c) // HEAD_DIM + 1 for c in range(spots)
    )
    return pl.pallas_call(
        functools.partial(last_kernel, axes, sizes, spots, heads, share),
        out_shape=[
            jax.ShapeDtypeStruct(parts.shape, F32),
            jax.ShapeDtypeStruct((slots,) + blocks.shape[1:], BF16),
        ],
        in_specs=[VMEM, VMEM],
        out_specs=[VMEM, VMEM],
        scratch_shapes=[
            pltpu.VMEM((group - 1,) + parts.shape[1:], F32),
            pltpu.SemaphoreType.DMA((2 * group,)),
            pltpu.SemaphoreType.DMA((2 * group,)),
            pltpu.SemaphoreType.DMA((6 * heads,)),
            pltpu.SemaphoreType.DMA((slots,)),
        ],
        name="last%d" % ident,
        compiler_params=pltpu.CompilerParams(collective_id=ident, has_side_effects=True),
    )(parts, blocks)


def nt(left, right):
    return lax.dot_general(left, right, (((1,), (1,)), ((), ())), preferred_element_type=F32)


def nn(left, right):
    return lax.dot_general(left, right, (((1,), (0,)), ((), ())), preferred_element_type=F32)


def rows_of(inv, ref, pair, low, high):
    first = pl.multiple_of(inv[2 * pair] * HEAD_DIM, HEAD_DIM)
    second = pl.multiple_of(inv[2 * pair + 1] * HEAD_DIM, HEAD_DIM)
    return jnp.concatenate(
        [ref[pl.ds(first, 64), low:high], ref[pl.ds(second, 64), low:high]], axis=0
    )


def put_rows(inv, ref, pair, low, high, values):
    first = pl.multiple_of(inv[2 * pair] * HEAD_DIM, HEAD_DIM)
    second = pl.multiple_of(inv[2 * pair + 1] * HEAD_DIM, HEAD_DIM)
    ref[pl.ds(first, 64), low:high] = values[:64]
    ref[pl.ds(second, 64), low:high] = values[64:]


def head_slice(values, part, heads, head):
    low = (part * heads + head) * HEAD_DIM
    return values[:, low : low + HEAD_DIM]


def diagonal(block):
    return lax.broadcasted_iota(jnp.int32, (block, block), 0) <= lax.broadcasted_iota(
        jnp.int32, (block, block), 1
    )


def attend_kernel(heads, block, inv, qkv, out, out_low, lse, qs, ks, vt, ot):
    length = qkv.shape[0]
    width = heads * HEAD_DIM

    def sort(pair, unused):
        at = pl.multiple_of(pair * 128, 128)
        values = rows_of(inv, qkv, pair, 0, 3 * width)
        for h in range(heads):
            qs[h, pl.ds(at, 128), :] = head_slice(values, 0, heads, h) * BF16(0.125)
            ks[h, pl.ds(at, 128), :] = head_slice(values, 1, heads, h)
            vt[h, :, pl.ds(at, 128)] = head_slice(values, 2, heads, h).astype(F32).T.astype(BF16)
        return unused

    lax.fori_loop(0, length // 128, sort, 0)
    allowed = diagonal(block)

    def row(qi, unused):
        q_at = pl.multiple_of(qi * block, block)

        def first(h):
            scores = nt(ks[h, pl.ds(q_at, block), :], qs[h, pl.ds(q_at, block), :])
            scores = jnp.where(allowed, scores, -1e30)
            high = jnp.max(scores, axis=0, keepdims=True)
            probs = jnp.exp(scores - high)
            return (
                high,
                jnp.sum(probs, axis=0, keepdims=True),
                nn(vt[h, :, pl.ds(q_at, block)], probs.astype(BF16)),
            )

        def column(kj, state):
            k_at = pl.multiple_of(kj * block, block)
            fresh_state = []
            for h in range(heads):
                high, weight, acc = state[h]
                scores = nt(ks[h, pl.ds(k_at, block), :], qs[h, pl.ds(q_at, block), :])
                fresh = jnp.maximum(high, jnp.max(scores, axis=0, keepdims=True))
                probs = jnp.exp(scores - fresh)
                fade = jnp.exp(high - fresh)
                fresh_state.append(
                    (
                        fresh,
                        weight * fade + jnp.sum(probs, axis=0, keepdims=True),
                        acc * fade + nn(vt[h, :, pl.ds(k_at, block)], probs.astype(BF16)),
                    )
                )
            return tuple(fresh_state)

        state = lax.fori_loop(0, qi, column, tuple(first(h) for h in range(heads)))
        for h in range(heads):
            high, weight, acc = state[h]
            ot[h, :, pl.ds(q_at, block)] = acc / weight
            lse[h : h + 1, pl.ds(q_at, block)] = high + jnp.log(weight)
        return unused

    lax.fori_loop(0, length // block, row, 0)

    def unsort(pair, unused):
        at = pl.multiple_of(pair * 128, 128)
        values = [ot[h, :, pl.ds(at, 128)].T for h in range(heads)]
        values = jnp.concatenate(values, axis=1)
        put_rows(inv, out, pair, 0, width, values)
        put_rows(inv, out_low, pair, 0, width, values.astype(BF16))
        return unused

    lax.fori_loop(0, length // 128, unsort, 0)


def attend(inv, qkv, heads):
    length = qkv.shape[0]
    width = heads * HEAD_DIM
    block = min(256, length)
    pairs = length * (length + block) // 2
    return pl.pallas_call(
        functools.partial(attend_kernel, heads, block),
        out_shape=(
            jax.ShapeDtypeStruct((length, width), F32),
            jax.ShapeDtypeStruct((length, width), BF16),
            jax.ShapeDtypeStruct((heads, length), F32),
        ),
        grid_spec=pltpu.PrefetchScalarGridSpec(
            num_scalar_prefetch=1,
            grid=(1,),
            in_specs=[pl.BlockSpec((length, 3 * width), lambda i, inv: (0, 0))],
            out_specs=(
                pl.BlockSpec((length, width), lambda i, inv: (0, 0)),
                pl.BlockSpec((length, width), lambda i, inv: (0, 0)),
                pl.BlockSpec((heads, length), lambda i, inv: (0, 0)),
            ),
            scratch_shapes=[
                pltpu.VMEM((heads, length, HEAD_DIM), BF16),
                pltpu.VMEM((heads, length, HEAD_DIM), BF16),
                pltpu.VMEM((heads, HEAD_DIM, length), BF16),
                pltpu.VMEM((heads, HEAD_DIM, length), F32),
            ],
        ),
        name="attend",
        cost_estimate=pl.CostEstimate(
            flops=4 * heads * pairs * HEAD_DIM * 4,
            bytes_accessed=length * width * 10,
            transcendentals=heads * pairs,
        ),
    )(inv, qkv)


def attend_back_kernel(
    heads, block, inv, qkv, grads, outs, lse, dqkv, qs, ks, vs, gs, kt, delta, dqt, dks, dvs
):
    length = qkv.shape[0]
    width = heads * HEAD_DIM
    count = length // block

    def sort(pair, unused):
        at = pl.multiple_of(pair * 128, 128)
        values = rows_of(inv, qkv, pair, 0, 3 * width)
        grad = rows_of(inv, grads, pair, 0, width)
        value = rows_of(inv, outs, pair, 0, width)
        product = (grad.astype(F32) * value).T
        for h in range(heads):
            qs[h, pl.ds(at, 128), :] = head_slice(values, 0, heads, h) * BF16(0.125)
            key = head_slice(values, 1, heads, h)
            ks[h, pl.ds(at, 128), :] = key
            kt[h, :, pl.ds(at, 128)] = key.astype(F32).T.astype(BF16)
            vs[h, pl.ds(at, 128), :] = head_slice(values, 2, heads, h)
            gs[h, pl.ds(at, 128), :] = head_slice(grad, 0, heads, h)
            delta[h : h + 1, pl.ds(at, 128)] = jnp.sum(
                product[h * HEAD_DIM : (h + 1) * HEAD_DIM], axis=0, keepdims=True
            )
            dqt[h, :, pl.ds(at, 128)] = jnp.zeros((HEAD_DIM, 128), F32)
        return unused

    lax.fori_loop(0, length // 128, sort, 0)
    allowed = diagonal(block)

    def column(kj, unused):
        k_at = pl.multiple_of(kj * block, block)

        def tile(h, q_at, masked):
            q = qs[h, pl.ds(q_at, block), :]
            g = gs[h, pl.ds(q_at, block), :]
            scores = nt(ks[h, pl.ds(k_at, block), :], q)
            probs = jnp.exp(scores - lse[h : h + 1, pl.ds(q_at, block)])
            if masked:
                probs = jnp.where(allowed, probs, 0.0)
            slopes = nt(vs[h, pl.ds(k_at, block), :], g)
            low = (probs * (slopes - delta[h : h + 1, pl.ds(q_at, block)])).astype(BF16)
            dqt[h, :, pl.ds(q_at, block)] += nn(kt[h, :, pl.ds(k_at, block)], low)
            return nn(low, q), nn(probs.astype(BF16), g)

        def row(qi, state):
            q_at = pl.multiple_of(qi * block, block)
            fresh = []
            for h in range(heads):
                dk, dv = tile(h, q_at, False)
                fresh.append((state[h][0] + dk, state[h][1] + dv))
            return tuple(fresh)

        state = tuple(tile(h, k_at, True) for h in range(heads))
        state = lax.fori_loop(kj + 1, count, row, state)
        for h in range(heads):
            dks[h, pl.ds(k_at, block), :] = state[h][0].astype(BF16)
            dvs[h, pl.ds(k_at, block), :] = state[h][1].astype(BF16)
        return unused

    lax.fori_loop(0, count, column, 0)

    def unsort(pair, unused):
        at = pl.multiple_of(pair * 128, 128)
        values = [(dqt[h, :, pl.ds(at, 128)].T * 0.125).astype(BF16) for h in range(heads)]
        values += [dks[h, pl.ds(at, 128), :] for h in range(heads)]
        values += [dvs[h, pl.ds(at, 128), :] for h in range(heads)]
        put_rows(inv, dqkv, pair, 0, 3 * width, jnp.concatenate(values, axis=1))
        return unused

    lax.fori_loop(0, length // 128, unsort, 0)


def attend_back(inv, qkv, grads, outs, lse, heads):
    length = qkv.shape[0]
    width = heads * HEAD_DIM
    block = min(256, length)
    pairs = length * (length + block) // 2
    row_shape = (heads, length, HEAD_DIM)
    return pl.pallas_call(
        functools.partial(attend_back_kernel, heads, block),
        out_shape=jax.ShapeDtypeStruct((length, 3 * width), BF16),
        grid_spec=pltpu.PrefetchScalarGridSpec(
            num_scalar_prefetch=1,
            grid=(1,),
            in_specs=[
                pl.BlockSpec((length, 3 * width), lambda i, inv: (0, 0)),
                pl.BlockSpec((length, width), lambda i, inv: (0, 0)),
                pl.BlockSpec((length, width), lambda i, inv: (0, 0)),
                pl.BlockSpec((heads, length), lambda i, inv: (0, 0)),
            ],
            out_specs=pl.BlockSpec((length, 3 * width), lambda i, inv: (0, 0)),
            scratch_shapes=[
                pltpu.VMEM(row_shape, BF16),
                pltpu.VMEM(row_shape, BF16),
                pltpu.VMEM(row_shape, BF16),
                pltpu.VMEM(row_shape, BF16),
                pltpu.VMEM((heads, HEAD_DIM, length), BF16),
                pltpu.VMEM((heads, length), F32),
                pltpu.VMEM((heads, HEAD_DIM, length), F32),
                pltpu.VMEM(row_shape, BF16),
                pltpu.VMEM(row_shape, BF16),
            ],
        ),
        name="attend_back",
        cost_estimate=pl.CostEstimate(
            flops=10 * heads * pairs * HEAD_DIM * 4,
            bytes_accessed=length * width * 20,
            transcendentals=heads * pairs,
        ),
    )(inv, qkv, grads, outs, lse)


def layer_norm(values, gain, shift):
    center = jnp.mean(values, axis=-1, keepdims=True)
    centred = values - center
    spread = jnp.mean(centred * centred, axis=-1, keepdims=True)
    return centred * lax.rsqrt(spread + EPSILON) * gain + shift


def smooth_gelu(values):
    return (
        0.5
        * values
        * (1.0 + jnp.tanh(0.7978845608028654 * (values + 0.044715 * values * values * values)))
    )


def matmul(left, right):
    return jnp.dot(left, right, preferred_element_type=F32)


def against(left, weight):
    return lax.dot_general(left, weight, (((1,), (1,)), ((), ())), preferred_element_type=F32)


def onto(left, right):
    return lax.dot_general(left, right, (((0,), (0,)), ((), ())), preferred_element_type=F32)


def body(
    sizes,
    tokens,
    block_order,
    qkv_weight,
    query_bias,
    value_bias,
    out_weight,
    out_bias,
    expand_weight,
    expand_bias,
    shrink_weight,
    shrink_bias,
    first_gain,
    first_shift,
    second_gain,
    second_shift,
    cotangent,
):
    outer, inner, ys, xs, ks = (sizes[a] for a in ("o", "i", "y", "x", "k"))
    spots = outer * inner * ys
    shards = xs * ks
    rows, width = tokens.shape[1:]
    o, i, y = lax.axis_index("o"), lax.axis_index("i"), lax.axis_index("y")
    shard = lax.axis_index("x") * ks + lax.axis_index("k")
    place = (o * inner + i) * ys + y
    heads = -(-HEADS // spots)
    span = heads * HEAD_DIM
    padded = spots * span
    part = qkv_weight.shape[0]
    hidden = expand_weight.shape[1]
    piece = hidden // (shards * inner)
    every = (("o", "i", "y"), (outer, inner, ys))
    ctx = (("o", "i"), (outer, inner), "y")
    group = (("i", "x"), (inner, xs), "k")
    pair = (("x",), (xs,), "k")
    own = tokens[0]
    own_grad = cotangent[0]

    def columns(values, count):
        wide = values.reshape(values.shape[:-1] + (count, width))
        wide = jnp.pad(wide, [(0, 0)] * (wide.ndim - 1) + [(0, padded - width)])
        return lax.dynamic_slice_in_dim(wide, place * span, span, axis=wide.ndim - 1)

    qkv_bias = jnp.concatenate(
        [columns(query_bias, 1)[0], jnp.zeros((span,), F32), columns(value_bias, 1)[0]]
    )
    gathered, qkv_columns, expand_columns = first_gather(
        own, qkv_weight, expand_weight, span, [ctx, pair], (xs, ks), every, piece, 0
    )
    sequence = gathered.reshape(spots * rows, width)
    qkv_columns = qkv_columns.reshape(width, 3 * span)
    expand_columns = expand_columns.reshape(width, piece)

    def doubled(values, axis_name):
        came = lax.ppermute(values, axis_name, [(0, 1), (1, 0)])
        return jnp.where(
            lax.axis_index(axis_name) == 0, jnp.stack([values, came]), jnp.stack([came, values])
        )

    def over_group(values):
        near = doubled(values, "x")
        near = doubled(near, "i")
        far = lax.ppermute(near, "k", [(0, 1), (1, 0)])
        first = lax.axis_index("k") == 0
        both = jnp.stack([jnp.where(first, near, far), jnp.where(first, far, near)], axis=2)
        return both.reshape(-1, width)

    sequence, out_own, later_grad = lax.optimization_barrier((sequence, out_weight, own_grad))
    swap = [(0, 1), (1, 0)]
    out_pair = jnp.stack([out_own, lax.ppermute(out_own, "x", swap)])
    out_mate = lax.ppermute(out_pair, "k", swap)
    group_grad = over_group(later_grad)
    shrink_rows = lax.dynamic_slice_in_dim(shrink_weight, i * piece, piece, axis=0)
    expand_own_bias = lax.dynamic_slice_in_dim(
        expand_bias, (shard * inner + i) * piece, piece, axis=0
    )

    order_row = block_order[0]
    blocks = order_row.shape[0]
    inv = jnp.sum(
        jnp.where(
            order_row[:, None] == jnp.arange(blocks, dtype=jnp.int32)[None, :],
            jnp.arange(blocks, dtype=jnp.int32)[:, None],
            0,
        ),
        axis=0,
    ).astype(jnp.int32)
    normed_low = layer_norm(sequence.astype(F32), first_gain, first_shift).astype(BF16)
    qkv = (matmul(normed_low, qkv_columns) + qkv_bias).astype(BF16)
    attended, attended_bf, log_sum = attend(inv, qkv, heads)
    attended_low = to_tokens(attended_bf.reshape(spots, rows, span), width, *every, 1)

    out_parts = [out_pair[0], out_mate[0], out_pair[1], out_mate[1]]
    out_spots = [shard, shard ^ 1, shard ^ 2, shard ^ 3]

    def out_project(low):
        terms = [
            matmul(lax.dynamic_slice_in_dim(low, spot * part, part, axis=1), weight)
            for spot, weight in zip(out_spots, out_parts)
        ]
        return terms[0] + terms[1] + terms[2] + terms[3]

    inputs = own.astype(F32)
    middle = inputs + out_project(attended_low) + out_bias
    lowered_two = layer_norm(middle, second_gain, second_shift).astype(BF16)

    def cut(values, axis_name, dim):
        index, size = lax.axis_index(axis_name), sizes[axis_name]
        return [
            lax.dynamic_index_in_dim(values, lax.rem(index + s, size), axis=dim, keepdims=False)
            for s in range(size)
        ]

    def added(pieces, axis_name):
        size = sizes[axis_name]
        total = pieces[0].astype(F32)
        for step in range(1, size):
            ring = [(d, (d + step) % size) for d in range(size)]
            total = total + lax.ppermute(pieces[step], axis_name, ring).astype(F32)
        return total.astype(BF16)

    cell = width // spots
    cuts = spots // (2 * shards)

    def cut_columns(left, right):
        local = onto(left, right).astype(BF16)
        return cut(local.reshape(outer, inner, ys, cell, right.shape[1]), "y", 2)

    def owned(local):
        kept, sent = cut(local, "i", 0)
        came = lax.ppermute(sent, "i", [(0, 1), (1, 0)])
        local = jnp.where(i == 0, jnp.stack([kept, came]), jnp.stack([came, kept]))
        return local.transpose(0, 2, 1).reshape(-1, cell).astype(F32)

    (group_low,) = gather([lowered_two], [group], 2)
    group_low = group_low.reshape(-1, width)
    expanded = matmul(group_low, expand_columns) + expand_own_bias
    hidden_low = smooth_gelu(expanded).astype(BF16)
    grad_hidden = against(group_grad, shrink_rows)
    unused, gelu_back = jax.vjp(smooth_gelu, expanded)
    (grad_expanded,) = gelu_back(grad_hidden)
    expanded_low = grad_expanded.astype(BF16)
    grad_partial = against(expanded_low, expand_columns).astype(BF16)
    shape = (inner * xs, ks, rows, width)
    shrink_cut = cut_columns(group_grad, hidden_low)
    expand_cut = onto(group_low, expanded_low).astype(BF16)
    expand_cut = expand_cut.reshape(shards, part, cuts, piece // cuts).transpose(0, 2, 1, 3)
    expand_cut = cut(expand_cut.reshape(outer, ys, part, piece // cuts), "y", 1)
    grad_partial, shrink_cut, expand_cut = lax.optimization_barrier(
        (grad_partial, shrink_cut, expand_cut)
    )
    (grad_normed_two,) = scatter([grad_partial.reshape(shape)], [group], 3)

    grad_result = own_grad.astype(F32)
    unused, second_back = jax.vjp(layer_norm, middle, second_gain, second_shift)
    grad_middle_norm, grad_second_gain, grad_second_shift = second_back(grad_normed_two)
    grad_middle = grad_result + grad_middle_norm
    middle_low = grad_middle.astype(BF16)
    turned = jnp.stack([against(middle_low, weight) for weight in out_parts])
    turned = turned.reshape(2, 2, rows, part)
    turned = jnp.where(lax.axis_index("x") == 0, turned, turned[::-1])
    turned = jnp.where(lax.axis_index("k") == 0, turned, turned[:, ::-1])
    grad_att_low = turned.reshape(shards, rows, part).transpose(1, 0, 2).reshape(rows, width)
    grad_att_low = grad_att_low.astype(BF16)
    grad_heads, att_group = to_heads(
        grad_att_low, attended_low, span, *every, ("i", "x", "k"), (inner, xs, ks), 4
    )
    grad_heads = grad_heads.reshape(spots * rows, span)
    middle_group = over_group(middle_low)
    att_group = att_group.reshape(middle_group.shape[0], -1)
    shrink_half, expand_half = added(shrink_cut, "y"), added(expand_cut, "y")
    shrink_cut, expand_cut = cut(shrink_half, "o", 0), cut(expand_half, "o", 0)
    grad_heads, shrink_cut, expand_cut = lax.optimization_barrier(
        (grad_heads, shrink_cut, expand_cut)
    )

    dqkv = attend_back(inv, qkv, grad_heads, attended, log_sum, heads)
    norm_partial = against(dqkv, qkv_columns).astype(BF16)
    qkv_partial = onto(normed_low, dqkv).astype(BF16)
    result_partial = matmul(hidden_low, shrink_rows).astype(BF16)
    outw_cut = cut_columns(middle_group, att_group)
    shrink_whole, expand_whole = added(shrink_cut, "o"), added(expand_cut, "o")
    norm_partial, shrink_whole, expand_whole, outw_cut = lax.optimization_barrier(
        (norm_partial, shrink_whole, expand_whole, outw_cut)
    )
    grad_normed_one, qkv_cells, shrunk = scatter(
        [
            norm_partial.reshape(outer * inner, ys, rows, width),
            qkv_partial.reshape(xs, ks, part, 3 * span),
            result_partial.reshape(shape),
        ],
        [ctx, pair, group],
        5,
    )
    result = middle + shrunk + shrink_bias
    unused, first_back = jax.vjp(layer_norm, inputs, first_gain, first_shift)
    grad_first_input, grad_first_gain, grad_first_shift = first_back(grad_normed_one)
    grad_inputs = grad_middle + grad_first_input

    grad_shrink = owned(shrink_whole)
    axes = ("o", "i", "y", "x", "k")
    routes = []
    for so, si, sy, sf in itertools.product(*map(range, (outer, inner, ys, shards))):
        index = so * ys + sy
        spot = sf * (spots // shards) + si * cuts + index % cuts
        routes.append((((so * inner + si) * ys + sy) * shards + sf, spot * shards + index // cuts))
    grad_expand = lax.ppermute(expand_whole, axes, routes).astype(F32)
    grad_outw = owned(added(cut(added(outw_cut, "y"), "o", 0), "o"))

    def placed(values, start, size):
        return lax.dynamic_update_slice_in_dim(jnp.zeros((size,), F32), values, start, axis=0)

    dqkv_sums = jnp.sum(dqkv.astype(F32), axis=0)
    small = [
        placed(dqkv_sums[:span], place * span, padded),
        placed(dqkv_sums[2 * span :], place * span, padded),
        jnp.sum(middle_low.astype(F32), axis=0),
        placed(
            jnp.sum(expanded_low.astype(F32), axis=0), (shard * inner + i) * piece, hidden
        ),
        jnp.sum(grad_result, axis=0),
        grad_first_gain,
        grad_first_shift,
        grad_second_gain,
        grad_second_shift,
    ]
    lengths = [s.shape[0] for s in small]
    devices = spots * shards
    lanes = 128 * (-(-sum(lengths) // (devices * 1024)))
    line = jnp.concatenate(small)
    line = jnp.pad(line, (0, devices * 8 * lanes - line.shape[0])).reshape(devices, 8, lanes)
    share = 3 * width // spots
    qkv_blocks = qkv_cells.astype(BF16).T.reshape(3 * heads, HEAD_DIM, part)
    line, routed = last_exchange(
        line, qkv_blocks, axes, (outer, inner, ys, xs, ks), spots, heads, share, 6
    )
    line = line.reshape(-1)
    start = share * place - HEAD_DIM * ((share * place) // HEAD_DIM)
    grad_qkv = lax.dynamic_slice_in_dim(routed.reshape(-1, part), start, share, axis=0)
    grad_qkv = grad_qkv.T.astype(F32)
    summed = []
    start = 0
    for length in lengths:
        summed.append(line[start : start + length])
        start += length
    summed[0] = summed[0][:width]
    summed[1] = summed[1][:width]
    return (
        result.astype(BF16)[None],
        grad_inputs[None],
        grad_qkv,
        grad_outw,
        grad_expand,
        grad_shrink,
        *summed,
    )


def solution(mesh):
    spots, shards = mesh.shape["ctx"], mesh.shape["fsdp"]
    sizes = {"o": spots // 4, "i": 2, "y": 2, "x": shards // 2, "k": 2}
    fine = Mesh(mesh.devices.reshape(tuple(sizes.values())), tuple(sizes))
    seq, pos = ("x", "k"), ("o", "i", "y")
    weight = P(seq, None)
    placed = (
        P(seq, pos, None),
        P(seq, None),
        weight,
        P(),
        P(),
        weight,
        P(),
        weight,
        P(),
        weight,
        P(),
        P(),
        P(),
        P(),
        P(),
        P(seq, pos, None),
    )
    given = (P(seq, pos, None),) * 2 + (P(seq, pos),) * 4 + (P(),) * 9
    return jax.shard_map(
        functools.partial(body, sizes),
        mesh=fine,
        in_specs=placed,
        out_specs=given,
        check_vma=False,
    )
```

```python
import functools
import itertools

import jax
import jax.numpy as jnp
from jax import lax
from jax.experimental import pallas as pl
from jax.experimental.pallas import tpu as pltpu
from jax.sharding import Mesh
from jax.sharding import PartitionSpec as P

HEADS = 25
HEAD_DIM = 64
EPSILON = 1e-05
MESH = pl.DeviceIdType.MESH
F32 = jnp.float32
BF16 = jnp.bfloat16
ANY = pl.BlockSpec(memory_space=pl.ANY)
VMEM = pl.BlockSpec(memory_space=pltpu.VMEM)


def offsets(sizes):
    return [o for o in itertools.product(*(range(s) for s in sizes)) if any(o)]


def moved(axes, sizes, offset, sign=1):
    return {
        a: lax.rem(lax.axis_index(a) + (o if sign > 0 else s - o), s)
        for a, s, o in zip(axes, sizes, offset)
    }


def flat(place, axes, sizes):
    index = 0
    for a, s in zip(axes, sizes):
        index = index * s + place[a]
    return index


def own_place(axes):
    return {a: lax.axis_index(a) for a in axes}


def greet(peers):
    barrier = pltpu.get_barrier_semaphore()
    for peer in peers:
        pl.semaphore_signal(barrier, inc=1, device_id=peer, device_id_type=MESH)
    pl.semaphore_wait(barrier, len(peers))


def remote(src, dst, send, recv, peer):
    return pltpu.make_async_remote_copy(
        src_ref=src,
        dst_ref=dst,
        send_sem=send,
        recv_sem=recv,
        device_id=peer,
        device_id_type=MESH,
    )


class Gather:
    def __init__(self, axes, sizes, pair, source, out, send, recv, local):
        self.axes, self.sizes = axes, sizes
        self.offs = offsets(sizes)
        self.side = lax.axis_index(pair)
        self.mate = {pair: 1 - self.side}
        self.source, self.out, self.send, self.recv, self.local = source, out, send, recv, local
        self.started = []

    def peers(self):
        return [moved(self.axes, self.sizes, o) for o in self.offs] + [self.mate]

    def mine(self):
        return self.out.at[flat(own_place(self.axes), self.axes, self.sizes), self.side]

    def start(self):
        pltpu.make_async_copy(self.source, self.mine(), self.local).start()
        last = len(self.offs)
        for t, peer in enumerate(self.peers()):
            copy = remote(self.source, self.mine(), self.send.at[t], self.recv.at[t], peer)
            copy.start()
            self.started.append(copy)

    def hand_on(self):
        last = len(self.offs)
        for t, off in enumerate(self.offs):
            came = flat(moved(self.axes, self.sizes, off, -1), self.axes, self.sizes)
            block = self.out.at[came, self.side]
            remote(self.source, block, self.send.at[t], self.recv.at[t], self.mate).wait_recv()
            slot = last + 1 + t
            copy = remote(block, block, self.send.at[slot], self.recv.at[slot], self.mate)
            copy.start()
            self.started.append(copy)

    def finish(self):
        last = len(self.offs)
        me = flat(own_place(self.axes), self.axes, self.sizes)
        pltpu.make_async_copy(self.source, self.mine(), self.local).wait()
        block = self.out.at[me, 1 - self.side]
        remote(self.source, block, self.send.at[last], self.recv.at[last], self.mate).wait_recv()
        for t, off in enumerate(self.offs):
            came = flat(moved(self.axes, self.sizes, off, -1), self.axes, self.sizes)
            slot = last + 1 + t
            block = self.out.at[came, 1 - self.side]
            remote(
                self.source, block, self.send.at[slot], self.recv.at[slot], self.mate
            ).wait_recv()
        for copy in self.started:
            copy.wait_send()


def gather_shape(block, spec):
    group = 1
    for s in spec[1]:
        group *= s
    return jax.ShapeDtypeStruct((group, 2) + block.shape, block.dtype)


def gather_scratch(spec):
    group = 1
    for s in spec[1]:
        group *= s
    return [
        pltpu.SemaphoreType.DMA((2 * group,)),
        pltpu.SemaphoreType.DMA((2 * group,)),
        pltpu.SemaphoreType.DMA,
    ]


def sent_estimate(size):
    return pl.CostEstimate(flops=0, bytes_accessed=20 * size, transcendentals=0)


def gather_kernel(specs, *refs):
    count = len(specs)
    gathers = [
        Gather(*spec, refs[n], refs[count + n], *refs[2 * count + 3 * n : 2 * count + 3 * n + 3])
        for n, spec in enumerate(specs)
    ]
    greet([peer for g in gathers for peer in g.peers()])
    for g in gathers:
        g.start()
    for g in gathers:
        g.hand_on()
    for g in gathers:
        g.finish()


def gather(blocks, specs, ident):
    shapes = [gather_shape(block, spec) for block, spec in zip(blocks, specs)]
    return pl.pallas_call(
        functools.partial(gather_kernel, specs),
        out_shape=shapes,
        in_specs=[VMEM] * len(blocks),
        out_specs=[ANY] * len(blocks),
        scratch_shapes=[s for spec in specs for s in gather_scratch(spec)],
        name="gather%d" % ident,
        compiler_params=pltpu.CompilerParams(collective_id=ident, has_side_effects=True),
        cost_estimate=sent_estimate(sum(s.size for s in shapes)),
    )(*blocks)


def first_kernel(
    specs,
    shard_sizes,
    ctx_axes,
    ctx_sizes,
    own,
    qkv_weight,
    weight,
    all_tokens,
    all_columns,
    pieces,
    qkv_whole,
    columns,
    whole,
    cut,
    *sems,
):
    axes = ("x", "k")
    offs = offsets(shard_sizes)
    tokens = Gather(*specs[0], own, all_tokens, *sems[0:3])
    heads = Gather(*specs[1], columns, all_columns, *sems[3:6])
    read, qkv_read, send, recv, local = sems[6:11]
    qkv_fetch = pltpu.make_async_copy(qkv_weight, qkv_whole, qkv_read)
    qkv_fetch.start()
    fetch = pltpu.make_async_copy(weight, whole, read)
    fetch.start()
    greet(tokens.peers() + heads.peers() + [moved(axes, shard_sizes, o) for o in offs])
    tokens.start()
    qkv_fetch.wait()
    place = flat(own_place(ctx_axes), ctx_axes, ctx_sizes)
    rows, span = columns.shape[0], columns.shape[1] // 3
    width = qkv_whole.shape[1] // 3
    for spot in range(-(-width // span)):

        @pl.when(place == spot)
        def _(spot=spot):
            size = min(span, width - spot * span)
            for section in range(3):
                low = section * width + spot * span
                if size < span:
                    columns[:, section * span : (section + 1) * span] = jnp.zeros(
                        (rows, span), BF16
                    )
                columns[:, section * span : section * span + size] = qkv_whole[:, low : low + size]

    @pl.when(place * span >= width)
    def _():
        columns[...] = jnp.zeros(columns.shape, BF16)

    heads.start()
    fetch.wait()
    width = cut.shape[2]
    inner = lax.axis_index("i")
    for half in range(2):

        @pl.when(inner == half)
        def _():
            for f in range(cut.shape[0]):
                low = (2 * f + half) * width
                cut[f] = whole[:, low : low + width]

    me = flat(own_place(axes), axes, shard_sizes)
    here = pltpu.make_async_copy(cut.at[me], pieces.at[me], local)
    here.start()
    started = []
    for t, off in enumerate(offs):
        peer = moved(axes, shard_sizes, off)
        there = flat(peer, axes, shard_sizes)
        copy = remote(cut.at[there], pieces.at[me], send.at[t], recv.at[t], peer)
        copy.start()
        started.append(copy)
    heads.hand_on()
    tokens.hand_on()
    here.wait()
    for t, off in enumerate(offs):
        peer = moved(axes, shard_sizes, off, -1)
        came = flat(peer, axes, shard_sizes)
        remote(cut.at[came], pieces.at[came], send.at[t], recv.at[t], peer).wait_recv()
    for copy in started:
        copy.wait_send()
    heads.finish()
    tokens.finish()


def first_gather(own, qkv_weight, weight, span, specs, shard_sizes, every, piece, ident):
    shards = shard_sizes[0] * shard_sizes[1]
    part = weight.shape[0]
    columns = jax.ShapeDtypeStruct((part, 3 * span), BF16)
    shapes = [
        gather_shape(own, specs[0]),
        gather_shape(columns, specs[1]),
        jax.ShapeDtypeStruct((shards, part, piece), BF16),
    ]
    return pl.pallas_call(
        functools.partial(first_kernel, specs, shard_sizes, *every),
        out_shape=shapes,
        in_specs=[VMEM, ANY, ANY],
        out_specs=[ANY] * 3,
        scratch_shapes=[
            pltpu.VMEM(qkv_weight.shape, BF16),
            pltpu.VMEM(columns.shape, BF16),
            pltpu.VMEM(weight.shape, BF16),
            pltpu.VMEM((shards, part, piece), BF16),
            *gather_scratch(specs[0]),
            *gather_scratch(specs[1]),
            pltpu.SemaphoreType.DMA,
            pltpu.SemaphoreType.DMA,
            pltpu.SemaphoreType.DMA((shards,)),
            pltpu.SemaphoreType.DMA((shards,)),
            pltpu.SemaphoreType.DMA,
        ],
        name="first%d" % ident,
        compiler_params=pltpu.CompilerParams(collective_id=ident, has_side_effects=True),
        cost_estimate=sent_estimate(sum(s.size for s in shapes)),
    )(own, qkv_weight, weight)


def pieces_out(axes, sizes, source, out, send, recv):
    me = flat(own_place(axes), axes, sizes)
    started = []
    for t, off in enumerate(offsets(sizes)):
        peer = moved(axes, sizes, off)
        copy = remote(
            source.at[flat(peer, axes, sizes)], out.at[me], send.at[t], recv.at[t], peer
        )
        copy.start()
        started.append(copy)
    return started


def pieces_in(axes, sizes, source, out, send, recv, started):
    for t, off in enumerate(offsets(sizes)):
        peer = moved(axes, sizes, off, -1)
        came = flat(peer, axes, sizes)
        remote(source.at[came], out.at[came], send.at[t], recv.at[t], peer).wait_recv()
    for copy in started:
        copy.wait_send()


def side_kernel(
    spec, axes, sizes, block, att, everyone, att_out, att_cut, send, recv, *gather_sems
):
    beside = Gather(*spec, block, everyone, *gather_sems)
    greet([moved(axes, sizes, o) for o in offsets(sizes)])
    beside.start()
    cell = att_cut.shape[2]
    inner, shards = sizes[0], sizes[1] * sizes[2]
    for half in range(inner):
        for f in range(shards):
            low = (f * inner + half) * cell
            att_cut[half * shards + f] = att[:, low : low + cell]
    started = pieces_out(axes, sizes, att_cut, att_out, send, recv)
    me = flat(own_place(axes), axes, sizes)
    att_out[me] = att_cut[me]
    beside.hand_on()
    pieces_in(axes, sizes, att_cut, att_out, send, recv, started)
    beside.finish()


def side_gather(block, att, spec, axes, sizes, ident):
    rows, width = block.shape
    group = sizes[0] * sizes[1] * sizes[2]
    cell = width // group
    return pl.pallas_call(
        functools.partial(side_kernel, spec, axes, sizes),
        out_shape=[
            gather_shape(block, spec),
            jax.ShapeDtypeStruct((group, rows, cell), att.dtype),
        ],
        in_specs=[VMEM, VMEM],
        out_specs=[ANY, VMEM],
        scratch_shapes=[
            pltpu.VMEM((group, rows, cell), att.dtype),
            pltpu.SemaphoreType.DMA((group,)),
            pltpu.SemaphoreType.DMA((group,)),
            *gather_scratch(spec),
        ],
        name="side%d" % ident,
        compiler_params=pltpu.CompilerParams(collective_id=ident, has_side_effects=True),
        cost_estimate=sent_estimate(8 * block.size),
    )(block, att)


class Scatter:
    def __init__(self, axes, sizes, pair, source, out, first, summed, last, send, recv):
        self.axes, self.sizes = axes, sizes
        self.offs = offsets(sizes)
        self.side = lax.axis_index(pair)
        self.mate = {pair: 1 - self.side}
        self.source, self.out = source, out
        self.first, self.summed, self.last = first, summed, last
        self.send, self.recv = send, recv
        self.started = []

    def peers(self):
        return [moved(self.axes, self.sizes, o) for o in self.offs] + [self.mate]

    def start(self):
        for t, off in enumerate(self.offs + [(0,) * len(self.sizes)]):
            there = flat(moved(self.axes, self.sizes, off), self.axes, self.sizes)
            copy = remote(
                self.source.at[there, 1 - self.side],
                self.first.at[t],
                self.send.at[t],
                self.recv.at[t],
                self.mate,
            )
            copy.start()
            self.started.append(copy)

    def add(self):
        count = len(self.offs)
        for t, off in enumerate(self.offs):
            peer = moved(self.axes, self.sizes, off)
            there = flat(peer, self.axes, self.sizes)
            self.started[t].wait_recv()
            self.summed[t] = (
                self.source[there, self.side].astype(F32) + self.first[t].astype(F32)
            ).astype(BF16)
            slot = count + 1 + t
            copy = remote(
                self.summed.at[t], self.last.at[t], self.send.at[slot], self.recv.at[slot], peer
            )
            copy.start()
            self.started.append(copy)

    def finish(self):
        count = len(self.offs)
        me = flat(own_place(self.axes), self.axes, self.sizes)
        self.started[count].wait_recv()
        self.out[...] = self.source[me, self.side].astype(F32) + self.first[count].astype(F32)
        for t in range(count):
            self.started[count + 1 + t].wait_recv()
            self.out[...] += self.last[t].astype(F32)
        for copy in self.started:
            copy.wait_send()


def scatter_kernel(specs, *refs):
    count = len(specs)
    scatters = [
        Scatter(*spec, refs[n], refs[count + n], *refs[2 * count + 5 * n : 2 * count + 5 * n + 5])
        for n, spec in enumerate(specs)
    ]
    greet([peer for s in scatters for peer in s.peers()])
    for s in scatters:
        s.start()
    for s in scatters:
        s.add()
    for s in scatters:
        s.finish()


def scatter(partials, specs, ident):
    scratch = []
    for partial in partials:
        group, block = partial.shape[0], partial.shape[2:]
        scratch += [
            pltpu.VMEM((group,) + block, BF16),
            pltpu.VMEM((group - 1,) + block, BF16),
            pltpu.VMEM((group - 1,) + block, BF16),
            pltpu.SemaphoreType.DMA((2 * group,)),
            pltpu.SemaphoreType.DMA((2 * group,)),
        ]
    return pl.pallas_call(
        functools.partial(scatter_kernel, specs),
        out_shape=[jax.ShapeDtypeStruct(p.shape[2:], F32) for p in partials],
        in_specs=[VMEM] * len(partials),
        out_specs=[VMEM] * len(partials),
        scratch_shapes=scratch,
        name="scatter%d" % ident,
        compiler_params=pltpu.CompilerParams(collective_id=ident, has_side_effects=True),
        cost_estimate=sent_estimate(sum(p.size for p in partials)),
    )(*partials)


def last_kernel(
    axes, sizes, spots, heads, share, source, blocks, out, routed, came, send, recv, hop, land
):
    offs = offsets(sizes)
    greet([moved(axes, sizes, o) for o in offs])
    me = flat(own_place(axes), axes, sizes)
    count = len(offs)
    started = []
    for t, off in enumerate(offs):
        peer = moved(axes, sizes, off)
        copy = remote(
            source.at[flat(peer, axes, sizes)], came.at[t], send.at[t], recv.at[t], peer
        )
        copy.start()
        started.append(copy)

    ctx_axes, ctx_sizes = axes[:3], sizes[:3]
    place = flat(own_place(ctx_axes), ctx_axes, ctx_sizes)

    def where(spot):
        return {
            ctx_axes[0]: spot // (ctx_sizes[1] * ctx_sizes[2]),
            ctx_axes[1]: (spot // ctx_sizes[2]) % ctx_sizes[1],
            ctx_axes[2]: spot % ctx_sizes[2],
        }

    def each_sent(act):
        for part in range(3):
            for h in range(heads):
                head = place * heads + h
                block = part * HEADS + head
                low = (block * HEAD_DIM) // share
                high = (block * HEAD_DIM + HEAD_DIM - 1) // share
                index = part * heads + h
                for which, owner, needed in (
                    (0, low, head < HEADS),
                    (1, high, (head < HEADS) & (high != low)),
                ):

                    @pl.when(needed)
                    def _(which=which, owner=owner, block=block, index=index):
                        act(index, 2 * index + which, owner, block - (share * owner) // HEAD_DIM)

    def send_block(index, slot, owner, target):
        @pl.when(owner != place)
        def _():
            remote(
                blocks.at[index], routed.at[target], hop.at[slot], land.at[target], where(owner)
            ).start()

        @pl.when(owner == place)
        def _():
            routed[target] = blocks[index]

    def sent_block(index, slot, owner, target):
        @pl.when(owner != place)
        def _():
            remote(
                blocks.at[index], routed.at[target], hop.at[slot], land.at[target], where(owner)
            ).wait_send()

    each_sent(send_block)
    for copy in started:
        copy.wait_recv()
    out[me] = source[me] + jnp.sum(came[...], axis=0)
    second = []
    for t, off in enumerate(offs):
        peer = moved(axes, sizes, off)
        copy = remote(out.at[me], out.at[me], send.at[count + t], recv.at[count + t], peer)
        copy.start()
        second.append(copy)

    base = (share * place) // HEAD_DIM
    for slot in range(routed.shape[0]):
        block = base + slot
        owner = (block % HEADS) // heads

        @pl.when((block * HEAD_DIM < share * (place + 1)) & (owner != place))
        def _(slot=slot):
            remote(
                blocks.at[0], routed.at[slot], hop.at[0], land.at[slot], where(place)
            ).wait_recv()

    each_sent(sent_block)
    for t, off in enumerate(offs):
        peer = moved(axes, sizes, off, -1)
        block = out.at[flat(peer, axes, sizes)]
        remote(block, block, send.at[count + t], recv.at[count + t], peer).wait_recv()
    for copy in started + second:
        copy.wait_send()


def last_exchange(parts, blocks, axes, sizes, spots, heads, share, ident):
    group = parts.shape[0]
    slots = max(
        (share * (c + 1) - 1) // HEAD_DIM - (share * c) // HEAD_DIM + 1 for c in range(spots)
    )
    return pl.pallas_call(
        functools.partial(last_kernel, axes, sizes, spots, heads, share),
        out_shape=[
            jax.ShapeDtypeStruct(parts.shape, F32),
            jax.ShapeDtypeStruct((slots,) + blocks.shape[1:], BF16),
        ],
        in_specs=[VMEM, VMEM],
        out_specs=[VMEM, VMEM],
        scratch_shapes=[
            pltpu.VMEM((group - 1,) + parts.shape[1:], F32),
            pltpu.SemaphoreType.DMA((2 * group,)),
            pltpu.SemaphoreType.DMA((2 * group,)),
            pltpu.SemaphoreType.DMA((6 * heads,)),
            pltpu.SemaphoreType.DMA((slots,)),
        ],
        name="last%d" % ident,
        compiler_params=pltpu.CompilerParams(collective_id=ident, has_side_effects=True),
    )(parts, blocks)


def normed(values):
    center = jnp.mean(values, axis=-1, keepdims=True)
    centred = values - center
    spread = jnp.mean(centred * centred, axis=-1, keepdims=True)
    scale = lax.rsqrt(spread + EPSILON)
    return centred * scale, scale


def norm_back(grad, gain, plain, scale):
    inner = grad * gain
    return scale * (
        inner
        - jnp.mean(inner, axis=-1, keepdims=True)
        - plain * jnp.mean(inner * plain, axis=-1, keepdims=True)
    )


def middle_kernel(
    every,
    spec,
    pieces,
    own,
    own_grad,
    out_own,
    out_far,
    expand,
    shrink,
    out_bias,
    expand_bias,
    shrink_bias,
    gain,
    shift,
    att_out,
    c_out,
    e_out,
    u_out,
    gz_out,
    result,
    grad_middle,
    low_middle,
    sums,
    hidden_sum,
    to_heads,
    came,
    att,
    out_w,
    expand_w,
    shrink_w,
    mid,
    c_own,
    c_all,
    e_all,
    gh,
    u_all,
    gz_all,
    part,
    first,
    summed,
    last,
    part_two,
    first_two,
    summed_two,
    last_two,
    cut,
    send,
    recv,
    c_send,
    c_recv,
    c_local,
    e_send,
    e_recv,
    e_local,
    w_sem,
    w_send,
    w_recv,
    r_send,
    r_recv,
    s_send,
    s_recv,
    h_send,
    h_recv,
    store,
):
    axes, sizes = every
    x, k, inner = lax.axis_index("x"), lax.axis_index("k"), lax.axis_index("i")
    mate = {"k": 1 - k}
    shard = 2 * x + k
    part_rows = out_own.shape[0]
    width = own.shape[1]
    rows = own.shape[0]
    piece = expand.shape[2]

    def chip(t):
        ti, tx = lax.rem(inner + t // 2, 2), lax.rem(x + t % 2, 2)
        return 2 * ti + tx, {"i": ti, "x": tx}

    loads = [
        pltpu.make_async_copy(out_own, out_w.at[pl.ds(shard * part_rows, part_rows)], w_sem.at[0]),
        pltpu.make_async_copy(
            out_far, out_w.at[pl.ds((shard ^ 2) * part_rows, part_rows)], w_sem.at[1]
        ),
        pltpu.make_async_copy(shrink.at[pl.ds(inner * piece, piece)], shrink_w, w_sem.at[2]),
    ]
    for f in range(expand.shape[0]):
        loads.append(
            pltpu.make_async_copy(
                expand.at[f], expand_w.at[pl.ds(f * part_rows, part_rows)], w_sem.at[3 + f]
            )
        )
    for copy in loads:
        copy.start()
    greet([moved(axes, sizes, o) for o in offsets(sizes)] + [chip(t)[1] for t in range(1, 4)] + [mate])

    started = pieces_out(axes, sizes, pieces, came, send, recv)
    out_sent = []
    for n, (source, owner) in enumerate(((out_own, shard), (out_far, shard ^ 2))):
        copy = remote(
            source, out_w.at[pl.ds(owner * part_rows, part_rows)], w_send.at[n], w_recv.at[n], mate
        )
        copy.start()
        out_sent.append(copy)
    e_gather = Gather(*spec, own_grad, e_all, e_send, e_recv, e_local)
    e_gather.start()
    here = flat(own_place(axes), axes, sizes)
    came[here] = pieces[here]
    pieces_in(axes, sizes, pieces, came, send, recv, started)
    span = came.shape[2]
    for d in range(came.shape[0]):
        low, high = d * span, min((d + 1) * span, width)
        if low < high:
            att[:, low:high] = came[d, :, : high - low]
    for copy in loads[:2]:
        copy.wait()
    for n, owner in enumerate((shard ^ 1, shard ^ 3)):
        remote(
            out_own,
            out_w.at[pl.ds(owner * part_rows, part_rows)],
            w_send.at[n],
            w_recv.at[n],
            mate,
        ).wait_recv()

    mid[...] = (
        own[...].astype(F32)
        + jnp.dot(att[...], out_w[...], preferred_element_type=F32)
        + out_bias[...]
    )
    plain, scale = normed(mid[...])
    c_own[...] = (plain * gain[...] + shift[...]).astype(BF16)
    c_gather = Gather(*spec, c_own, c_all, c_send, c_recv, c_local)
    c_gather.start()
    att_copy = pltpu.make_async_copy(att, att_out, store.at[0])
    att_copy.start()
    e_gather.hand_on()
    e_gather.finish()
    e_copy = pltpu.make_async_copy(e_all, e_out, store.at[1])
    e_copy.start()
    for copy in loads[2:]:
        copy.wait()

    def both(ref, place):
        return ref[place].reshape(2 * rows, ref.shape[3])

    def slopes(t, unused):
        place, unused_peer = chip(t)
        gh[place] = nt(both(e_all, place), shrink_w[...])
        return unused

    lax.fori_loop(0, 4, slopes, 0)
    hidden_sum[...] = jnp.zeros(hidden_sum.shape, F32)

    def c_wait(t):
        place, peer = chip(t)
        block = c_all.at[place, 1 - k]
        remote(c_own, block, c_send.at[3 + t], c_recv.at[3 + t], mate).wait_recv()

    def c_hand_on(t):
        place, peer = chip(t)
        block = c_all.at[place, k]
        remote(c_own, block, c_send.at[t - 1], c_recv.at[t - 1], mate).wait_recv()
        remote(block, block, c_send.at[3 + t], c_recv.at[3 + t], mate).start()

    def to_mate(t, source, target, sends, recvs):
        place, peer = chip(t)
        return remote(source.at[place, 1 - k], target.at[t], sends.at[t], recvs.at[t], mate)

    def to_chip(t, source, target, sends, recvs):
        place, peer = chip(t)
        return remote(
            source.at[t - 1], target.at[t - 1], sends.at[3 + t], recvs.at[3 + t], peer
        )

    def add_and_send(t, parts, firsts, sums_of, lasts, sends, recvs):
        place, peer = chip(t)
        to_mate(t, parts, firsts, sends, recvs).wait_recv()
        sums_of[t - 1] = (parts[place, k].astype(F32) + firsts[t].astype(F32)).astype(BF16)
        to_chip(t, sums_of, lasts, sends, recvs).start()

    pltpu.make_async_copy(c_own, c_gather.mine(), c_local).wait()

    def feed(t, unused):
        c_wait(t)
        place, peer = chip(t)
        expanded = jnp.dot(both(c_all, place), expand_w[...], preferred_element_type=F32)
        expanded = expanded + expand_bias[...]
        square = expanded * expanded
        bent = jnp.tanh(0.7978845608028654 * (expanded + 0.044715 * square * expanded))
        half = 0.5 * (1.0 + bent)
        u_all[place] = (expanded * half).astype(BF16)
        slope = half + 0.5 * expanded * (1.0 - bent * bent) * (
            0.7978845608028654 * (1.0 + 3 * 0.044715 * square)
        )
        low = (slope * gh[place]).astype(BF16)
        gz_all[place] = low
        hidden_sum[...] += jnp.sum(low.astype(F32), axis=0, keepdims=True)
        back = nt(low, expand_w[...]).astype(BF16)
        part[place] = back.reshape(2, rows, width)
        to_mate(t, part, first, r_send, r_recv).start()

        @pl.when(t < 3)
        def _():
            c_hand_on(t + 1)

        @pl.when(t > 1)
        def _():
            add_and_send(t - 1, part, first, summed, last, r_send, r_recv)

        return unused

    lax.fori_loop(0, 4, feed, 0)
    add_and_send(3, part, first, summed, last, r_send, r_recv)
    c_copy = pltpu.make_async_copy(c_all, c_out, store.at[2])
    c_copy.start()
    u_copy = pltpu.make_async_copy(u_all, u_out, store.at[3])
    u_copy.start()
    gz_copy = pltpu.make_async_copy(gz_all, gz_out, store.at[4])
    gz_copy.start()

    def shrunk(t, unused):
        place, peer = chip(t)
        terms = jnp.dot(u_all[place], shrink_w[...], preferred_element_type=F32).astype(BF16)
        part_two[place] = terms.reshape(2, rows, width)
        to_mate(t, part_two, first_two, s_send, s_recv).start()
        return unused

    lax.fori_loop(0, 4, shrunk, 0)

    def gathered_sum(parts, firsts, lasts, sends, recvs):
        place, unused_peer = chip(0)
        to_mate(0, parts, firsts, sends, recvs).wait_recv()
        total = parts[place, k].astype(F32) + firsts[0].astype(F32)
        for t in range(1, 4):
            to_chip(t, firsts, lasts, sends, recvs).wait_recv()
            total = total + lasts[t - 1].astype(F32)
        return total

    grad = gathered_sum(part, first, last, r_send, r_recv)
    plain, scale = normed(mid[...])
    grad_mid = own_grad[...].astype(F32) + norm_back(grad, gain[...], plain, scale)
    grad_middle[...] = grad_mid
    low = grad_mid.astype(BF16)
    low_middle[...] = low
    sums[0:1, :] = jnp.sum(low.astype(F32), axis=0, keepdims=True)
    sums[1:2, :] = jnp.sum(own_grad[...].astype(F32), axis=0, keepdims=True)
    sums[2:3, :] = jnp.sum(grad * plain, axis=0, keepdims=True)
    sums[3:4, :] = jnp.sum(grad, axis=0, keepdims=True)
    back = nt(low, out_w[...]).astype(BF16)
    for d in range(cut.shape[0]):
        low_end, high = d * span, min((d + 1) * span, width)
        if high - low_end < span:
            cut[d] = jnp.zeros(cut.shape[1:], cut.dtype)
        if low_end < high:
            cut[d, :, : high - low_end] = back[:, low_end:high]
    head_started = pieces_out(axes, sizes, cut, to_heads, h_send, h_recv)
    for t in range(1, 4):
        add_and_send(t, part_two, first_two, summed_two, last_two, s_send, s_recv)
    to_heads[here] = cut[here]
    result[...] = (
        mid[...] + gathered_sum(part_two, first_two, last_two, s_send, s_recv) + shrink_bias[...]
    ).astype(BF16)
    pieces_in(axes, sizes, cut, to_heads, h_send, h_recv, head_started)

    for copy in out_sent + c_gather.started:
        copy.wait_send()
    for t in range(1, 4):
        place, peer = chip(t)
        remote(c_own, c_own, c_send.at[3 + t], c_recv.at[3 + t], mate).wait_send()
    for t in range(4):
        to_mate(t, part, first, r_send, r_recv).wait_send()
        to_mate(t, part_two, first_two, s_send, s_recv).wait_send()
    for t in range(1, 4):
        to_chip(t, summed, last, r_send, r_recv).wait_send()
        to_chip(t, summed_two, last_two, s_send, s_recv).wait_send()
    for copy in (att_copy, e_copy, c_copy, u_copy, gz_copy):
        copy.wait()


def middle_part(
    pieces, own, own_grad, out_own, out_far, expand, shrink, vectors, every, spec, ident
):
    spots, rows, span = pieces.shape
    width = own.shape[1]
    piece = expand.shape[2]
    everyone = jax.ShapeDtypeStruct((4, 2, rows, width), BF16)
    hidden = jax.ShapeDtypeStruct((4, 2 * rows, piece), BF16)
    flat_f32 = jax.ShapeDtypeStruct((rows, width), F32)
    flat_low = jax.ShapeDtypeStruct((rows, width), BF16)

    def scatter_buffers():
        return [
            pltpu.VMEM(everyone.shape, BF16),
            pltpu.VMEM((4, rows, width), BF16),
            pltpu.VMEM((3, rows, width), BF16),
            pltpu.VMEM((3, rows, width), BF16),
        ]

    return pl.pallas_call(
        functools.partial(middle_kernel, every, spec),
        out_shape=[
            flat_low,
            everyone,
            everyone,
            hidden,
            hidden,
            flat_low,
            flat_f32,
            flat_low,
            jax.ShapeDtypeStruct((4, width), F32),
            jax.ShapeDtypeStruct((1, piece), F32),
            jax.ShapeDtypeStruct(pieces.shape, BF16),
        ],
        in_specs=[VMEM] * 3 + [ANY] * 4 + [VMEM] * 5,
        out_specs=[ANY] * 5 + [VMEM] * 6,
        scratch_shapes=[
            pltpu.VMEM(pieces.shape, BF16),
            pltpu.VMEM((rows, width), BF16),
            pltpu.VMEM((width, width), BF16),
            pltpu.VMEM((width, piece), BF16),
            pltpu.VMEM((piece, width), BF16),
            pltpu.VMEM((rows, width), F32),
            pltpu.VMEM((rows, width), BF16),
            pltpu.VMEM(everyone.shape, BF16),
            pltpu.VMEM(everyone.shape, BF16),
            pltpu.VMEM(hidden.shape, F32),
            pltpu.VMEM(hidden.shape, BF16),
            pltpu.VMEM(hidden.shape, BF16),
            *scatter_buffers(),
            *scatter_buffers(),
            pltpu.VMEM(pieces.shape, BF16),
            pltpu.SemaphoreType.DMA((spots,)),
            pltpu.SemaphoreType.DMA((spots,)),
            *gather_scratch(spec),
            *gather_scratch(spec),
            pltpu.SemaphoreType.DMA((7,)),
            pltpu.SemaphoreType.DMA((2,)),
            pltpu.SemaphoreType.DMA((2,)),
            pltpu.SemaphoreType.DMA((7,)),
            pltpu.SemaphoreType.DMA((7,)),
            pltpu.SemaphoreType.DMA((7,)),
            pltpu.SemaphoreType.DMA((7,)),
            pltpu.SemaphoreType.DMA((spots,)),
            pltpu.SemaphoreType.DMA((spots,)),
            pltpu.SemaphoreType.DMA((5,)),
        ],
        name="middle%d" % ident,
        compiler_params=pltpu.CompilerParams(
            collective_id=ident, has_side_effects=True, vmem_limit_bytes=60 * 2**20
        ),
        cost_estimate=pl.CostEstimate(
            flops=8 * rows * 8 * width * piece,
            bytes_accessed=100 * rows * width * 2,
            transcendentals=8 * rows * piece,
        ),
    )(pieces, own, own_grad, out_own, out_far, expand, shrink, *vectors)


def nt(left, right):
    return lax.dot_general(left, right, (((1,), (1,)), ((), ())), preferred_element_type=F32)


def nn(left, right):
    return lax.dot_general(left, right, (((1,), (0,)), ((), ())), preferred_element_type=F32)


def rows_of(inv, ref, pair, low, high):
    first = pl.multiple_of(inv[2 * pair] * HEAD_DIM, HEAD_DIM)
    second = pl.multiple_of(inv[2 * pair + 1] * HEAD_DIM, HEAD_DIM)
    return jnp.concatenate(
        [ref[pl.ds(first, 64), low:high], ref[pl.ds(second, 64), low:high]], axis=0
    )


def put_rows(inv, ref, pair, low, high, values):
    first = pl.multiple_of(inv[2 * pair] * HEAD_DIM, HEAD_DIM)
    second = pl.multiple_of(inv[2 * pair + 1] * HEAD_DIM, HEAD_DIM)
    ref[pl.ds(first, 64), low:high] = values[:64]
    ref[pl.ds(second, 64), low:high] = values[64:]


def head_slice(values, part, heads, head):
    low = (part * heads + head) * HEAD_DIM
    return values[:, low : low + HEAD_DIM]


def diagonal(block):
    return lax.broadcasted_iota(jnp.int32, (block, block), 0) <= lax.broadcasted_iota(
        jnp.int32, (block, block), 1
    )


def attend_kernel(heads, block, inv, qkv, out, out_low, lse, qs, ks, vt, ot):
    length = qkv.shape[0]
    width = heads * HEAD_DIM

    def sort(pair, unused):
        at = pl.multiple_of(pair * 128, 128)
        values = rows_of(inv, qkv, pair, 0, 3 * width)
        for h in range(heads):
            qs[h, pl.ds(at, 128), :] = head_slice(values, 0, heads, h) * BF16(0.125)
            ks[h, pl.ds(at, 128), :] = head_slice(values, 1, heads, h)
            vt[h, :, pl.ds(at, 128)] = head_slice(values, 2, heads, h).astype(F32).T.astype(BF16)
        return unused

    lax.fori_loop(0, length // 128, sort, 0)
    allowed = diagonal(block)

    def row(qi, unused):
        q_at = pl.multiple_of(qi * block, block)

        def first(h):
            scores = nt(ks[h, pl.ds(q_at, block), :], qs[h, pl.ds(q_at, block), :])
            scores = jnp.where(allowed, scores, -1e30)
            high = jnp.max(scores, axis=0, keepdims=True)
            probs = jnp.exp(scores - high)
            return (
                high,
                jnp.sum(probs, axis=0, keepdims=True),
                nn(vt[h, :, pl.ds(q_at, block)], probs.astype(BF16)),
            )

        def column(kj, state):
            k_at = pl.multiple_of(kj * block, block)
            fresh_state = []
            for h in range(heads):
                high, weight, acc = state[h]
                scores = nt(ks[h, pl.ds(k_at, block), :], qs[h, pl.ds(q_at, block), :])
                fresh = jnp.maximum(high, jnp.max(scores, axis=0, keepdims=True))
                probs = jnp.exp(scores - fresh)
                fade = jnp.exp(high - fresh)
                fresh_state.append(
                    (
                        fresh,
                        weight * fade + jnp.sum(probs, axis=0, keepdims=True),
                        acc * fade + nn(vt[h, :, pl.ds(k_at, block)], probs.astype(BF16)),
                    )
                )
            return tuple(fresh_state)

        state = lax.fori_loop(0, qi, column, tuple(first(h) for h in range(heads)))
        for h in range(heads):
            high, weight, acc = state[h]
            ot[h, :, pl.ds(q_at, block)] = acc / weight
            lse[h : h + 1, pl.ds(q_at, block)] = high + jnp.log(weight)
        return unused

    lax.fori_loop(0, length // block, row, 0)

    def unsort(pair, unused):
        at = pl.multiple_of(pair * 128, 128)
        values = [ot[h, :, pl.ds(at, 128)].T for h in range(heads)]
        values = jnp.concatenate(values, axis=1)
        put_rows(inv, out, pair, 0, width, values)
        put_rows(inv, out_low, pair, 0, width, values.astype(BF16))
        return unused

    lax.fori_loop(0, length // 128, unsort, 0)


def attend(inv, qkv, heads):
    length = qkv.shape[0]
    width = heads * HEAD_DIM
    block = min(256, length)
    pairs = length * (length + block) // 2
    return pl.pallas_call(
        functools.partial(attend_kernel, heads, block),
        out_shape=(
            jax.ShapeDtypeStruct((length, width), F32),
            jax.ShapeDtypeStruct((length, width), BF16),
            jax.ShapeDtypeStruct((heads, length), F32),
        ),
        grid_spec=pltpu.PrefetchScalarGridSpec(
            num_scalar_prefetch=1,
            grid=(1,),
            in_specs=[pl.BlockSpec((length, 3 * width), lambda i, inv: (0, 0))],
            out_specs=(
                pl.BlockSpec((length, width), lambda i, inv: (0, 0)),
                pl.BlockSpec((length, width), lambda i, inv: (0, 0)),
                pl.BlockSpec((heads, length), lambda i, inv: (0, 0)),
            ),
            scratch_shapes=[
                pltpu.VMEM((heads, length, HEAD_DIM), BF16),
                pltpu.VMEM((heads, length, HEAD_DIM), BF16),
                pltpu.VMEM((heads, HEAD_DIM, length), BF16),
                pltpu.VMEM((heads, HEAD_DIM, length), F32),
            ],
        ),
        name="attend",
        cost_estimate=pl.CostEstimate(
            flops=4 * heads * pairs * HEAD_DIM * 4,
            bytes_accessed=length * width * 10,
            transcendentals=heads * pairs,
        ),
    )(inv, qkv)


def attend_back_kernel(
    heads, block, inv, qkv, grads, outs, lse, dqkv, qs, ks, vs, gs, kt, delta, dqt, dks, dvs
):
    length = qkv.shape[0]
    width = heads * HEAD_DIM
    count = length // block

    def sort(pair, unused):
        at = pl.multiple_of(pair * 128, 128)
        values = rows_of(inv, qkv, pair, 0, 3 * width)
        grad = rows_of(inv, grads, pair, 0, width)
        value = rows_of(inv, outs, pair, 0, width)
        product = (grad.astype(F32) * value).T
        for h in range(heads):
            qs[h, pl.ds(at, 128), :] = head_slice(values, 0, heads, h) * BF16(0.125)
            key = head_slice(values, 1, heads, h)
            ks[h, pl.ds(at, 128), :] = key
            kt[h, :, pl.ds(at, 128)] = key.astype(F32).T.astype(BF16)
            vs[h, pl.ds(at, 128), :] = head_slice(values, 2, heads, h)
            gs[h, pl.ds(at, 128), :] = head_slice(grad, 0, heads, h)
            delta[h : h + 1, pl.ds(at, 128)] = jnp.sum(
                product[h * HEAD_DIM : (h + 1) * HEAD_DIM], axis=0, keepdims=True
            )
            dqt[h, :, pl.ds(at, 128)] = jnp.zeros((HEAD_DIM, 128), F32)
        return unused

    lax.fori_loop(0, length // 128, sort, 0)
    allowed = diagonal(block)

    def column(kj, unused):
        k_at = pl.multiple_of(kj * block, block)

        def tile(h, q_at, masked):
            q = qs[h, pl.ds(q_at, block), :]
            g = gs[h, pl.ds(q_at, block), :]
            scores = nt(ks[h, pl.ds(k_at, block), :], q)
            probs = jnp.exp(scores - lse[h : h + 1, pl.ds(q_at, block)])
            if masked:
                probs = jnp.where(allowed, probs, 0.0)
            slopes = nt(vs[h, pl.ds(k_at, block), :], g)
            low = (probs * (slopes - delta[h : h + 1, pl.ds(q_at, block)])).astype(BF16)
            dqt[h, :, pl.ds(q_at, block)] += nn(kt[h, :, pl.ds(k_at, block)], low)
            return nn(low, q), nn(probs.astype(BF16), g)

        def row(qi, state):
            q_at = pl.multiple_of(qi * block, block)
            fresh = []
            for h in range(heads):
                dk, dv = tile(h, q_at, False)
                fresh.append((state[h][0] + dk, state[h][1] + dv))
            return tuple(fresh)

        state = tuple(tile(h, k_at, True) for h in range(heads))
        state = lax.fori_loop(kj + 1, count, row, state)
        for h in range(heads):
            dks[h, pl.ds(k_at, block), :] = state[h][0].astype(BF16)
            dvs[h, pl.ds(k_at, block), :] = state[h][1].astype(BF16)
        return unused

    lax.fori_loop(0, count, column, 0)

    def unsort(pair, unused):
        at = pl.multiple_of(pair * 128, 128)
        values = [(dqt[h, :, pl.ds(at, 128)].T * 0.125).astype(BF16) for h in range(heads)]
        values += [dks[h, pl.ds(at, 128), :] for h in range(heads)]
        values += [dvs[h, pl.ds(at, 128), :] for h in range(heads)]
        put_rows(inv, dqkv, pair, 0, 3 * width, jnp.concatenate(values, axis=1))
        return unused

    lax.fori_loop(0, length // 128, unsort, 0)


def attend_back(inv, qkv, grads, outs, lse, heads):
    length = qkv.shape[0]
    width = heads * HEAD_DIM
    block = min(256, length)
    pairs = length * (length + block) // 2
    row_shape = (heads, length, HEAD_DIM)
    return pl.pallas_call(
        functools.partial(attend_back_kernel, heads, block),
        out_shape=jax.ShapeDtypeStruct((length, 3 * width), BF16),
        grid_spec=pltpu.PrefetchScalarGridSpec(
            num_scalar_prefetch=1,
            grid=(1,),
            in_specs=[
                pl.BlockSpec((length, 3 * width), lambda i, inv: (0, 0)),
                pl.BlockSpec((length, width), lambda i, inv: (0, 0)),
                pl.BlockSpec((length, width), lambda i, inv: (0, 0)),
                pl.BlockSpec((heads, length), lambda i, inv: (0, 0)),
            ],
            out_specs=pl.BlockSpec((length, 3 * width), lambda i, inv: (0, 0)),
            scratch_shapes=[
                pltpu.VMEM(row_shape, BF16),
                pltpu.VMEM(row_shape, BF16),
                pltpu.VMEM(row_shape, BF16),
                pltpu.VMEM(row_shape, BF16),
                pltpu.VMEM((heads, HEAD_DIM, length), BF16),
                pltpu.VMEM((heads, length), F32),
                pltpu.VMEM((heads, HEAD_DIM, length), F32),
                pltpu.VMEM(row_shape, BF16),
                pltpu.VMEM(row_shape, BF16),
            ],
        ),
        name="attend_back",
        cost_estimate=pl.CostEstimate(
            flops=10 * heads * pairs * HEAD_DIM * 4,
            bytes_accessed=length * width * 20,
            transcendentals=heads * pairs,
        ),
    )(inv, qkv, grads, outs, lse)


def layer_norm(values, gain, shift):
    center = jnp.mean(values, axis=-1, keepdims=True)
    centred = values - center
    spread = jnp.mean(centred * centred, axis=-1, keepdims=True)
    return centred * lax.rsqrt(spread + EPSILON) * gain + shift


def smooth_gelu(values):
    return (
        0.5
        * values
        * (1.0 + jnp.tanh(0.7978845608028654 * (values + 0.044715 * values * values * values)))
    )


def matmul(left, right):
    return jnp.dot(left, right, preferred_element_type=F32)


def against(left, weight):
    return lax.dot_general(left, weight, (((1,), (1,)), ((), ())), preferred_element_type=F32)


def onto(left, right):
    return lax.dot_general(left, right, (((0,), (0,)), ((), ())), preferred_element_type=F32)


def body(
    sizes,
    tokens,
    block_order,
    qkv_weight,
    query_bias,
    value_bias,
    out_weight,
    out_bias,
    expand_weight,
    expand_bias,
    shrink_weight,
    shrink_bias,
    first_gain,
    first_shift,
    second_gain,
    second_shift,
    cotangent,
):
    outer, inner, ys, xs, ks = (sizes[a] for a in ("o", "i", "y", "x", "k"))
    spots = outer * inner * ys
    shards = xs * ks
    rows, width = tokens.shape[1:]
    o, i, y = lax.axis_index("o"), lax.axis_index("i"), lax.axis_index("y")
    shard = lax.axis_index("x") * ks + lax.axis_index("k")
    place = (o * inner + i) * ys + y
    heads = -(-HEADS // spots)
    span = heads * HEAD_DIM
    padded = spots * span
    part = qkv_weight.shape[0]
    hidden = expand_weight.shape[1]
    piece = hidden // (shards * inner)
    every = (("o", "i", "y"), (outer, inner, ys))
    ctx = (("o", "i"), (outer, inner), "y")
    group = (("i", "x"), (inner, xs), "k")
    pair = (("x",), (xs,), "k")
    own = tokens[0]
    own_grad = cotangent[0]

    def columns(values, count):
        wide = values.reshape(values.shape[:-1] + (count, width))
        wide = jnp.pad(wide, [(0, 0)] * (wide.ndim - 1) + [(0, padded - width)])
        return lax.dynamic_slice_in_dim(wide, place * span, span, axis=wide.ndim - 1)

    qkv_bias = jnp.concatenate(
        [columns(query_bias, 1)[0], jnp.zeros((span,), F32), columns(value_bias, 1)[0]]
    )
    gathered, qkv_columns, expand_columns = first_gather(
        own, qkv_weight, expand_weight, span, [ctx, pair], (xs, ks), every, piece, 0
    )
    sequence = gathered.reshape(spots * rows, width)
    qkv_columns = qkv_columns.reshape(width, 3 * span)

    def doubled(values, axis_name):
        came = lax.ppermute(values, axis_name, [(0, 1), (1, 0)])
        return jnp.where(
            lax.axis_index(axis_name) == 0, jnp.stack([values, came]), jnp.stack([came, values])
        )

    def over_group(values):
        near = doubled(values, "x")
        near = doubled(near, "i")
        far = lax.ppermute(near, "k", [(0, 1), (1, 0)])
        first = lax.axis_index("k") == 0
        both = jnp.stack([jnp.where(first, near, far), jnp.where(first, far, near)], axis=2)
        return both.reshape(-1, width)

    sequence, out_own = lax.optimization_barrier((sequence, out_weight))
    out_far = lax.ppermute(out_own, "x", [(0, 1), (1, 0)])
    expand_own_bias = lax.dynamic_slice_in_dim(
        expand_bias, (shard * inner + i) * piece, piece, axis=0
    )

    order_row = block_order[0]
    blocks = order_row.shape[0]
    inv = jnp.sum(
        jnp.where(
            order_row[:, None] == jnp.arange(blocks, dtype=jnp.int32)[None, :],
            jnp.arange(blocks, dtype=jnp.int32)[:, None],
            0,
        ),
        axis=0,
    ).astype(jnp.int32)
    normed_low = layer_norm(sequence.astype(F32), first_gain, first_shift).astype(BF16)
    qkv = (matmul(normed_low, qkv_columns) + qkv_bias).astype(BF16)
    attended, attended_bf, log_sum = attend(inv, qkv, heads)
    def cut(values, axis_name, dim):
        index, size = lax.axis_index(axis_name), sizes[axis_name]
        return [
            lax.dynamic_index_in_dim(values, lax.rem(index + s, size), axis=dim, keepdims=False)
            for s in range(size)
        ]

    def added(pieces, axis_name):
        size = sizes[axis_name]
        total = pieces[0].astype(F32)
        for step in range(1, size):
            ring = [(d, (d + step) % size) for d in range(size)]
            total = total + lax.ppermute(pieces[step], axis_name, ring).astype(F32)
        return total.astype(BF16)

    cell = width // spots
    cuts = spots // (2 * shards)

    def cut_columns(left, right):
        local = onto(left, right).astype(BF16)
        return cut(local.reshape(outer, inner, ys, cell, right.shape[1]), "y", 2)

    def owned(local):
        kept, sent = cut(local, "i", 0)
        came = lax.ppermute(sent, "i", [(0, 1), (1, 0)])
        local = jnp.where(i == 0, jnp.stack([kept, came]), jnp.stack([came, kept]))
        return local.transpose(0, 2, 1).reshape(-1, cell).astype(F32)

    (
        attended_low,
        group_low,
        group_grad,
        hidden_low,
        expanded_low,
        result,
        grad_middle,
        middle_low,
        row_sums,
        hidden_sums,
        grad_heads,
    ) = middle_part(
        attended_bf.reshape(spots, rows, span),
        own,
        own_grad,
        out_own,
        out_far,
        expand_columns,
        shrink_weight,
        [
            v[None]
            for v in (out_bias, expand_own_bias, shrink_bias, second_gain, second_shift)
        ],
        every,
        group,
        1,
    )
    group_low, group_grad = group_low.reshape(-1, width), group_grad.reshape(-1, width)
    hidden_low, expanded_low = hidden_low.reshape(-1, piece), expanded_low.reshape(-1, piece)
    inputs = own.astype(F32)
    grad_heads = grad_heads.reshape(spots * rows, span)
    shrink_cut = cut_columns(group_grad, hidden_low)
    expand_cut = onto(group_low, expanded_low).astype(BF16)
    expand_cut = expand_cut.reshape(shards, part, cuts, piece // cuts).transpose(0, 2, 1, 3)
    expand_cut = cut(expand_cut.reshape(outer, ys, part, piece // cuts), "y", 1)
    grad_heads, shrink_cut, expand_cut = lax.optimization_barrier(
        (grad_heads, shrink_cut, expand_cut)
    )

    dqkv = attend_back(inv, qkv, grad_heads, attended, log_sum, heads)
    shrink_half, expand_half = added(shrink_cut, "y"), added(expand_cut, "y")
    shrink_cut, expand_cut = cut(shrink_half, "o", 0), cut(expand_half, "o", 0)
    dqkv, shrink_cut, expand_cut = lax.optimization_barrier((dqkv, shrink_cut, expand_cut))
    norm_partial = against(dqkv, qkv_columns).astype(BF16)
    qkv_partial = onto(normed_low, dqkv).astype(BF16)
    shrink_whole, expand_whole = added(shrink_cut, "o"), added(expand_cut, "o")
    middle_group, att_group = side_gather(
        middle_low, attended_low, group, ("i", "x", "k"), (inner, xs, ks), 4
    )
    middle_group = middle_group.reshape(-1, width)
    outw_cut = cut_columns(middle_group, att_group.reshape(middle_group.shape[0], -1))
    grad_normed_one, qkv_cells = scatter(
        [
            norm_partial.reshape(outer * inner, ys, rows, width),
            qkv_partial.reshape(xs, ks, part, 3 * span),
        ],
        [ctx, pair],
        5,
    )
    unused, first_back = jax.vjp(layer_norm, inputs, first_gain, first_shift)
    grad_first_input, grad_first_gain, grad_first_shift = first_back(grad_normed_one)
    grad_inputs = grad_middle + grad_first_input

    grad_shrink = owned(shrink_whole)
    axes = ("o", "i", "y", "x", "k")
    routes = []
    for so, si, sy, sf in itertools.product(*map(range, (outer, inner, ys, shards))):
        index = so * ys + sy
        spot = sf * (spots // shards) + si * cuts + index % cuts
        routes.append((((so * inner + si) * ys + sy) * shards + sf, spot * shards + index // cuts))
    grad_expand = lax.ppermute(expand_whole, axes, routes).astype(F32)
    grad_outw = owned(added(cut(added(outw_cut, "y"), "o", 0), "o"))

    def placed(values, start, size):
        return lax.dynamic_update_slice_in_dim(jnp.zeros((size,), F32), values, start, axis=0)

    dqkv_sums = jnp.sum(dqkv.astype(F32), axis=0)
    small = [
        placed(dqkv_sums[:span], place * span, padded),
        placed(dqkv_sums[2 * span :], place * span, padded),
        row_sums[0],
        placed(
            hidden_sums[0], (shard * inner + i) * piece, hidden
        ),
        row_sums[1],
        grad_first_gain,
        grad_first_shift,
        row_sums[2],
        row_sums[3],
    ]
    lengths = [s.shape[0] for s in small]
    devices = spots * shards
    lanes = 128 * (-(-sum(lengths) // (devices * 1024)))
    line = jnp.concatenate(small)
    line = jnp.pad(line, (0, devices * 8 * lanes - line.shape[0])).reshape(devices, 8, lanes)
    share = 3 * width // spots
    qkv_blocks = qkv_cells.astype(BF16).T.reshape(3 * heads, HEAD_DIM, part)
    line, routed = last_exchange(
        line, qkv_blocks, axes, (outer, inner, ys, xs, ks), spots, heads, share, 6
    )
    line = line.reshape(-1)
    start = share * place - HEAD_DIM * ((share * place) // HEAD_DIM)
    grad_qkv = lax.dynamic_slice_in_dim(routed.reshape(-1, part), start, share, axis=0)
    grad_qkv = grad_qkv.T.astype(F32)
    summed = []
    start = 0
    for length in lengths:
        summed.append(line[start : start + length])
        start += length
    summed[0] = summed[0][:width]
    summed[1] = summed[1][:width]
    return (
        result[None],
        grad_inputs[None],
        grad_qkv,
        grad_outw,
        grad_expand,
        grad_shrink,
        *summed,
    )


def solution(mesh):
    spots, shards = mesh.shape["ctx"], mesh.shape["fsdp"]
    sizes = {"o": spots // 4, "i": 2, "y": 2, "x": shards // 2, "k": 2}
    fine = Mesh(mesh.devices.reshape(tuple(sizes.values())), tuple(sizes))
    seq, pos = ("x", "k"), ("o", "i", "y")
    weight = P(seq, None)
    placed = (
        P(seq, pos, None),
        P(seq, None),
        weight,
        P(),
        P(),
        weight,
        P(),
        weight,
        P(),
        weight,
        P(),
        P(),
        P(),
        P(),
        P(),
        P(seq, pos, None),
    )
    given = (P(seq, pos, None),) * 2 + (P(seq, pos),) * 4 + (P(),) * 9
    return jax.shard_map(
        functools.partial(body, sizes),
        mesh=fine,
        in_specs=placed,
        out_specs=given,
        check_vma=False,
    )
```

```python
import functools
import itertools

import jax
import jax.numpy as jnp
from jax import lax
from jax.experimental import pallas as pl
from jax.experimental.pallas import tpu as pltpu
from jax.sharding import Mesh
from jax.sharding import PartitionSpec as P

HEADS = 25
HEAD_DIM = 64
EPSILON = 1e-05
MESH = pl.DeviceIdType.MESH
F32 = jnp.float32
BF16 = jnp.bfloat16
ANY = pl.BlockSpec(memory_space=pl.ANY)
VMEM = pl.BlockSpec(memory_space=pltpu.VMEM)


def offsets(sizes):
    return [o for o in itertools.product(*(range(s) for s in sizes)) if any(o)]


def moved(axes, sizes, offset, sign=1):
    return {
        a: lax.rem(lax.axis_index(a) + (o if sign > 0 else s - o), s)
        for a, s, o in zip(axes, sizes, offset)
    }


def flat(place, axes, sizes):
    index = 0
    for a, s in zip(axes, sizes):
        index = index * s + place[a]
    return index


def own_place(axes):
    return {a: lax.axis_index(a) for a in axes}


def greet(peers):
    barrier = pltpu.get_barrier_semaphore()
    for peer in peers:
        pl.semaphore_signal(barrier, inc=1, device_id=peer, device_id_type=MESH)
    pl.semaphore_wait(barrier, len(peers))


def remote(src, dst, send, recv, peer):
    return pltpu.make_async_remote_copy(
        src_ref=src,
        dst_ref=dst,
        send_sem=send,
        recv_sem=recv,
        device_id=peer,
        device_id_type=MESH,
    )


class Gather:
    def __init__(self, axes, sizes, pair, source, out, send, recv, local):
        self.axes, self.sizes = axes, sizes
        self.offs = offsets(sizes)
        self.side = lax.axis_index(pair)
        self.mate = {pair: 1 - self.side}
        self.source, self.out, self.send, self.recv, self.local = source, out, send, recv, local
        self.started = []

    def peers(self):
        return [moved(self.axes, self.sizes, o) for o in self.offs] + [self.mate]

    def mine(self):
        return self.out.at[flat(own_place(self.axes), self.axes, self.sizes), self.side]

    def start(self):
        pltpu.make_async_copy(self.source, self.mine(), self.local).start()
        last = len(self.offs)
        for t, peer in enumerate(self.peers()):
            copy = remote(self.source, self.mine(), self.send.at[t], self.recv.at[t], peer)
            copy.start()
            self.started.append(copy)

    def hand_on(self):
        last = len(self.offs)
        for t, off in enumerate(self.offs):
            came = flat(moved(self.axes, self.sizes, off, -1), self.axes, self.sizes)
            block = self.out.at[came, self.side]
            remote(self.source, block, self.send.at[t], self.recv.at[t], self.mate).wait_recv()
            slot = last + 1 + t
            copy = remote(block, block, self.send.at[slot], self.recv.at[slot], self.mate)
            copy.start()
            self.started.append(copy)

    def finish(self):
        last = len(self.offs)
        me = flat(own_place(self.axes), self.axes, self.sizes)
        pltpu.make_async_copy(self.source, self.mine(), self.local).wait()
        block = self.out.at[me, 1 - self.side]
        remote(self.source, block, self.send.at[last], self.recv.at[last], self.mate).wait_recv()
        for t, off in enumerate(self.offs):
            came = flat(moved(self.axes, self.sizes, off, -1), self.axes, self.sizes)
            slot = last + 1 + t
            block = self.out.at[came, 1 - self.side]
            remote(
                self.source, block, self.send.at[slot], self.recv.at[slot], self.mate
            ).wait_recv()
        for copy in self.started:
            copy.wait_send()


def gather_shape(block, spec):
    group = 1
    for s in spec[1]:
        group *= s
    return jax.ShapeDtypeStruct((group, 2) + block.shape, block.dtype)


def gather_scratch(spec):
    group = 1
    for s in spec[1]:
        group *= s
    return [
        pltpu.SemaphoreType.DMA((2 * group,)),
        pltpu.SemaphoreType.DMA((2 * group,)),
        pltpu.SemaphoreType.DMA,
    ]


def sent_estimate(size):
    return pl.CostEstimate(flops=0, bytes_accessed=20 * size, transcendentals=0)


def first_kernel(
    specs,
    shard_sizes,
    ctx_axes,
    ctx_sizes,
    own,
    qkv_weight,
    weight,
    all_tokens,
    all_columns,
    pieces,
    qkv_whole,
    columns,
    whole,
    cut,
    *sems,
):
    axes = ("x", "k")
    offs = offsets(shard_sizes)
    tokens = Gather(*specs[0], own, all_tokens, *sems[0:3])
    heads = Gather(*specs[1], columns, all_columns, *sems[3:6])
    read, qkv_read, send, recv, local = sems[6:11]
    qkv_fetch = pltpu.make_async_copy(qkv_weight, qkv_whole, qkv_read)
    qkv_fetch.start()
    fetch = pltpu.make_async_copy(weight, whole, read)
    fetch.start()
    greet(tokens.peers() + heads.peers() + [moved(axes, shard_sizes, o) for o in offs])
    tokens.start()
    qkv_fetch.wait()
    place = flat(own_place(ctx_axes), ctx_axes, ctx_sizes)
    rows, span = columns.shape[0], columns.shape[1] // 3
    width = qkv_whole.shape[1] // 3
    for spot in range(-(-width // span)):

        @pl.when(place == spot)
        def _(spot=spot):
            size = min(span, width - spot * span)
            for section in range(3):
                low = section * width + spot * span
                if size < span:
                    columns[:, section * span : (section + 1) * span] = jnp.zeros(
                        (rows, span), BF16
                    )
                columns[:, section * span : section * span + size] = qkv_whole[:, low : low + size]

    @pl.when(place * span >= width)
    def _():
        columns[...] = jnp.zeros(columns.shape, BF16)

    heads.start()
    fetch.wait()
    width = cut.shape[2]
    inner = lax.axis_index("i")
    for half in range(2):

        @pl.when(inner == half)
        def _():
            for f in range(cut.shape[0]):
                low = (2 * f + half) * width
                cut[f] = whole[:, low : low + width]

    me = flat(own_place(axes), axes, shard_sizes)
    here = pltpu.make_async_copy(cut.at[me], pieces.at[me], local)
    here.start()
    started = []
    for t, off in enumerate(offs):
        peer = moved(axes, shard_sizes, off)
        there = flat(peer, axes, shard_sizes)
        copy = remote(cut.at[there], pieces.at[me], send.at[t], recv.at[t], peer)
        copy.start()
        started.append(copy)
    heads.hand_on()
    tokens.hand_on()
    here.wait()
    for t, off in enumerate(offs):
        peer = moved(axes, shard_sizes, off, -1)
        came = flat(peer, axes, shard_sizes)
        remote(cut.at[came], pieces.at[came], send.at[t], recv.at[t], peer).wait_recv()
    for copy in started:
        copy.wait_send()
    heads.finish()
    tokens.finish()


def first_gather(own, qkv_weight, weight, span, specs, shard_sizes, every, piece, ident):
    shards = shard_sizes[0] * shard_sizes[1]
    part = weight.shape[0]
    columns = jax.ShapeDtypeStruct((part, 3 * span), BF16)
    shapes = [
        gather_shape(own, specs[0]),
        gather_shape(columns, specs[1]),
        jax.ShapeDtypeStruct((shards, part, piece), BF16),
    ]
    return pl.pallas_call(
        functools.partial(first_kernel, specs, shard_sizes, *every),
        out_shape=shapes,
        in_specs=[VMEM, ANY, ANY],
        out_specs=[ANY] * 3,
        scratch_shapes=[
            pltpu.VMEM(qkv_weight.shape, BF16),
            pltpu.VMEM(columns.shape, BF16),
            pltpu.VMEM(weight.shape, BF16),
            pltpu.VMEM((shards, part, piece), BF16),
            *gather_scratch(specs[0]),
            *gather_scratch(specs[1]),
            pltpu.SemaphoreType.DMA,
            pltpu.SemaphoreType.DMA,
            pltpu.SemaphoreType.DMA((shards,)),
            pltpu.SemaphoreType.DMA((shards,)),
            pltpu.SemaphoreType.DMA,
        ],
        name="first%d" % ident,
        compiler_params=pltpu.CompilerParams(collective_id=ident, has_side_effects=True),
        cost_estimate=sent_estimate(sum(s.size for s in shapes)),
    )(own, qkv_weight, weight)


def pieces_out(axes, sizes, source, out, send, recv):
    me = flat(own_place(axes), axes, sizes)
    started = []
    for t, off in enumerate(offsets(sizes)):
        peer = moved(axes, sizes, off)
        copy = remote(
            source.at[flat(peer, axes, sizes)], out.at[me], send.at[t], recv.at[t], peer
        )
        copy.start()
        started.append(copy)
    return started


def pieces_in(axes, sizes, source, out, send, recv, started):
    for t, off in enumerate(offsets(sizes)):
        peer = moved(axes, sizes, off, -1)
        came = flat(peer, axes, sizes)
        remote(source.at[came], out.at[came], send.at[t], recv.at[t], peer).wait_recv()
    for copy in started:
        copy.wait_send()


def normed(values):
    center = jnp.mean(values, axis=-1, keepdims=True)
    centred = values - center
    spread = jnp.mean(centred * centred, axis=-1, keepdims=True)
    scale = lax.rsqrt(spread + EPSILON)
    return centred * scale, scale


def norm_back(grad, gain, plain, scale):
    inner = grad * gain
    return scale * (
        inner
        - jnp.mean(inner, axis=-1, keepdims=True)
        - plain * jnp.mean(inner * plain, axis=-1, keepdims=True)
    )


def by_columns(left, right, out):
    tokens = left.shape[0] * left.shape[1] * left.shape[2]
    cell = out.shape[1]
    wide = 400 // cell
    others = right[...].reshape(tokens, right.shape[-1])
    for c in range(left.shape[3] // 400):
        terms = tn(left[:, :, :, c * 400 : (c + 1) * 400].reshape(tokens, 400), others)
        for n in range(wide):
            out[c * wide + n] = terms[n * cell : (n + 1) * cell].astype(BF16)


def middle_kernel(
    every,
    spec,
    pieces,
    own,
    own_grad,
    out_own,
    out_far,
    expand,
    shrink,
    out_bias,
    expand_bias,
    shrink_bias,
    gain,
    shift,
    att,
    result,
    grad_middle,
    low_middle,
    sums,
    hidden_sum,
    to_heads,
    expand_half,
    shrink_terms,
    came,
    out_w,
    expand_w,
    shrink_w,
    mid,
    c_own,
    c_all,
    e_all,
    gh,
    u_all,
    gz_all,
    part,
    first,
    summed,
    last,
    part_two,
    first_two,
    summed_two,
    last_two,
    cut,
    expand_terms,
    expand_came,
    send,
    recv,
    c_send,
    c_recv,
    c_local,
    e_send,
    e_recv,
    e_local,
    w_sem,
    w_send,
    w_recv,
    r_send,
    r_recv,
    s_send,
    s_recv,
    h_send,
    h_recv,
    y_send,
    y_recv,
):
    axes, sizes = every
    y = lax.axis_index("y")
    x, k, inner = lax.axis_index("x"), lax.axis_index("k"), lax.axis_index("i")
    mate = {"k": 1 - k}
    shard = 2 * x + k
    part_rows = out_own.shape[0]
    width = own.shape[1]
    rows = own.shape[0]
    piece = expand.shape[2]

    def chip(t):
        ti, tx = lax.rem(inner + t // 2, 2), lax.rem(x + t % 2, 2)
        return 2 * ti + tx, {"i": ti, "x": tx}

    loads = [
        pltpu.make_async_copy(out_own, out_w.at[pl.ds(shard * part_rows, part_rows)], w_sem.at[0]),
        pltpu.make_async_copy(
            out_far, out_w.at[pl.ds((shard ^ 2) * part_rows, part_rows)], w_sem.at[1]
        ),
        pltpu.make_async_copy(shrink.at[pl.ds(inner * piece, piece)], shrink_w, w_sem.at[2]),
    ]
    for f in range(expand.shape[0]):
        loads.append(
            pltpu.make_async_copy(
                expand.at[f], expand_w.at[pl.ds(f * part_rows, part_rows)], w_sem.at[3 + f]
            )
        )
    for copy in loads:
        copy.start()
    greet([moved(axes, sizes, o) for o in offsets(sizes)] + [chip(t)[1] for t in range(1, 4)] + [mate])

    started = pieces_out(axes, sizes, pieces, came, send, recv)
    out_sent = []
    for n, (source, owner) in enumerate(((out_own, shard), (out_far, shard ^ 2))):
        copy = remote(
            source, out_w.at[pl.ds(owner * part_rows, part_rows)], w_send.at[n], w_recv.at[n], mate
        )
        copy.start()
        out_sent.append(copy)
    e_gather = Gather(*spec, own_grad, e_all, e_send, e_recv, e_local)
    e_gather.start()
    here = flat(own_place(axes), axes, sizes)
    came[here] = pieces[here]
    pieces_in(axes, sizes, pieces, came, send, recv, started)
    span = came.shape[2]
    for d in range(came.shape[0]):
        low, high = d * span, min((d + 1) * span, width)
        if low < high:
            att[:, low:high] = came[d, :, : high - low]
    for copy in loads[:2]:
        copy.wait()
    for n, owner in enumerate((shard ^ 1, shard ^ 3)):
        remote(
            out_own,
            out_w.at[pl.ds(owner * part_rows, part_rows)],
            w_send.at[n],
            w_recv.at[n],
            mate,
        ).wait_recv()

    mid[...] = (
        own[...].astype(F32)
        + jnp.dot(att[...], out_w[...], preferred_element_type=F32)
        + out_bias[...]
    )
    plain, scale = normed(mid[...])
    c_own[...] = (plain * gain[...] + shift[...]).astype(BF16)
    c_gather = Gather(*spec, c_own, c_all, c_send, c_recv, c_local)
    c_gather.start()
    e_gather.hand_on()
    e_gather.finish()
    for copy in loads[2:]:
        copy.wait()

    def both(ref, place):
        return ref[place].reshape(2 * rows, ref.shape[3])

    def slopes(t, unused):
        place, unused_peer = chip(t)
        gh[place] = nt(both(e_all, place), shrink_w[...])
        return unused

    lax.fori_loop(0, 4, slopes, 0)
    hidden_sum[...] = jnp.zeros(hidden_sum.shape, F32)

    def c_wait(t):
        place, peer = chip(t)
        block = c_all.at[place, 1 - k]
        remote(c_own, block, c_send.at[3 + t], c_recv.at[3 + t], mate).wait_recv()

    def c_hand_on(t):
        place, peer = chip(t)
        block = c_all.at[place, k]
        remote(c_own, block, c_send.at[t - 1], c_recv.at[t - 1], mate).wait_recv()
        remote(block, block, c_send.at[3 + t], c_recv.at[3 + t], mate).start()

    def to_mate(t, source, target, sends, recvs):
        place, peer = chip(t)
        return remote(source.at[place, 1 - k], target.at[t], sends.at[t], recvs.at[t], mate)

    def to_chip(t, source, target, sends, recvs):
        place, peer = chip(t)
        return remote(
            source.at[t - 1], target.at[t - 1], sends.at[3 + t], recvs.at[3 + t], peer
        )

    def add_and_send(t, parts, firsts, sums_of, lasts, sends, recvs):
        place, peer = chip(t)
        to_mate(t, parts, firsts, sends, recvs).wait_recv()
        sums_of[t - 1] = (parts[place, k].astype(F32) + firsts[t].astype(F32)).astype(BF16)
        to_chip(t, sums_of, lasts, sends, recvs).start()

    pltpu.make_async_copy(c_own, c_gather.mine(), c_local).wait()

    def feed(t, unused):
        c_wait(t)
        place, peer = chip(t)
        expanded = jnp.dot(both(c_all, place), expand_w[...], preferred_element_type=F32)
        expanded = expanded + expand_bias[...]
        square = expanded * expanded
        bent = jnp.tanh(0.7978845608028654 * (expanded + 0.044715 * square * expanded))
        half = 0.5 * (1.0 + bent)
        u_all[place] = (expanded * half).astype(BF16)
        slope = half + 0.5 * expanded * (1.0 - bent * bent) * (
            0.7978845608028654 * (1.0 + 3 * 0.044715 * square)
        )
        low = (slope * gh[place]).astype(BF16)
        gz_all[place] = low
        hidden_sum[...] += jnp.sum(low.astype(F32), axis=0, keepdims=True)
        back = nt(low, expand_w[...]).astype(BF16)
        part[place] = back.reshape(2, rows, width)
        to_mate(t, part, first, r_send, r_recv).start()

        @pl.when(t < 3)
        def _():
            c_hand_on(t + 1)

        @pl.when(t > 1)
        def _():
            add_and_send(t - 1, part, first, summed, last, r_send, r_recv)

        return unused

    lax.fori_loop(0, 4, feed, 0)
    add_and_send(3, part, first, summed, last, r_send, r_recv)

    parts, cuts = expand.shape[0], expand_terms.shape[0] * 2 // expand.shape[0]
    cut_width = expand_terms.shape[3]
    for f in range(parts):
        terms = tn(
            c_all[:, :, :, f * part_rows : (f + 1) * part_rows].reshape(8 * rows, part_rows),
            gz_all[...].reshape(8 * rows, piece),
        )
        for c in range(cuts):
            index = f * cuts + c
            expand_terms[index // 2, index % 2] = terms[
                :, c * cut_width : (c + 1) * cut_width
            ].astype(BF16)
    y_mate = {"y": 1 - y}
    y_copies = [
        remote(
            expand_terms.at[n, 1 - y], expand_came.at[n], y_send.at[n], y_recv.at[n], y_mate
        )
        for n in range(expand_terms.shape[0])
    ]
    for copy in y_copies:
        copy.start()

    def gathered_sum(parts, firsts, lasts, sends, recvs):
        place, unused_peer = chip(0)
        to_mate(0, parts, firsts, sends, recvs).wait_recv()
        total = parts[place, k].astype(F32) + firsts[0].astype(F32)
        for t in range(1, 4):
            to_chip(t, firsts, lasts, sends, recvs).wait_recv()
            total = total + lasts[t - 1].astype(F32)
        return total

    grad = gathered_sum(part, first, last, r_send, r_recv)
    plain, scale = normed(mid[...])
    grad_mid = own_grad[...].astype(F32) + norm_back(grad, gain[...], plain, scale)
    grad_middle[...] = grad_mid
    low = grad_mid.astype(BF16)
    low_middle[...] = low
    sums[0:1, :] = jnp.sum(low.astype(F32), axis=0, keepdims=True)
    sums[1:2, :] = jnp.sum(own_grad[...].astype(F32), axis=0, keepdims=True)
    sums[2:3, :] = jnp.sum(grad * plain, axis=0, keepdims=True)
    sums[3:4, :] = jnp.sum(grad, axis=0, keepdims=True)
    back = nt(low, out_w[...]).astype(BF16)
    for d in range(cut.shape[0]):
        low_end, high = d * span, min((d + 1) * span, width)
        if high - low_end < span:
            cut[d] = jnp.zeros(cut.shape[1:], cut.dtype)
        if low_end < high:
            cut[d, :, : high - low_end] = back[:, low_end:high]
    head_started = pieces_out(axes, sizes, cut, to_heads, h_send, h_recv)

    def shrunk(t, unused):
        place, peer = chip(t)
        terms = jnp.dot(u_all[place], shrink_w[...], preferred_element_type=F32).astype(BF16)
        part_two[place] = terms.reshape(2, rows, width)
        to_mate(t, part_two, first_two, s_send, s_recv).start()
        return unused

    lax.fori_loop(0, 4, shrunk, 0)
    for t in range(1, 4):
        add_and_send(t, part_two, first_two, summed_two, last_two, s_send, s_recv)
    to_heads[here] = cut[here]
    by_columns(e_all, u_all, shrink_terms)
    result[...] = (
        mid[...] + gathered_sum(part_two, first_two, last_two, s_send, s_recv) + shrink_bias[...]
    ).astype(BF16)
    pieces_in(axes, sizes, cut, to_heads, h_send, h_recv, head_started)
    for n, copy in enumerate(y_copies):
        copy.wait_recv()
        expand_half[n] = (
            expand_terms[n, y].astype(F32) + expand_came[n].astype(F32)
        ).astype(BF16)

    for copy in out_sent + c_gather.started:
        copy.wait_send()
    for t in range(1, 4):
        place, peer = chip(t)
        remote(c_own, c_own, c_send.at[3 + t], c_recv.at[3 + t], mate).wait_send()
    for t in range(4):
        to_mate(t, part, first, r_send, r_recv).wait_send()
        to_mate(t, part_two, first_two, s_send, s_recv).wait_send()
    for t in range(1, 4):
        to_chip(t, summed, last, r_send, r_recv).wait_send()
        to_chip(t, summed_two, last_two, s_send, s_recv).wait_send()
    for copy in y_copies:
        copy.wait_send()


def middle_part(
    pieces, own, own_grad, out_own, out_far, expand, shrink, vectors, every, spec, ident
):
    spots, rows, span = pieces.shape
    width = own.shape[1]
    piece = expand.shape[2]
    outer = every[1][0]
    cuts = outer * 2 // expand.shape[0]
    expand_cut = (outer, 2, expand.shape[1], piece // cuts)
    everyone = jax.ShapeDtypeStruct((4, 2, rows, width), BF16)
    hidden = jax.ShapeDtypeStruct((4, 2 * rows, piece), BF16)
    flat_f32 = jax.ShapeDtypeStruct((rows, width), F32)
    flat_low = jax.ShapeDtypeStruct((rows, width), BF16)

    def scatter_buffers():
        return [
            pltpu.VMEM(everyone.shape, BF16),
            pltpu.VMEM((4, rows, width), BF16),
            pltpu.VMEM((3, rows, width), BF16),
            pltpu.VMEM((3, rows, width), BF16),
        ]

    return pl.pallas_call(
        functools.partial(middle_kernel, every, spec),
        out_shape=[
            flat_low,
            flat_low,
            flat_f32,
            flat_low,
            jax.ShapeDtypeStruct((4, width), F32),
            jax.ShapeDtypeStruct((1, piece), F32),
            jax.ShapeDtypeStruct(pieces.shape, BF16),
            jax.ShapeDtypeStruct(expand_cut[:1] + expand_cut[2:], BF16),
            jax.ShapeDtypeStruct((spots, width // spots, piece), BF16),
        ],
        in_specs=[VMEM] * 3 + [ANY] * 4 + [VMEM] * 5,
        out_specs=[VMEM] * 9,
        scratch_shapes=[
            pltpu.VMEM(pieces.shape, BF16),
            pltpu.VMEM((width, width), BF16),
            pltpu.VMEM((width, piece), BF16),
            pltpu.VMEM((piece, width), BF16),
            pltpu.VMEM((rows, width), F32),
            pltpu.VMEM((rows, width), BF16),
            pltpu.VMEM(everyone.shape, BF16),
            pltpu.VMEM(everyone.shape, BF16),
            pltpu.VMEM(hidden.shape, F32),
            pltpu.VMEM(hidden.shape, BF16),
            pltpu.VMEM(hidden.shape, BF16),
            *scatter_buffers(),
            *scatter_buffers(),
            pltpu.VMEM(pieces.shape, BF16),
            pltpu.VMEM(expand_cut, BF16),
            pltpu.VMEM(expand_cut[:1] + expand_cut[2:], BF16),
            pltpu.SemaphoreType.DMA((spots,)),
            pltpu.SemaphoreType.DMA((spots,)),
            *gather_scratch(spec),
            *gather_scratch(spec),
            pltpu.SemaphoreType.DMA((7,)),
            pltpu.SemaphoreType.DMA((2,)),
            pltpu.SemaphoreType.DMA((2,)),
            pltpu.SemaphoreType.DMA((7,)),
            pltpu.SemaphoreType.DMA((7,)),
            pltpu.SemaphoreType.DMA((7,)),
            pltpu.SemaphoreType.DMA((7,)),
            pltpu.SemaphoreType.DMA((spots,)),
            pltpu.SemaphoreType.DMA((spots,)),
            pltpu.SemaphoreType.DMA(expand_cut[:1]),
            pltpu.SemaphoreType.DMA(expand_cut[:1]),
        ],
        name="middle%d" % ident,
        compiler_params=pltpu.CompilerParams(
            collective_id=ident, has_side_effects=True, vmem_limit_bytes=67_000_000
        ),
        cost_estimate=pl.CostEstimate(
            flops=8 * rows * 8 * width * piece,
            bytes_accessed=100 * rows * width * 2,
            transcendentals=8 * rows * piece,
        ),
    )(pieces, own, own_grad, out_own, out_far, expand, shrink, *vectors)


class Owned:
    def __init__(self, outer, terms, out, came, half, last, whole, y_sems, o_sems, i_sems):
        self.outer = outer
        self.terms, self.out = terms, out
        self.came, self.half, self.last, self.whole = came, half, last, whole
        self.y_sems, self.o_sems, self.i_sems = y_sems, o_sems, i_sems
        self.o, self.i, self.y = (lax.axis_index(a) for a in ("o", "i", "y"))

    def start(self):
        mate = {"y": 1 - self.y}
        self.first = [
            remote(
                self.terms.at[2 * n + 1 - self.y],
                self.came.at[n],
                self.y_sems.at[0, n],
                self.y_sems.at[1, n],
                mate,
            )
            for n in range(2 * self.outer)
        ]
        for copy in self.first:
            copy.start()

    def over_o(self):
        for n, copy in enumerate(self.first):
            copy.wait_recv()
            self.half[n // 2, n % 2] = (
                self.terms[2 * n + self.y].astype(F32) + self.came[n].astype(F32)
            ).astype(BF16)
        self.second = []
        for step in range(1, self.outer):
            there = lax.rem(self.o + step, self.outer)
            copy = remote(
                self.half.at[there],
                self.last.at[step - 1],
                self.o_sems.at[0, step],
                self.o_sems.at[1, step],
                {"o": there},
            )
            copy.start()
            self.second.append(copy)

    def over_i(self):
        total = self.half[self.o].astype(F32)
        for step, copy in enumerate(self.second):
            copy.wait_recv()
            total = total + self.last[step].astype(F32)
        self.whole[...] = total.astype(BF16)
        self.third = remote(
            self.whole.at[1 - self.i],
            self.out.at[self.i],
            self.i_sems.at[0],
            self.i_sems.at[1],
            {"i": 1 - self.i},
        )
        self.third.start()
        self.out[self.i] = self.whole[self.i]

    def finish(self):
        self.third.wait_recv()
        for copy in self.first + self.second + [self.third]:
            copy.wait_send()


def owned_scratch(outer, cell, rows):
    return [
        pltpu.VMEM((2 * outer, cell, rows), BF16),
        pltpu.VMEM((outer, 2, cell, rows), BF16),
        pltpu.VMEM((max(outer - 1, 1), 2, cell, rows), BF16),
        pltpu.VMEM((2, cell, rows), BF16),
        pltpu.SemaphoreType.DMA((2, 2 * outer)),
        pltpu.SemaphoreType.DMA((2, outer)),
        pltpu.SemaphoreType.DMA((2,)),
    ]


def final_kernel(
    axes,
    sizes,
    heads,
    share,
    dqkv,
    columns,
    normed_low,
    shrink_terms,
    low_middle,
    att,
    own,
    grad_middle,
    gain,
    row_sums,
    hidden_sum,
    grad_inputs,
    routed,
    shrink_out,
    outw_out,
    query_out,
    value_out,
    rows_out,
    hidden_out,
    part,
    first,
    last,
    normed_part,
    q_part,
    q_first,
    q_sum,
    q_last,
    blocks,
    gy_all,
    att_cut,
    att_all,
    outw_terms,
    line,
    line_came,
    line_out,
    r_send,
    r_recv,
    q_send,
    q_recv,
    hop,
    land,
    a_send,
    a_recv,
    l_send,
    l_recv,
    g_send,
    g_recv,
    g_local,
    load_sem,
    *owned,
):
    outer, inner, ys, xs, ks = sizes
    o, i, y, x, k = (lax.axis_index(a) for a in axes)
    offs = offsets(sizes)
    chips = outer * inner
    spots = chips * ys
    place = (o * inner + i) * ys + y
    shard = x * ks + k
    me = place * xs * ks + shard
    rows, width = own.shape
    span = heads * HEAD_DIM
    y_mate, k_mate, x_mate = {"y": 1 - y}, {"k": 1 - k}, {"x": 1 - x}
    shrink = Owned(outer, shrink_terms, shrink_out, *owned[:7])
    outw = Owned(outer, outw_terms, outw_out, *owned[7:])

    def load_normed(n):
        some = normed_part.shape[0]
        return pltpu.make_async_copy(
            normed_low.at[pl.ds(n * some, some)], normed_part, load_sem
        )

    load_normed(0).start()
    greet([moved(axes, sizes, off) for off in offs])

    group = (("i", "x", "k"), (inner, xs, ks))
    side = Gather(("i", "x"), (inner, xs), "k", low_middle, gy_all, g_send, g_recv, g_local)
    side.start()
    cell = att_cut.shape[2]
    for half in range(inner):
        for f in range(xs * ks):
            low = (f * inner + half) * cell
            att_cut[half * xs * ks + f] = att[:, low : low + cell]
    att_started = pieces_out(*group, att_cut, att_all, a_send, a_recv)
    here = (i * xs + x) * ks + k
    att_all[here] = att_cut[here]

    def chip(t):
        to, ti = lax.rem(o + t // inner, outer), lax.rem(i + t % inner, inner)
        return to * inner + ti, {"o": to, "i": ti}

    def back_chip(t):
        to = lax.rem(o + outer - t // inner, outer)
        ti = lax.rem(i + inner - t % inner, inner)
        return to * inner + ti

    def to_mate(t):
        return remote(
            part.at[chip(t)[0], 1 - y], first.at[t], r_send.at[t], r_recv.at[t], y_mate
        )

    def to_chip(t):
        slot = chips + t - 1
        return remote(
            part.at[chip(t)[0], y], last.at[t - 1], r_send.at[slot], r_recv.at[slot], chip(t)[1]
        )

    def terms(step, unused):
        t = lax.rem(step + 1, chips)
        spot = chip(t)[0]
        at = pl.multiple_of(spot * 2 * rows, 2 * rows)
        values = nt(dqkv[pl.ds(at, 2 * rows), :], columns[...]).astype(BF16)
        part[spot] = values.reshape(2, rows, width)
        to_mate(t).start()
        return unused

    lax.fori_loop(0, chips, terms, 0)
    shrink.start()

    quarter = q_part.shape[3]
    some = normed_part.shape[0]
    pieces = dqkv.shape[0] // some
    for section in range(3):
        low = section * span
        values = 0.0
        for n in range(pieces):
            if n or section == 0 or pieces > 1:
                copy = load_normed(n)
                if n or section:
                    copy.start()
                copy.wait()
            values = values + tn(
                dqkv[n * some : (n + 1) * some, low : low + span], normed_part[...]
            )
        for f in range(xs * ks):
            q_part[f // ks, f % ks, low : low + span, :] = values[
                :, f * quarter : (f + 1) * quarter
            ].astype(BF16)
    q_copies = [
        remote(q_part.at[1 - x, 1 - k], q_first.at[1], q_send.at[1], q_recv.at[1], k_mate),
        remote(q_part.at[x, 1 - k], q_first.at[0], q_send.at[0], q_recv.at[0], k_mate),
    ]
    for copy in q_copies:
        copy.start()

    def add_and_send(step, unused):
        t = step + 1
        to_mate(t).wait_recv()
        spot = chip(t)[0]
        part[spot, y] = (part[spot, y].astype(F32) + first[t].astype(F32)).astype(BF16)
        to_chip(t).start()
        return unused

    lax.fori_loop(0, chips - 1, add_and_send, 0)
    q_copies[0].wait_recv()
    q_sum[...] = (q_part[1 - x, k].astype(F32) + q_first[1].astype(F32)).astype(BF16)
    q_over = remote(q_sum, q_last, q_send.at[2], q_recv.at[2], x_mate)
    q_over.start()

    side.hand_on()
    pieces_in(*group, att_cut, att_all, a_send, a_recv, att_started)
    side.finish()
    by_columns(gy_all, att_all, outw_terms)
    outw.start()

    q_copies[1].wait_recv()
    q_over.wait_recv()
    total = q_part[x, k].astype(F32) + q_first[0].astype(F32) + q_last[...].astype(F32)
    blocks[...] = total.astype(BF16).reshape(blocks.shape)

    def where(spot):
        return {
            "o": spot // (inner * ys),
            "i": (spot // ys) % inner,
            "y": spot % ys,
        }

    def each_sent(act):
        for section in range(3):
            for h in range(heads):
                head = place * heads + h
                block = section * HEADS + head
                low = (block * HEAD_DIM) // share
                high = (block * HEAD_DIM + HEAD_DIM - 1) // share
                index = section * heads + h
                for which, owner, needed in (
                    (0, low, head < HEADS),
                    (1, high, (head < HEADS) & (high != low)),
                ):

                    @pl.when(needed)
                    def _(which=which, owner=owner, block=block, index=index):
                        act(index, 2 * index + which, owner, block - (share * owner) // HEAD_DIM)

    def block_copy(index, slot, owner, target):
        return remote(
            blocks.at[index], routed.at[target], hop.at[slot], land.at[target], where(owner)
        )

    def send_block(index, slot, owner, target):
        @pl.when(owner != place)
        def _():
            block_copy(index, slot, owner, target).start()

        @pl.when(owner == place)
        def _():
            routed[target] = blocks[index]

    def sent_block(index, slot, owner, target):
        @pl.when(owner != place)
        def _():
            block_copy(index, slot, owner, target).wait_send()

    each_sent(send_block)

    to_mate(0).wait_recv()
    grad = part[chip(0)[0], y].astype(F32) + first[0].astype(F32)
    for t in range(1, chips):
        to_chip(t).wait_recv()
        grad = grad + last[t - 1].astype(F32)
    plain, scale = normed(own[...].astype(F32))
    grad_inputs[...] = grad_middle[...] + norm_back(grad, gain[...], plain, scale)

    def fill(base, values):
        size = values.shape[1]
        for n in range(-(-size // 128)):
            low, high = n * 128, min(n * 128 + 128, size)
            line[pl.ds(base + n, 1), 0 : high - low] = values[:, low:high]

    q_rows, w_rows = -(-span // 128), -(-width // 128)
    piece = hidden_sum.shape[1]
    p_rows = -(-piece // 128)
    value_base = spots * q_rows
    rows_base = 2 * spots * q_rows
    hidden_base = rows_base + 6 * w_rows
    line[...] = jnp.zeros(line.shape, F32)
    fill(place * q_rows, jnp.sum(dqkv[:, 0:span].astype(F32), axis=0, keepdims=True))
    fill(
        value_base + place * q_rows,
        jnp.sum(dqkv[:, 2 * span : 3 * span].astype(F32), axis=0, keepdims=True),
    )
    for n in range(4):
        fill(rows_base + n * w_rows, row_sums[n : n + 1, :])
    fill(rows_base + 4 * w_rows, jnp.sum(grad * plain, axis=0, keepdims=True))
    fill(rows_base + 5 * w_rows, jnp.sum(grad, axis=0, keepdims=True))
    fill(hidden_base + (shard * inner + i) * p_rows, hidden_sum[...])
    line_rows = line_came.shape[1]

    def share_of(ref, device):
        return ref.at[pl.ds(pl.multiple_of(device * line_rows, line_rows), line_rows)]

    line_started = []
    for t, off in enumerate(offs):
        peer = moved(axes, sizes, off)
        device = flat(peer, axes, sizes)
        copy = remote(
            share_of(line, device), line_came.at[t], l_send.at[t], l_recv.at[t], peer
        )
        copy.start()
        line_started.append(copy)
    shrink.over_o()
    outw.over_o()
    for copy in line_started:
        copy.wait_recv()
    mine = pl.ds(pl.multiple_of(me * line_rows, line_rows), line_rows)
    line_out[mine, :] = line[mine, :] + jnp.sum(line_came[...], axis=0)
    count = len(offs)
    for t, off in enumerate(offs):
        peer = moved(axes, sizes, off)
        copy = remote(
            share_of(line_out, me),
            share_of(line_out, me),
            l_send.at[count + t],
            l_recv.at[count + t],
            peer,
        )
        copy.start()
        line_started.append(copy)
    shrink.over_i()
    outw.over_i()

    base = (share * place) // HEAD_DIM
    for slot in range(routed.shape[0]):
        block = base + slot
        owner = (block % HEADS) // heads

        @pl.when((block * HEAD_DIM < share * (place + 1)) & (owner != place))
        def _(slot=slot):
            remote(
                blocks.at[0], routed.at[slot], hop.at[0], land.at[slot], where(place)
            ).wait_recv()

    for t, off in enumerate(offs):
        peer = moved(axes, sizes, off, -1)
        block = share_of(line_out, flat(peer, axes, sizes))
        remote(block, block, l_send.at[count + t], l_recv.at[count + t], peer).wait_recv()

    def take(base, ref, row, start, size):
        for n in range(-(-size // 128)):
            low, high = n * 128, min(n * 128 + 128, size)
            ref[row : row + 1, start + low : start + high] = line_out[
                base + n : base + n + 1, 0 : high - low
            ]

    for c in range(spots):
        take(c * q_rows, query_out, 0, c * span, span)
        take(value_base + c * q_rows, value_out, 0, c * span, span)
    for n in range(6):
        take(rows_base + n * w_rows, rows_out, n, 0, width)
    for n in range(xs * ks * inner):
        take(hidden_base + n * p_rows, hidden_out, 0, n * piece, piece)
    shrink.finish()
    outw.finish()
    each_sent(sent_block)
    for copy in line_started + q_copies + [q_over]:
        copy.wait_send()
    for t in range(chips):
        to_mate(t).wait_send()
    for t in range(1, chips):
        to_chip(t).wait_send()


def final_part(
    dqkv,
    columns,
    normed_low,
    shrink_terms,
    low_middle,
    att,
    own,
    grad_middle,
    gain,
    row_sums,
    hidden_sum,
    axes,
    sizes,
    heads,
    share,
    ident,
):
    outer, inner, ys, xs, ks = sizes
    spots, cell, piece = shrink_terms.shape
    rows, width = own.shape
    chips = outer * inner
    devices = spots * xs * ks
    group = inner * xs * ks
    span = heads * HEAD_DIM
    part_rows = width // (xs * ks)
    slots = max(
        (share * (c + 1) - 1) // HEAD_DIM - (share * c) // HEAD_DIM + 1 for c in range(spots)
    )
    line_rows = (
        2 * spots * -(-span // 128) + 6 * -(-width // 128) + xs * ks * inner * -(-piece // 128)
    )
    line_rows = 8 * -(-line_rows // (8 * devices))
    block = (rows, width)
    q_block = (3 * span, part_rows)
    out_rows = width // group
    return pl.pallas_call(
        functools.partial(final_kernel, axes, sizes, heads, share),
        out_shape=[
            jax.ShapeDtypeStruct(block, F32),
            jax.ShapeDtypeStruct((slots, HEAD_DIM, part_rows), BF16),
            jax.ShapeDtypeStruct((inner, cell, piece), BF16),
            jax.ShapeDtypeStruct((inner, cell, out_rows), BF16),
            jax.ShapeDtypeStruct((1, spots * span), F32),
            jax.ShapeDtypeStruct((1, spots * span), F32),
            jax.ShapeDtypeStruct((6, width), F32),
            jax.ShapeDtypeStruct((1, group * piece), F32),
        ],
        in_specs=[VMEM] * 2 + [ANY] + [VMEM] * 8,
        out_specs=[VMEM] * 8,
        scratch_shapes=[
            pltpu.VMEM((chips, ys) + block, BF16),
            pltpu.VMEM((chips,) + block, BF16),
            pltpu.VMEM((chips - 1,) + block, BF16),
            pltpu.VMEM((min(1024, dqkv.shape[0]), width), BF16),
            pltpu.VMEM((xs, ks) + q_block, BF16),
            pltpu.VMEM((2,) + q_block, BF16),
            pltpu.VMEM(q_block, BF16),
            pltpu.VMEM(q_block, BF16),
            pltpu.VMEM((3 * heads, HEAD_DIM, part_rows), BF16),
            pltpu.VMEM((inner * xs, ks) + block, BF16),
            pltpu.VMEM((group, rows, out_rows), BF16),
            pltpu.VMEM((group, rows, out_rows), BF16),
            pltpu.VMEM((spots, cell, out_rows), BF16),
            pltpu.VMEM((devices * line_rows, 128), F32),
            pltpu.VMEM((devices - 1, line_rows, 128), F32),
            pltpu.VMEM((devices * line_rows, 128), F32),
            pltpu.SemaphoreType.DMA((2 * chips,)),
            pltpu.SemaphoreType.DMA((2 * chips,)),
            pltpu.SemaphoreType.DMA((3,)),
            pltpu.SemaphoreType.DMA((3,)),
            pltpu.SemaphoreType.DMA((6 * heads,)),
            pltpu.SemaphoreType.DMA((slots,)),
            pltpu.SemaphoreType.DMA((group,)),
            pltpu.SemaphoreType.DMA((group,)),
            pltpu.SemaphoreType.DMA((2 * devices,)),
            pltpu.SemaphoreType.DMA((2 * devices,)),
            *gather_scratch((("i", "x"), (inner, xs), "k")),
            pltpu.SemaphoreType.DMA,
            *owned_scratch(outer, cell, piece),
            *owned_scratch(outer, cell, out_rows),
        ],
        name="final%d" % ident,
        compiler_params=pltpu.CompilerParams(
            collective_id=ident, has_side_effects=True, vmem_limit_bytes=67_000_000
        ),
        cost_estimate=pl.CostEstimate(
            flops=12 * rows * spots * width * span,
            bytes_accessed=100 * rows * width * 2,
            transcendentals=0,
        ),
    )(
        dqkv,
        columns,
        normed_low,
        shrink_terms,
        low_middle,
        att,
        own,
        grad_middle,
        gain,
        row_sums,
        hidden_sum,
    )


def nt(left, right):
    return lax.dot_general(left, right, (((1,), (1,)), ((), ())), preferred_element_type=F32)


def nn(left, right):
    return lax.dot_general(left, right, (((1,), (0,)), ((), ())), preferred_element_type=F32)


def tn(left, right):
    return lax.dot_general(left, right, (((0,), (0,)), ((), ())), preferred_element_type=F32)


def rows_of(inv, ref, pair, low, high):
    first = pl.multiple_of(inv[2 * pair] * HEAD_DIM, HEAD_DIM)
    second = pl.multiple_of(inv[2 * pair + 1] * HEAD_DIM, HEAD_DIM)
    return jnp.concatenate(
        [ref[pl.ds(first, 64), low:high], ref[pl.ds(second, 64), low:high]], axis=0
    )


def put_rows(inv, ref, pair, low, high, values):
    first = pl.multiple_of(inv[2 * pair] * HEAD_DIM, HEAD_DIM)
    second = pl.multiple_of(inv[2 * pair + 1] * HEAD_DIM, HEAD_DIM)
    ref[pl.ds(first, 64), low:high] = values[:64]
    ref[pl.ds(second, 64), low:high] = values[64:]


def head_slice(values, part, heads, head):
    low = (part * heads + head) * HEAD_DIM
    return values[:, low : low + HEAD_DIM]


def diagonal(block):
    return lax.broadcasted_iota(jnp.int32, (block, block), 0) <= lax.broadcasted_iota(
        jnp.int32, (block, block), 1
    )


def attend_kernel(heads, block, inv, qkv, out, out_low, lse, qs, ks, vt, ot):
    length = qkv.shape[0]
    width = heads * HEAD_DIM

    def sort(pair, unused):
        at = pl.multiple_of(pair * 128, 128)
        values = rows_of(inv, qkv, pair, 0, 3 * width)
        for h in range(heads):
            qs[h, pl.ds(at, 128), :] = head_slice(values, 0, heads, h) * BF16(0.125)
            ks[h, pl.ds(at, 128), :] = head_slice(values, 1, heads, h)
            vt[h, :, pl.ds(at, 128)] = head_slice(values, 2, heads, h).astype(F32).T.astype(BF16)
        return unused

    lax.fori_loop(0, length // 128, sort, 0)
    allowed = diagonal(block)

    def row(qi, unused):
        q_at = pl.multiple_of(qi * block, block)

        def first(h):
            scores = nt(ks[h, pl.ds(q_at, block), :], qs[h, pl.ds(q_at, block), :])
            scores = jnp.where(allowed, scores, -1e30)
            high = jnp.max(scores, axis=0, keepdims=True)
            probs = jnp.exp(scores - high)
            return (
                high,
                jnp.sum(probs, axis=0, keepdims=True),
                nn(vt[h, :, pl.ds(q_at, block)], probs.astype(BF16)),
            )

        def column(kj, state):
            k_at = pl.multiple_of(kj * block, block)
            fresh_state = []
            for h in range(heads):
                high, weight, acc = state[h]
                scores = nt(ks[h, pl.ds(k_at, block), :], qs[h, pl.ds(q_at, block), :])
                fresh = jnp.maximum(high, jnp.max(scores, axis=0, keepdims=True))
                probs = jnp.exp(scores - fresh)
                fade = jnp.exp(high - fresh)
                fresh_state.append(
                    (
                        fresh,
                        weight * fade + jnp.sum(probs, axis=0, keepdims=True),
                        acc * fade + nn(vt[h, :, pl.ds(k_at, block)], probs.astype(BF16)),
                    )
                )
            return tuple(fresh_state)

        state = lax.fori_loop(0, qi, column, tuple(first(h) for h in range(heads)))
        for h in range(heads):
            high, weight, acc = state[h]
            ot[h, :, pl.ds(q_at, block)] = acc / weight
            lse[h : h + 1, pl.ds(q_at, block)] = high + jnp.log(weight)
        return unused

    lax.fori_loop(0, length // block, row, 0)

    def unsort(pair, unused):
        at = pl.multiple_of(pair * 128, 128)
        values = [ot[h, :, pl.ds(at, 128)].T for h in range(heads)]
        values = jnp.concatenate(values, axis=1)
        put_rows(inv, out, pair, 0, width, values)
        put_rows(inv, out_low, pair, 0, width, values.astype(BF16))
        return unused

    lax.fori_loop(0, length // 128, unsort, 0)


def attend(inv, qkv, heads):
    length = qkv.shape[0]
    width = heads * HEAD_DIM
    block = min(256, length)
    pairs = length * (length + block) // 2
    return pl.pallas_call(
        functools.partial(attend_kernel, heads, block),
        out_shape=(
            jax.ShapeDtypeStruct((length, width), F32),
            jax.ShapeDtypeStruct((length, width), BF16),
            jax.ShapeDtypeStruct((heads, length), F32),
        ),
        grid_spec=pltpu.PrefetchScalarGridSpec(
            num_scalar_prefetch=1,
            grid=(1,),
            in_specs=[pl.BlockSpec((length, 3 * width), lambda i, inv: (0, 0))],
            out_specs=(
                pl.BlockSpec((length, width), lambda i, inv: (0, 0)),
                pl.BlockSpec((length, width), lambda i, inv: (0, 0)),
                pl.BlockSpec((heads, length), lambda i, inv: (0, 0)),
            ),
            scratch_shapes=[
                pltpu.VMEM((heads, length, HEAD_DIM), BF16),
                pltpu.VMEM((heads, length, HEAD_DIM), BF16),
                pltpu.VMEM((heads, HEAD_DIM, length), BF16),
                pltpu.VMEM((heads, HEAD_DIM, length), F32),
            ],
        ),
        name="attend",
        cost_estimate=pl.CostEstimate(
            flops=4 * heads * pairs * HEAD_DIM * 4,
            bytes_accessed=length * width * 10,
            transcendentals=heads * pairs,
        ),
    )(inv, qkv)


def attend_back_kernel(
    heads, block, inv, qkv, grads, outs, lse, dqkv, qs, ks, vs, gs, kt, delta, dqt, dks, dvs
):
    length = qkv.shape[0]
    width = heads * HEAD_DIM
    count = length // block

    def sort(pair, unused):
        at = pl.multiple_of(pair * 128, 128)
        values = rows_of(inv, qkv, pair, 0, 3 * width)
        grad = rows_of(inv, grads, pair, 0, width)
        value = rows_of(inv, outs, pair, 0, width)
        product = (grad.astype(F32) * value).T
        for h in range(heads):
            qs[h, pl.ds(at, 128), :] = head_slice(values, 0, heads, h) * BF16(0.125)
            key = head_slice(values, 1, heads, h)
            ks[h, pl.ds(at, 128), :] = key
            kt[h, :, pl.ds(at, 128)] = key.astype(F32).T.astype(BF16)
            vs[h, pl.ds(at, 128), :] = head_slice(values, 2, heads, h)
            gs[h, pl.ds(at, 128), :] = head_slice(grad, 0, heads, h)
            delta[h : h + 1, pl.ds(at, 128)] = jnp.sum(
                product[h * HEAD_DIM : (h + 1) * HEAD_DIM], axis=0, keepdims=True
            )
            dqt[h, :, pl.ds(at, 128)] = jnp.zeros((HEAD_DIM, 128), F32)
        return unused

    lax.fori_loop(0, length // 128, sort, 0)
    allowed = diagonal(block)

    def column(kj, unused):
        k_at = pl.multiple_of(kj * block, block)

        def tile(h, q_at, masked):
            q = qs[h, pl.ds(q_at, block), :]
            g = gs[h, pl.ds(q_at, block), :]
            scores = nt(ks[h, pl.ds(k_at, block), :], q)
            probs = jnp.exp(scores - lse[h : h + 1, pl.ds(q_at, block)])
            if masked:
                probs = jnp.where(allowed, probs, 0.0)
            slopes = nt(vs[h, pl.ds(k_at, block), :], g)
            low = (probs * (slopes - delta[h : h + 1, pl.ds(q_at, block)])).astype(BF16)
            dqt[h, :, pl.ds(q_at, block)] += nn(kt[h, :, pl.ds(k_at, block)], low)
            return nn(low, q), nn(probs.astype(BF16), g)

        def row(qi, state):
            q_at = pl.multiple_of(qi * block, block)
            fresh = []
            for h in range(heads):
                dk, dv = tile(h, q_at, False)
                fresh.append((state[h][0] + dk, state[h][1] + dv))
            return tuple(fresh)

        state = tuple(tile(h, k_at, True) for h in range(heads))
        state = lax.fori_loop(kj + 1, count, row, state)
        for h in range(heads):
            dks[h, pl.ds(k_at, block), :] = state[h][0].astype(BF16)
            dvs[h, pl.ds(k_at, block), :] = state[h][1].astype(BF16)
        return unused

    lax.fori_loop(0, count, column, 0)

    def unsort(pair, unused):
        at = pl.multiple_of(pair * 128, 128)
        values = [(dqt[h, :, pl.ds(at, 128)].T * 0.125).astype(BF16) for h in range(heads)]
        values += [dks[h, pl.ds(at, 128), :] for h in range(heads)]
        values += [dvs[h, pl.ds(at, 128), :] for h in range(heads)]
        put_rows(inv, dqkv, pair, 0, 3 * width, jnp.concatenate(values, axis=1))
        return unused

    lax.fori_loop(0, length // 128, unsort, 0)


def attend_back(inv, qkv, grads, outs, lse, heads):
    length = qkv.shape[0]
    width = heads * HEAD_DIM
    block = min(256, length)
    pairs = length * (length + block) // 2
    row_shape = (heads, length, HEAD_DIM)
    return pl.pallas_call(
        functools.partial(attend_back_kernel, heads, block),
        out_shape=jax.ShapeDtypeStruct((length, 3 * width), BF16),
        grid_spec=pltpu.PrefetchScalarGridSpec(
            num_scalar_prefetch=1,
            grid=(1,),
            in_specs=[
                pl.BlockSpec((length, 3 * width), lambda i, inv: (0, 0)),
                pl.BlockSpec((length, width), lambda i, inv: (0, 0)),
                pl.BlockSpec((length, width), lambda i, inv: (0, 0)),
                pl.BlockSpec((heads, length), lambda i, inv: (0, 0)),
            ],
            out_specs=pl.BlockSpec((length, 3 * width), lambda i, inv: (0, 0)),
            scratch_shapes=[
                pltpu.VMEM(row_shape, BF16),
                pltpu.VMEM(row_shape, BF16),
                pltpu.VMEM(row_shape, BF16),
                pltpu.VMEM(row_shape, BF16),
                pltpu.VMEM((heads, HEAD_DIM, length), BF16),
                pltpu.VMEM((heads, length), F32),
                pltpu.VMEM((heads, HEAD_DIM, length), F32),
                pltpu.VMEM(row_shape, BF16),
                pltpu.VMEM(row_shape, BF16),
            ],
        ),
        name="attend_back",
        cost_estimate=pl.CostEstimate(
            flops=10 * heads * pairs * HEAD_DIM * 4,
            bytes_accessed=length * width * 20,
            transcendentals=heads * pairs,
        ),
    )(inv, qkv, grads, outs, lse)


def layer_norm(values, gain, shift):
    center = jnp.mean(values, axis=-1, keepdims=True)
    centred = values - center
    spread = jnp.mean(centred * centred, axis=-1, keepdims=True)
    return centred * lax.rsqrt(spread + EPSILON) * gain + shift


def matmul(left, right):
    return jnp.dot(left, right, preferred_element_type=F32)


def body(
    sizes,
    tokens,
    block_order,
    qkv_weight,
    query_bias,
    value_bias,
    out_weight,
    out_bias,
    expand_weight,
    expand_bias,
    shrink_weight,
    shrink_bias,
    first_gain,
    first_shift,
    second_gain,
    second_shift,
    cotangent,
):
    outer, inner, ys, xs, ks = (sizes[a] for a in ("o", "i", "y", "x", "k"))
    spots = outer * inner * ys
    shards = xs * ks
    rows, width = tokens.shape[1:]
    o, i, y = lax.axis_index("o"), lax.axis_index("i"), lax.axis_index("y")
    shard = lax.axis_index("x") * ks + lax.axis_index("k")
    place = (o * inner + i) * ys + y
    heads = -(-HEADS // spots)
    span = heads * HEAD_DIM
    padded = spots * span
    part = qkv_weight.shape[0]
    hidden = expand_weight.shape[1]
    piece = hidden // (shards * inner)
    every = (("o", "i", "y"), (outer, inner, ys))
    ctx = (("o", "i"), (outer, inner), "y")
    group = (("i", "x"), (inner, xs), "k")
    pair = (("x",), (xs,), "k")
    own = tokens[0]
    own_grad = cotangent[0]

    def columns(values, count):
        wide = values.reshape(values.shape[:-1] + (count, width))
        wide = jnp.pad(wide, [(0, 0)] * (wide.ndim - 1) + [(0, padded - width)])
        return lax.dynamic_slice_in_dim(wide, place * span, span, axis=wide.ndim - 1)

    qkv_bias = jnp.concatenate(
        [columns(query_bias, 1)[0], jnp.zeros((span,), F32), columns(value_bias, 1)[0]]
    )
    gathered, qkv_columns, expand_columns = first_gather(
        own, qkv_weight, expand_weight, span, [ctx, pair], (xs, ks), every, piece, 0
    )
    sequence = gathered.reshape(spots * rows, width)
    qkv_columns = qkv_columns.reshape(width, 3 * span)

    sequence, out_own = lax.optimization_barrier((sequence, out_weight))
    out_far = lax.ppermute(out_own, "x", [(0, 1), (1, 0)])
    expand_own_bias = lax.dynamic_slice_in_dim(
        expand_bias, (shard * inner + i) * piece, piece, axis=0
    )

    order_row = block_order[0]
    blocks = order_row.shape[0]
    inv = jnp.sum(
        jnp.where(
            order_row[:, None] == jnp.arange(blocks, dtype=jnp.int32)[None, :],
            jnp.arange(blocks, dtype=jnp.int32)[:, None],
            0,
        ),
        axis=0,
    ).astype(jnp.int32)
    normed_low = layer_norm(sequence.astype(F32), first_gain, first_shift).astype(BF16)
    qkv = (matmul(normed_low, qkv_columns) + qkv_bias).astype(BF16)
    attended, attended_bf, log_sum = attend(inv, qkv, heads)
    def cut(values, axis_name, dim):
        index, size = lax.axis_index(axis_name), sizes[axis_name]
        return [
            lax.dynamic_index_in_dim(values, lax.rem(index + s, size), axis=dim, keepdims=False)
            for s in range(size)
        ]

    def added(pieces, axis_name):
        size = sizes[axis_name]
        total = pieces[0].astype(F32)
        for step in range(1, size):
            ring = [(d, (d + step) % size) for d in range(size)]
            total = total + lax.ppermute(pieces[step], axis_name, ring).astype(F32)
        return total.astype(BF16)

    cuts = spots // (2 * shards)
    (
        attended_low,
        result,
        grad_middle,
        middle_low,
        row_sums,
        hidden_sums,
        grad_heads,
        expand_half,
        shrink_terms,
    ) = middle_part(
        attended_bf.reshape(spots, rows, span),
        own,
        own_grad,
        out_own,
        out_far,
        expand_columns,
        shrink_weight,
        [
            v[None]
            for v in (out_bias, expand_own_bias, shrink_bias, second_gain, second_shift)
        ],
        every,
        group,
        1,
    )
    grad_heads = grad_heads.reshape(spots * rows, span)
    dqkv = attend_back(inv, qkv, grad_heads, attended, log_sum, heads)
    expand_whole = added(cut(expand_half, "o", 0), "o")
    dqkv, expand_whole = lax.optimization_barrier((dqkv, expand_whole))
    axes = ("o", "i", "y", "x", "k")
    routes = []
    for so, si, sy, sf in itertools.product(*map(range, (outer, inner, ys, shards))):
        index = so * ys + sy
        spot = sf * (spots // shards) + si * cuts + index % cuts
        routes.append((((so * inner + si) * ys + sy) * shards + sf, spot * shards + index // cuts))
    grad_expand = lax.ppermute(expand_whole, axes, routes).astype(F32)
    share = 3 * width // spots
    (
        grad_inputs,
        routed,
        shrink_cells,
        outw_cells,
        query_sums,
        value_sums,
        row_totals,
        hidden_totals,
    ) = final_part(
        dqkv,
        qkv_columns,
        normed_low,
        shrink_terms,
        middle_low,
        attended_low,
        own,
        grad_middle,
        first_gain[None],
        row_sums,
        hidden_sums,
        axes,
        (outer, inner, ys, xs, ks),
        heads,
        share,
        2,
    )

    def upright(cells):
        return cells.transpose(0, 2, 1).reshape(-1, cells.shape[1]).astype(F32)

    start = share * place - HEAD_DIM * ((share * place) // HEAD_DIM)
    grad_qkv = lax.dynamic_slice_in_dim(routed.reshape(-1, part), start, share, axis=0)
    return (
        result[None],
        grad_inputs[None],
        grad_qkv.T.astype(F32),
        upright(outw_cells),
        grad_expand,
        upright(shrink_cells),
        query_sums[0, :width],
        value_sums[0, :width],
        row_totals[0],
        hidden_totals[0],
        row_totals[1],
        row_totals[4],
        row_totals[5],
        row_totals[2],
        row_totals[3],
    )


def solution(mesh):
    spots, shards = mesh.shape["ctx"], mesh.shape["fsdp"]
    sizes = {"o": spots // 4, "i": 2, "y": 2, "x": shards // 2, "k": 2}
    fine = Mesh(mesh.devices.reshape(tuple(sizes.values())), tuple(sizes))
    seq, pos = ("x", "k"), ("o", "i", "y")
    weight = P(seq, None)
    placed = (
        P(seq, pos, None),
        P(seq, None),
        weight,
        P(),
        P(),
        weight,
        P(),
        weight,
        P(),
        weight,
        P(),
        P(),
        P(),
        P(),
        P(),
        P(seq, pos, None),
    )
    given = (P(seq, pos, None),) * 2 + (P(seq, pos),) * 4 + (P(),) * 9
    return jax.shard_map(
        functools.partial(body, sizes),
        mesh=fine,
        in_specs=placed,
        out_specs=given,
        check_vma=False,
    )
```

```python
import functools
import itertools

import jax
import jax.numpy as jnp
from jax import lax
from jax.experimental import pallas as pl
from jax.experimental.pallas import tpu as pltpu
from jax.sharding import Mesh
from jax.sharding import PartitionSpec as P

HEADS = 25
HEAD_DIM = 64
EPSILON = 1e-05
MESH = pl.DeviceIdType.MESH
F32 = jnp.float32
BF16 = jnp.bfloat16
ANY = pl.BlockSpec(memory_space=pl.ANY)
VMEM = pl.BlockSpec(memory_space=pltpu.VMEM)


def offsets(sizes):
    return [o for o in itertools.product(*(range(s) for s in sizes)) if any(o)]


def moved(axes, sizes, offset, sign=1):
    return {
        a: lax.rem(lax.axis_index(a) + (o if sign > 0 else s - o), s)
        for a, s, o in zip(axes, sizes, offset)
    }


def flat(place, axes, sizes):
    index = 0
    for a, s in zip(axes, sizes):
        index = index * s + place[a]
    return index


def own_place(axes):
    return {a: lax.axis_index(a) for a in axes}


def greet(peers):
    barrier = pltpu.get_barrier_semaphore()
    for peer in peers:
        pl.semaphore_signal(barrier, inc=1, device_id=peer, device_id_type=MESH)
    pl.semaphore_wait(barrier, len(peers))


def remote(src, dst, send, recv, peer):
    return pltpu.make_async_remote_copy(
        src_ref=src,
        dst_ref=dst,
        send_sem=send,
        recv_sem=recv,
        device_id=peer,
        device_id_type=MESH,
    )


class Gather:
    def __init__(self, axes, sizes, pair, source, out, send, recv, local):
        self.axes, self.sizes = axes, sizes
        self.offs = offsets(sizes)
        self.side = lax.axis_index(pair)
        self.mate = {pair: 1 - self.side}
        self.source, self.out, self.send, self.recv, self.local = source, out, send, recv, local
        self.started = []

    def peers(self):
        return [moved(self.axes, self.sizes, o) for o in self.offs] + [self.mate]

    def mine(self):
        return self.out.at[flat(own_place(self.axes), self.axes, self.sizes), self.side]

    def start(self):
        pltpu.make_async_copy(self.source, self.mine(), self.local).start()
        last = len(self.offs)
        for t, peer in enumerate(self.peers()):
            copy = remote(self.source, self.mine(), self.send.at[t], self.recv.at[t], peer)
            copy.start()
            self.started.append(copy)

    def hand_on(self):
        last = len(self.offs)
        for t, off in enumerate(self.offs):
            came = flat(moved(self.axes, self.sizes, off, -1), self.axes, self.sizes)
            block = self.out.at[came, self.side]
            remote(self.source, block, self.send.at[t], self.recv.at[t], self.mate).wait_recv()
            slot = last + 1 + t
            copy = remote(block, block, self.send.at[slot], self.recv.at[slot], self.mate)
            copy.start()
            self.started.append(copy)

    def finish(self):
        last = len(self.offs)
        me = flat(own_place(self.axes), self.axes, self.sizes)
        pltpu.make_async_copy(self.source, self.mine(), self.local).wait()
        block = self.out.at[me, 1 - self.side]
        remote(self.source, block, self.send.at[last], self.recv.at[last], self.mate).wait_recv()
        for t, off in enumerate(self.offs):
            came = flat(moved(self.axes, self.sizes, off, -1), self.axes, self.sizes)
            slot = last + 1 + t
            block = self.out.at[came, 1 - self.side]
            remote(
                self.source, block, self.send.at[slot], self.recv.at[slot], self.mate
            ).wait_recv()
        for copy in self.started:
            copy.wait_send()


def gather_shape(block, spec):
    group = 1
    for s in spec[1]:
        group *= s
    return jax.ShapeDtypeStruct((group, 2) + block.shape, block.dtype)


def gather_scratch(spec):
    group = 1
    for s in spec[1]:
        group *= s
    return [
        pltpu.SemaphoreType.DMA((2 * group,)),
        pltpu.SemaphoreType.DMA((2 * group,)),
        pltpu.SemaphoreType.DMA,
    ]


def sent_estimate(size):
    return pl.CostEstimate(flops=0, bytes_accessed=20 * size, transcendentals=0)


class Line:
    def __init__(self, sizes, source, out, send, recv, local):
        self.outer, self.inner = sizes
        self.count = self.outer * self.inner
        self.at = lax.axis_index("o") * self.inner + lax.axis_index("i")
        self.y = lax.axis_index("y")
        self.mate = {"y": 1 - self.y}
        self.source, self.out, self.send, self.recv, self.local = source, out, send, recv, local

    def spot(self, at):
        return {"o": at // self.inner, "i": at % self.inner}

    def copies(self, at, here):
        block = self.out.at[at, self.y]
        source = self.source if here else block
        right, left = lax.rem(self.at + 1, self.count), lax.rem(
            self.at + self.count - 1, self.count
        )
        return [
            (
                (at <= self.at) & (self.at + 1 < self.count),
                remote(source, block, self.send.at[0, at], self.recv.at[0, at], self.spot(right)),
            ),
            (
                (at >= self.at) & (self.at > 0),
                remote(source, block, self.send.at[1, at], self.recv.at[0, at], self.spot(left)),
            ),
            (True, remote(source, block, self.send.at[2, at], self.recv.at[1, at], self.mate)),
        ]

    def each(self, at, here, act):
        for needed, copy in self.copies(at, here):
            if needed is True:
                act(copy)
            else:

                @pl.when(needed)
                def _(copy=copy):
                    act(copy)

    def start(self):
        pltpu.make_async_copy(
            self.source, self.out.at[self.at, self.y], self.local
        ).start()
        self.each(self.at, True, lambda copy: copy.start())

    def arrive(self, at):
        block = self.out.at[at, self.y]
        remote(self.source, block, self.send.at[0, at], self.recv.at[0, at], self.mate).wait_recv()
        self.each(at, False, lambda copy: copy.start())

    def across(self, at):
        block = self.out.at[at, 1 - self.y]
        remote(self.source, block, self.send.at[2, at], self.recv.at[1, at], self.mate).wait_recv()

    def finish(self):
        for at in range(self.count):
            self.each(at, False, lambda copy: copy.wait_send())


def first_kernel(
    sizes,
    own,
    qkv_weight,
    weight,
    gain,
    shift,
    bias,
    qkv,
    normed_out,
    all_columns,
    pieces,
    sequence,
    qkv_whole,
    columns,
    columns_in,
    whole,
    cut,
    send,
    recv,
    local,
    head_send,
    head_recv,
    head_local,
    read,
    qkv_read,
    cut_send,
    cut_recv,
    cut_local,
):
    outer, inner, ys, xs, ks = sizes
    axes, shard_sizes = ("x", "k"), (xs, ks)
    offs = offsets(shard_sizes)
    line = Line((outer, inner), own, sequence, send, recv, local)
    heads = Gather(
        ("x",), (xs,), "k", columns, all_columns, head_send, head_recv, head_local
    )
    qkv_fetch = pltpu.make_async_copy(qkv_weight, qkv_whole, qkv_read)
    qkv_fetch.start()
    fetch = pltpu.make_async_copy(weight, whole, read)
    fetch.start()
    peers = [moved(axes, shard_sizes, o) for o in offs] + [
        moved(("o", "i", "y"), (outer, inner, ys), o) for o in offsets((outer, inner, ys))
    ]
    greet(peers)
    line.start()
    qkv_fetch.wait()
    place = line.at * ys + line.y
    part, span = columns.shape[0], columns.shape[1] // 3
    width = qkv_whole.shape[1] // 3
    for spot in range(-(-width // span)):

        @pl.when(place == spot)
        def _(spot=spot):
            size = min(span, width - spot * span)
            for section in range(3):
                low = section * width + spot * span
                if size < span:
                    columns[:, section * span : (section + 1) * span] = jnp.zeros(
                        (part, span), BF16
                    )
                columns[:, section * span : section * span + size] = qkv_whole[:, low : low + size]

    @pl.when(place * span >= width)
    def _():
        columns[...] = jnp.zeros(columns.shape, BF16)

    heads.start()
    fetch.wait()
    cut_width = cut.shape[2]
    side = lax.axis_index("i")
    for half in range(2):

        @pl.when(side == half)
        def _():
            for f in range(cut.shape[0]):
                low = (2 * f + half) * cut_width
                cut[f] = whole[:, low : low + cut_width]

    me = flat(own_place(axes), axes, shard_sizes)
    here = pltpu.make_async_copy(cut.at[me], pieces.at[me], cut_local)
    here.start()
    started = []
    for t, off in enumerate(offs):
        peer = moved(axes, shard_sizes, off)
        there = flat(peer, axes, shard_sizes)
        copy = remote(cut.at[there], pieces.at[me], cut_send.at[t], cut_recv.at[t], peer)
        copy.start()
        started.append(copy)
    pltpu.make_async_copy(own, sequence.at[line.at, line.y], local).wait()
    for distance in range(1, line.count):
        for sign in (-1, 1):
            at = line.at + sign * distance

            @pl.when((at >= 0) & (at < line.count))
            def _(at=at):
                line.arrive(at)

        if distance == 1:
            heads.hand_on()

    heads.finish()
    load = pltpu.make_async_copy(all_columns, columns_in, qkv_read)
    load.start()
    load.wait()
    rows = own.shape[0]

    def project(at):
        values = sequence[at].reshape(ys * rows, width).astype(F32)
        plain, unused_scale = normed(values)
        low = (plain * gain[...] + shift[...]).astype(BF16)
        start = pl.multiple_of(at * ys * rows, ys * rows)
        normed_out[pl.ds(start, ys * rows), :] = low
        weights = columns_in[...].reshape(width, 3 * span)
        qkv[pl.ds(start, ys * rows), :] = (
            jnp.dot(low, weights, preferred_element_type=F32) + bias[...]
        ).astype(BF16)

    nearest = [sorted(range(line.count), key=lambda q: abs(q - p)) for p in range(line.count)]

    def step(n, unused):
        at = line.at
        for p in range(line.count):
            for m in range(1, line.count):
                at = jnp.where((line.at == p) & (n == m), nearest[p][m], at)
        line.across(at)
        project(at)
        return unused

    lax.fori_loop(0, line.count, step, 0)
    here.wait()
    for t, off in enumerate(offs):
        peer = moved(axes, shard_sizes, off, -1)
        came = flat(peer, axes, shard_sizes)
        remote(cut.at[came], pieces.at[came], cut_send.at[t], cut_recv.at[t], peer).wait_recv()
    for copy in started:
        copy.wait_send()
    line.finish()


def first_part(own, qkv_weight, weight, vectors, span, sizes, piece, ident):
    outer, inner, ys, xs, ks = sizes
    shards, chips = xs * ks, outer * inner
    part = weight.shape[0]
    rows, width = own.shape
    tokens = chips * ys * rows
    columns = jax.ShapeDtypeStruct((part, 3 * span), BF16)
    spec = (("x",), (xs,), "k")
    gathered = gather_shape(columns, spec)
    return pl.pallas_call(
        functools.partial(first_kernel, sizes),
        out_shape=[
            jax.ShapeDtypeStruct((tokens, 3 * span), BF16),
            jax.ShapeDtypeStruct((tokens, width), BF16),
            gathered,
            jax.ShapeDtypeStruct((shards, part, piece), BF16),
        ],
        in_specs=[VMEM, ANY, ANY, VMEM, VMEM, VMEM],
        out_specs=[VMEM, VMEM, ANY, ANY],
        scratch_shapes=[
            pltpu.VMEM((chips, ys, rows, width), BF16),
            pltpu.VMEM(qkv_weight.shape, BF16),
            pltpu.VMEM(columns.shape, BF16),
            pltpu.VMEM(gathered.shape, BF16),
            pltpu.VMEM(weight.shape, BF16),
            pltpu.VMEM((shards, part, piece), BF16),
            pltpu.SemaphoreType.DMA((3, chips)),
            pltpu.SemaphoreType.DMA((2, chips)),
            pltpu.SemaphoreType.DMA,
            *gather_scratch(spec),
            pltpu.SemaphoreType.DMA,
            pltpu.SemaphoreType.DMA,
            pltpu.SemaphoreType.DMA((shards,)),
            pltpu.SemaphoreType.DMA((shards,)),
            pltpu.SemaphoreType.DMA,
        ],
        name="first%d" % ident,
        compiler_params=pltpu.CompilerParams(
            collective_id=ident, has_side_effects=True, vmem_limit_bytes=67_000_000
        ),
        cost_estimate=pl.CostEstimate(
            flops=6 * tokens * width * span,
            bytes_accessed=40 * tokens * width,
            transcendentals=0,
        ),
    )(own, qkv_weight, weight, *vectors)


def pieces_out(axes, sizes, source, out, send, recv):
    me = flat(own_place(axes), axes, sizes)
    started = []
    for t, off in enumerate(offsets(sizes)):
        peer = moved(axes, sizes, off)
        copy = remote(
            source.at[flat(peer, axes, sizes)], out.at[me], send.at[t], recv.at[t], peer
        )
        copy.start()
        started.append(copy)
    return started


def pieces_in(axes, sizes, source, out, send, recv, started):
    for t, off in enumerate(offsets(sizes)):
        peer = moved(axes, sizes, off, -1)
        came = flat(peer, axes, sizes)
        remote(source.at[came], out.at[came], send.at[t], recv.at[t], peer).wait_recv()
    for copy in started:
        copy.wait_send()


def normed(values):
    center = jnp.mean(values, axis=-1, keepdims=True)
    centred = values - center
    spread = jnp.mean(centred * centred, axis=-1, keepdims=True)
    scale = lax.rsqrt(spread + EPSILON)
    return centred * scale, scale


def norm_back(grad, gain, plain, scale):
    inner = grad * gain
    return scale * (
        inner
        - jnp.mean(inner, axis=-1, keepdims=True)
        - plain * jnp.mean(inner * plain, axis=-1, keepdims=True)
    )


def by_columns(left, right, cell, put):
    tokens = left.shape[0] * left.shape[1] * left.shape[2]
    wide = 400 // cell
    others = right[...].reshape(tokens, right.shape[-1])
    for c in range(left.shape[3] // 400):
        terms = tn(left[:, :, :, c * 400 : (c + 1) * 400].reshape(tokens, 400), others)
        for n in range(wide):
            put(c * wide + n, terms[n * cell : (n + 1) * cell].astype(BF16))


def middle_kernel(
    every,
    spec,
    pieces,
    own,
    own_grad,
    out_own,
    out_far,
    expand,
    shrink,
    out_bias,
    expand_bias,
    shrink_bias,
    gain,
    shift,
    att,
    result,
    grad_middle,
    low_middle,
    sums,
    hidden_sum,
    to_heads,
    shrink_kept,
    shrink_sent,
    *rest,
):
    outer = every[1][0]
    middle_body(every, spec, pieces, own, own_grad, out_own, out_far, expand, shrink, out_bias,
        expand_bias, shrink_bias, gain, shift, att, result, grad_middle, low_middle, sums,
        hidden_sum, to_heads, shrink_kept, shrink_sent, rest[:outer], *rest[outer:])


def middle_body(
    every, spec, pieces, own, own_grad, out_own, out_far, expand, shrink, out_bias,
    expand_bias, shrink_bias, gain, shift, att, result, grad_middle, low_middle, sums,
    hidden_sum, to_heads, shrink_kept, shrink_sent, expand_half,
    came,
    out_w,
    expand_w,
    shrink_w,
    mid,
    c_own,
    c_all,
    e_all,
    gh,
    u_all,
    gz_all,
    part,
    first,
    summed,
    last,
    part_two,
    first_two,
    summed_two,
    last_two,
    cut,
    expand_terms,
    expand_came,
    send,
    recv,
    c_send,
    c_recv,
    c_local,
    e_send,
    e_recv,
    e_local,
    w_sem,
    w_send,
    w_recv,
    r_send,
    r_recv,
    s_send,
    s_recv,
    h_send,
    h_recv,
    y_send,
    y_recv,
):
    axes, sizes = every
    y = lax.axis_index("y")
    x, k, inner = lax.axis_index("x"), lax.axis_index("k"), lax.axis_index("i")
    mate = {"k": 1 - k}
    shard = 2 * x + k
    part_rows = out_own.shape[0]
    width = own.shape[1]
    rows = own.shape[0]
    piece = expand.shape[2]

    def chip(t):
        ti, tx = lax.rem(inner + t // 2, 2), lax.rem(x + t % 2, 2)
        return 2 * ti + tx, {"i": ti, "x": tx}

    loads = [
        pltpu.make_async_copy(out_own, out_w.at[pl.ds(shard * part_rows, part_rows)], w_sem.at[0]),
        pltpu.make_async_copy(
            out_far, out_w.at[pl.ds((shard ^ 2) * part_rows, part_rows)], w_sem.at[1]
        ),
        pltpu.make_async_copy(shrink.at[pl.ds(inner * piece, piece)], shrink_w, w_sem.at[2]),
    ]
    for f in range(expand.shape[0]):
        loads.append(
            pltpu.make_async_copy(
                expand.at[f], expand_w.at[pl.ds(f * part_rows, part_rows)], w_sem.at[3 + f]
            )
        )
    for copy in loads:
        copy.start()
    greet([moved(axes, sizes, o) for o in offsets(sizes)] + [chip(t)[1] for t in range(1, 4)] + [mate])

    started = pieces_out(axes, sizes, pieces, came, send, recv)
    out_sent = []
    for n, (source, owner) in enumerate(((out_own, shard), (out_far, shard ^ 2))):
        copy = remote(
            source, out_w.at[pl.ds(owner * part_rows, part_rows)], w_send.at[n], w_recv.at[n], mate
        )
        copy.start()
        out_sent.append(copy)
    e_gather = Gather(*spec, own_grad, e_all, e_send, e_recv, e_local)
    e_gather.start()
    here = flat(own_place(axes), axes, sizes)
    came[here] = pieces[here]
    pieces_in(axes, sizes, pieces, came, send, recv, started)
    span = came.shape[2]
    for d in range(came.shape[0]):
        low, high = d * span, min((d + 1) * span, width)
        if low < high:
            att[:, low:high] = came[d, :, : high - low]
    for copy in loads[:2]:
        copy.wait()
    for n, owner in enumerate((shard ^ 1, shard ^ 3)):
        remote(
            out_own,
            out_w.at[pl.ds(owner * part_rows, part_rows)],
            w_send.at[n],
            w_recv.at[n],
            mate,
        ).wait_recv()

    mid[...] = (
        own[...].astype(F32)
        + jnp.dot(att[...], out_w[...], preferred_element_type=F32)
        + out_bias[...]
    )
    plain, scale = normed(mid[...])
    c_own[...] = (plain * gain[...] + shift[...]).astype(BF16)
    c_gather = Gather(*spec, c_own, c_all, c_send, c_recv, c_local)
    c_gather.start()
    e_gather.hand_on()
    e_gather.finish()
    for copy in loads[2:]:
        copy.wait()

    def both(ref, place):
        return ref[place].reshape(2 * rows, ref.shape[3])

    def slopes(t, unused):
        place, unused_peer = chip(t)
        gh[place] = nt(both(e_all, place), shrink_w[...])
        return unused

    lax.fori_loop(0, 4, slopes, 0)
    hidden_sum[...] = jnp.zeros(hidden_sum.shape, F32)

    def c_wait(t):
        place, peer = chip(t)
        block = c_all.at[place, 1 - k]
        remote(c_own, block, c_send.at[3 + t], c_recv.at[3 + t], mate).wait_recv()

    def c_hand_on(t):
        place, peer = chip(t)
        block = c_all.at[place, k]
        remote(c_own, block, c_send.at[t - 1], c_recv.at[t - 1], mate).wait_recv()
        remote(block, block, c_send.at[3 + t], c_recv.at[3 + t], mate).start()

    def to_mate(t, source, target, sends, recvs):
        place, peer = chip(t)
        return remote(source.at[place, 1 - k], target.at[t], sends.at[t], recvs.at[t], mate)

    def to_chip(t, source, target, sends, recvs):
        place, peer = chip(t)
        return remote(
            source.at[t - 1], target.at[t - 1], sends.at[3 + t], recvs.at[3 + t], peer
        )

    def add_and_send(t, parts, firsts, sums_of, lasts, sends, recvs):
        place, peer = chip(t)
        to_mate(t, parts, firsts, sends, recvs).wait_recv()
        sums_of[t - 1] = (parts[place, k].astype(F32) + firsts[t].astype(F32)).astype(BF16)
        to_chip(t, sums_of, lasts, sends, recvs).start()

    pltpu.make_async_copy(c_own, c_gather.mine(), c_local).wait()

    def feed(t, unused):
        c_wait(t)
        place, peer = chip(t)
        expanded = jnp.dot(both(c_all, place), expand_w[...], preferred_element_type=F32)
        expanded = expanded + expand_bias[...]
        square = expanded * expanded
        bent = jnp.tanh(0.7978845608028654 * (expanded + 0.044715 * square * expanded))
        half = 0.5 * (1.0 + bent)
        u_all[place] = (expanded * half).astype(BF16)
        slope = half + 0.5 * expanded * (1.0 - bent * bent) * (
            0.7978845608028654 * (1.0 + 3 * 0.044715 * square)
        )
        low = (slope * gh[place]).astype(BF16)
        gz_all[place] = low
        hidden_sum[...] += jnp.sum(low.astype(F32), axis=0, keepdims=True)
        back = nt(low, expand_w[...]).astype(BF16)
        part[place] = back.reshape(2, rows, width)
        to_mate(t, part, first, r_send, r_recv).start()

        @pl.when(t < 3)
        def _():
            c_hand_on(t + 1)

        @pl.when(t > 1)
        def _():
            add_and_send(t - 1, part, first, summed, last, r_send, r_recv)

        return unused

    lax.fori_loop(0, 4, feed, 0)
    add_and_send(3, part, first, summed, last, r_send, r_recv)

    parts, cuts = expand.shape[0], expand_terms.shape[0] * 2 // expand.shape[0]
    cut_width = expand_terms.shape[3]
    for f in range(parts):
        terms = tn(
            c_all[:, :, :, f * part_rows : (f + 1) * part_rows].reshape(8 * rows, part_rows),
            gz_all[...].reshape(8 * rows, piece),
        )
        for c in range(cuts):
            index = f * cuts + c
            expand_terms[index // 2, index % 2] = terms[
                :, c * cut_width : (c + 1) * cut_width
            ].astype(BF16)
    y_mate = {"y": 1 - y}
    y_copies = [
        remote(
            expand_terms.at[n, 1 - y], expand_came.at[n], y_send.at[n], y_recv.at[n], y_mate
        )
        for n in range(expand_terms.shape[0])
    ]
    for copy in y_copies:
        copy.start()

    def gathered_sum(parts, firsts, lasts, sends, recvs):
        place, unused_peer = chip(0)
        to_mate(0, parts, firsts, sends, recvs).wait_recv()
        total = parts[place, k].astype(F32) + firsts[0].astype(F32)
        for t in range(1, 4):
            to_chip(t, firsts, lasts, sends, recvs).wait_recv()
            total = total + lasts[t - 1].astype(F32)
        return total

    grad = gathered_sum(part, first, last, r_send, r_recv)
    plain, scale = normed(mid[...])
    grad_mid = own_grad[...].astype(F32) + norm_back(grad, gain[...], plain, scale)
    grad_middle[...] = grad_mid
    low = grad_mid.astype(BF16)
    low_middle[...] = low
    sums[0:1, :] = jnp.sum(low.astype(F32), axis=0, keepdims=True)
    sums[1:2, :] = jnp.sum(own_grad[...].astype(F32), axis=0, keepdims=True)
    sums[2:3, :] = jnp.sum(grad * plain, axis=0, keepdims=True)
    sums[3:4, :] = jnp.sum(grad, axis=0, keepdims=True)
    back = nt(low, out_w[...]).astype(BF16)
    for d in range(cut.shape[0]):
        low_end, high = d * span, min((d + 1) * span, width)
        if high - low_end < span:
            cut[d] = jnp.zeros(cut.shape[1:], cut.dtype)
        if low_end < high:
            cut[d, :, : high - low_end] = back[:, low_end:high]
    head_started = pieces_out(axes, sizes, cut, to_heads, h_send, h_recv)

    def shrunk(t, unused):
        place, peer = chip(t)
        terms = jnp.dot(u_all[place], shrink_w[...], preferred_element_type=F32).astype(BF16)
        part_two[place] = terms.reshape(2, rows, width)
        to_mate(t, part_two, first_two, s_send, s_recv).start()
        return unused

    lax.fori_loop(0, 4, shrunk, 0)
    for t in range(1, 4):
        add_and_send(t, part_two, first_two, summed_two, last_two, s_send, s_recv)
    to_heads[here] = cut[here]

    def keep_or_send(spot, values):
        @pl.when(y == spot % 2)
        def _():
            shrink_kept[spot // 2] = values

        @pl.when(y != spot % 2)
        def _():
            shrink_sent[spot // 2] = values

    by_columns(e_all, u_all, shrink_kept.shape[1], keep_or_send)
    result[...] = (
        mid[...] + gathered_sum(part_two, first_two, last_two, s_send, s_recv) + shrink_bias[...]
    ).astype(BF16)
    pieces_in(axes, sizes, cut, to_heads, h_send, h_recv, head_started)
    for n, copy in enumerate(y_copies):
        copy.wait_recv()
        half = (expand_terms[n, y].astype(F32) + expand_came[n].astype(F32)).astype(BF16)
        for step, out in enumerate(expand_half):

            @pl.when(lax.rem(lax.axis_index("o") + step, len(expand_half)) == n)
            def _(out=out, half=half):
                out[...] = half


    for copy in out_sent + c_gather.started:
        copy.wait_send()
    for t in range(1, 4):
        place, peer = chip(t)
        remote(c_own, c_own, c_send.at[3 + t], c_recv.at[3 + t], mate).wait_send()
    for t in range(4):
        to_mate(t, part, first, r_send, r_recv).wait_send()
        to_mate(t, part_two, first_two, s_send, s_recv).wait_send()
    for t in range(1, 4):
        to_chip(t, summed, last, r_send, r_recv).wait_send()
        to_chip(t, summed_two, last_two, s_send, s_recv).wait_send()
    for copy in y_copies:
        copy.wait_send()


def middle_part(
    pieces, own, own_grad, out_own, out_far, expand, shrink, vectors, every, spec, ident
):
    spots, rows, span = pieces.shape
    width = own.shape[1]
    piece = expand.shape[2]
    outer = every[1][0]
    cuts = outer * 2 // expand.shape[0]
    expand_cut = (outer, 2, expand.shape[1], piece // cuts)
    everyone = jax.ShapeDtypeStruct((4, 2, rows, width), BF16)
    hidden = jax.ShapeDtypeStruct((4, 2 * rows, piece), BF16)
    flat_f32 = jax.ShapeDtypeStruct((rows, width), F32)
    flat_low = jax.ShapeDtypeStruct((rows, width), BF16)

    def scatter_buffers():
        return [
            pltpu.VMEM(everyone.shape, BF16),
            pltpu.VMEM((4, rows, width), BF16),
            pltpu.VMEM((3, rows, width), BF16),
            pltpu.VMEM((3, rows, width), BF16),
        ]

    return pl.pallas_call(
        functools.partial(middle_kernel, every, spec),
        out_shape=[
            flat_low,
            flat_low,
            flat_f32,
            flat_low,
            jax.ShapeDtypeStruct((4, width), F32),
            jax.ShapeDtypeStruct((1, piece), F32),
            jax.ShapeDtypeStruct(pieces.shape, BF16),
            jax.ShapeDtypeStruct((spots // 2, width // spots, piece), BF16),
            jax.ShapeDtypeStruct((spots // 2, width // spots, piece), BF16),
        ]
        + [jax.ShapeDtypeStruct(expand_cut[2:], BF16)] * outer,
        in_specs=[VMEM] * 3 + [ANY] * 4 + [VMEM] * 5,
        out_specs=[VMEM] * (9 + outer),
        scratch_shapes=[
            pltpu.VMEM(pieces.shape, BF16),
            pltpu.VMEM((width, width), BF16),
            pltpu.VMEM((width, piece), BF16),
            pltpu.VMEM((piece, width), BF16),
            pltpu.VMEM((rows, width), F32),
            pltpu.VMEM((rows, width), BF16),
            pltpu.VMEM(everyone.shape, BF16),
            pltpu.VMEM(everyone.shape, BF16),
            pltpu.VMEM(hidden.shape, F32),
            pltpu.VMEM(hidden.shape, BF16),
            pltpu.VMEM(hidden.shape, BF16),
            *scatter_buffers(),
            *scatter_buffers(),
            pltpu.VMEM(pieces.shape, BF16),
            pltpu.VMEM(expand_cut, BF16),
            pltpu.VMEM(expand_cut[:1] + expand_cut[2:], BF16),
            pltpu.SemaphoreType.DMA((spots,)),
            pltpu.SemaphoreType.DMA((spots,)),
            *gather_scratch(spec),
            *gather_scratch(spec),
            pltpu.SemaphoreType.DMA((7,)),
            pltpu.SemaphoreType.DMA((2,)),
            pltpu.SemaphoreType.DMA((2,)),
            pltpu.SemaphoreType.DMA((7,)),
            pltpu.SemaphoreType.DMA((7,)),
            pltpu.SemaphoreType.DMA((7,)),
            pltpu.SemaphoreType.DMA((7,)),
            pltpu.SemaphoreType.DMA((spots,)),
            pltpu.SemaphoreType.DMA((spots,)),
            pltpu.SemaphoreType.DMA(expand_cut[:1]),
            pltpu.SemaphoreType.DMA(expand_cut[:1]),
        ],
        name="middle%d" % ident,
        compiler_params=pltpu.CompilerParams(
            collective_id=ident, has_side_effects=True, vmem_limit_bytes=67_000_000
        ),
        cost_estimate=pl.CostEstimate(
            flops=8 * rows * 8 * width * piece,
            bytes_accessed=100 * rows * width * 2,
            transcendentals=8 * rows * piece,
        ),
    )(pieces, own, own_grad, out_own, out_far, expand, shrink, *vectors)


class Owned:
    def __init__(self, outer, terms, out, came, half, last, whole, y_sems, o_sems, i_sems):
        self.outer = outer
        self.terms, self.out = terms, out
        self.came, self.half, self.last, self.whole = came, half, last, whole
        self.y_sems, self.o_sems, self.i_sems = y_sems, o_sems, i_sems
        self.o, self.i, self.y = (lax.axis_index(a) for a in ("o", "i", "y"))

    def come(self, kept, came):
        self.first = []
        for n in range(2 * self.outer):
            self.half[n // 2, n % 2] = (kept[n].astype(F32) + came[n].astype(F32)).astype(BF16)

    def start(self):
        mate = {"y": 1 - self.y}
        self.first = [
            remote(
                self.terms.at[2 * n + 1 - self.y],
                self.came.at[n],
                self.y_sems.at[0, n],
                self.y_sems.at[1, n],
                mate,
            )
            for n in range(2 * self.outer)
        ]
        for copy in self.first:
            copy.start()

    def over_o(self):
        for n, copy in enumerate(self.first):
            copy.wait_recv()
            self.half[n // 2, n % 2] = (
                self.terms[2 * n + self.y].astype(F32) + self.came[n].astype(F32)
            ).astype(BF16)
        self.send_o()

    def send_o(self):
        self.second = []
        for step in range(1, self.outer):
            there = lax.rem(self.o + step, self.outer)
            copy = remote(
                self.half.at[there],
                self.last.at[step - 1],
                self.o_sems.at[0, step],
                self.o_sems.at[1, step],
                {"o": there},
            )
            copy.start()
            self.second.append(copy)

    def over_i(self):
        total = self.half[self.o].astype(F32)
        for step, copy in enumerate(self.second):
            copy.wait_recv()
            total = total + self.last[step].astype(F32)
        self.whole[...] = total.astype(BF16)
        self.third = remote(
            self.whole.at[1 - self.i],
            self.out.at[self.i],
            self.i_sems.at[0],
            self.i_sems.at[1],
            {"i": 1 - self.i},
        )
        self.third.start()
        self.out[self.i] = self.whole[self.i]

    def finish(self):
        self.third.wait_recv()
        for copy in self.first + self.second + [self.third]:
            copy.wait_send()


def owned_scratch(outer, cell, rows, first=True):
    return [
        pltpu.VMEM((2 * outer if first else 1, cell, rows), BF16),
        pltpu.VMEM((outer, 2, cell, rows), BF16),
        pltpu.VMEM((max(outer - 1, 1), 2, cell, rows), BF16),
        pltpu.VMEM((2, cell, rows), BF16),
        pltpu.SemaphoreType.DMA((2, 2 * outer)),
        pltpu.SemaphoreType.DMA((2, outer)),
        pltpu.SemaphoreType.DMA((2,)),
    ]


def final_kernel(
    axes,
    sizes,
    heads,
    share,
    dqkv,
    columns,
    normed_low,
    shrink_kept,
    shrink_came,
    expand_kept,
    low_middle,
    att,
    own,
    grad_middle,
    gain,
    row_sums,
    hidden_sum,
    *rest,
):
    others = sizes[0] - 1
    final_body(axes, sizes, heads, share, dqkv, columns, normed_low, shrink_kept, shrink_came,
        [expand_kept, *rest[:others]], low_middle, att, own, grad_middle, gain, row_sums,
        hidden_sum, *rest[others:])


def final_body(
    axes, sizes, heads, share, dqkv, columns, normed_low, shrink_kept, shrink_came,
    expand_parts, low_middle, att, own, grad_middle, gain, row_sums,
    hidden_sum,
    grad_inputs,
    routed,
    shrink_out,
    outw_out,
    query_out,
    value_out,
    rows_out,
    hidden_out,
    expand_out,
    part,
    first,
    last,
    normed_part,
    q_part,
    q_first,
    q_sum,
    q_last,
    blocks,
    gy_all,
    att_cut,
    att_all,
    outw_terms,
    line,
    line_came,
    line_out,
    r_send,
    r_recv,
    q_send,
    q_recv,
    hop,
    land,
    a_send,
    a_recv,
    l_send,
    l_recv,
    g_send,
    g_recv,
    g_local,
    load_sem,
    expand_sum,
    expand_came,
    e_send,
    e_recv,
    *owned,
):
    outer, inner, ys, xs, ks = sizes
    o, i, y, x, k = (lax.axis_index(a) for a in axes)
    offs = offsets(sizes)
    chips = outer * inner
    spots = chips * ys
    place = (o * inner + i) * ys + y
    shard = x * ks + k
    me = place * xs * ks + shard
    rows, width = own.shape
    span = heads * HEAD_DIM
    y_mate, k_mate, x_mate = {"y": 1 - y}, {"k": 1 - k}, {"x": 1 - x}
    shrink = Owned(outer, None, shrink_out, *owned[:7])
    outw = Owned(outer, outw_terms, outw_out, *owned[7:])

    def load_normed(n):
        some = normed_part.shape[0]
        return pltpu.make_async_copy(
            normed_low.at[pl.ds(n * some, some)], normed_part, load_sem
        )

    load_normed(0).start()
    greet([moved(axes, sizes, off) for off in offs])

    group = (("i", "x", "k"), (inner, xs, ks))
    side = Gather(("i", "x"), (inner, xs), "k", low_middle, gy_all, g_send, g_recv, g_local)
    side.start()
    cell = att_cut.shape[2]
    for half in range(inner):
        for f in range(xs * ks):
            low = (f * inner + half) * cell
            att_cut[half * xs * ks + f] = att[:, low : low + cell]
    att_started = pieces_out(*group, att_cut, att_all, a_send, a_recv)
    here = (i * xs + x) * ks + k
    att_all[here] = att_cut[here]

    def chip(t):
        to, ti = lax.rem(o + t // inner, outer), lax.rem(i + t % inner, inner)
        return to * inner + ti, {"o": to, "i": ti}

    def back_chip(t):
        to = lax.rem(o + outer - t // inner, outer)
        ti = lax.rem(i + inner - t % inner, inner)
        return to * inner + ti

    def to_mate(t):
        return remote(
            part.at[chip(t)[0], 1 - y], first.at[t], r_send.at[t], r_recv.at[t], y_mate
        )

    def to_chip(t):
        slot = chips + t - 1
        return remote(
            part.at[chip(t)[0], y], last.at[t - 1], r_send.at[slot], r_recv.at[slot], chip(t)[1]
        )

    def terms(step, unused):
        t = lax.rem(step + 1, chips)
        spot = chip(t)[0]
        at = pl.multiple_of(spot * 2 * rows, 2 * rows)
        values = nt(dqkv[pl.ds(at, 2 * rows), :], columns[...]).astype(BF16)
        part[spot] = values.reshape(2, rows, width)
        to_mate(t).start()
        return unused

    lax.fori_loop(0, chips, terms, 0)

    shards = xs * ks
    cuts = spots // (2 * shards)
    total = expand_parts[0][...].astype(F32)
    for other in expand_parts[1:]:
        total = total + other[...].astype(F32)
    expand_sum[...] = total.astype(BF16)
    index = o * ys + y
    goal = shard * (spots // shards) + i * cuts + index % cuts
    goal_shard = index // cuts
    away = goal * shards + goal_shard != me
    route = remote(
        expand_sum,
        expand_came,
        e_send,
        e_recv,
        {
            "o": goal // (inner * ys),
            "i": (goal // ys) % inner,
            "y": goal % ys,
            "x": goal_shard // ks,
            "k": goal_shard % ks,
        },
    )

    @pl.when(away)
    def _():
        route.start()

    @pl.when(jnp.logical_not(away))
    def _():
        expand_came[...] = expand_sum[...]

    shrink.come(shrink_kept, shrink_came)
    shrink.send_o()

    quarter = q_part.shape[3]
    some = normed_part.shape[0]
    pieces = dqkv.shape[0] // some
    for section in range(3):
        low = section * span
        values = 0.0
        for n in range(pieces):
            if n or section == 0 or pieces > 1:
                copy = load_normed(n)
                if n or section:
                    copy.start()
                copy.wait()
            values = values + tn(
                dqkv[n * some : (n + 1) * some, low : low + span], normed_part[...]
            )
        for f in range(xs * ks):
            q_part[f // ks, f % ks, low : low + span, :] = values[
                :, f * quarter : (f + 1) * quarter
            ].astype(BF16)
    q_copies = [
        remote(q_part.at[1 - x, 1 - k], q_first.at[1], q_send.at[1], q_recv.at[1], k_mate),
        remote(q_part.at[x, 1 - k], q_first.at[0], q_send.at[0], q_recv.at[0], k_mate),
    ]
    for copy in q_copies:
        copy.start()

    def add_and_send(step, unused):
        t = step + 1
        to_mate(t).wait_recv()
        spot = chip(t)[0]
        part[spot, y] = (part[spot, y].astype(F32) + first[t].astype(F32)).astype(BF16)
        to_chip(t).start()
        return unused

    lax.fori_loop(0, chips - 1, add_and_send, 0)
    q_copies[0].wait_recv()
    q_sum[...] = (q_part[1 - x, k].astype(F32) + q_first[1].astype(F32)).astype(BF16)
    q_over = remote(q_sum, q_last, q_send.at[2], q_recv.at[2], x_mate)
    q_over.start()

    side.hand_on()
    pieces_in(*group, att_cut, att_all, a_send, a_recv, att_started)
    side.finish()

    def put_terms(spot, values):
        outw_terms[spot] = values

    by_columns(gy_all, att_all, outw_terms.shape[1], put_terms)
    outw.start()

    q_copies[1].wait_recv()
    q_over.wait_recv()
    total = q_part[x, k].astype(F32) + q_first[0].astype(F32) + q_last[...].astype(F32)
    blocks[...] = total.astype(BF16).reshape(blocks.shape)

    def where(spot):
        return {
            "o": spot // (inner * ys),
            "i": (spot // ys) % inner,
            "y": spot % ys,
        }

    def each_sent(act):
        for section in range(3):
            for h in range(heads):
                head = place * heads + h
                block = section * HEADS + head
                low = (block * HEAD_DIM) // share
                high = (block * HEAD_DIM + HEAD_DIM - 1) // share
                index = section * heads + h
                for which, owner, needed in (
                    (0, low, head < HEADS),
                    (1, high, (head < HEADS) & (high != low)),
                ):

                    @pl.when(needed)
                    def _(which=which, owner=owner, block=block, index=index):
                        act(index, 2 * index + which, owner, block - (share * owner) // HEAD_DIM)

    def block_copy(index, slot, owner, target):
        return remote(
            blocks.at[index], routed.at[target], hop.at[slot], land.at[target], where(owner)
        )

    def send_block(index, slot, owner, target):
        @pl.when(owner != place)
        def _():
            block_copy(index, slot, owner, target).start()

        @pl.when(owner == place)
        def _():
            routed[target] = blocks[index]

    def sent_block(index, slot, owner, target):
        @pl.when(owner != place)
        def _():
            block_copy(index, slot, owner, target).wait_send()

    each_sent(send_block)

    to_mate(0).wait_recv()
    grad = part[chip(0)[0], y].astype(F32) + first[0].astype(F32)
    for t in range(1, chips):
        to_chip(t).wait_recv()
        grad = grad + last[t - 1].astype(F32)
    plain, scale = normed(own[...].astype(F32))
    grad_inputs[...] = grad_middle[...] + norm_back(grad, gain[...], plain, scale)

    def fill(base, values):
        size = values.shape[1]
        for n in range(-(-size // 128)):
            low, high = n * 128, min(n * 128 + 128, size)
            line[pl.ds(base + n, 1), 0 : high - low] = values[:, low:high]

    q_rows, w_rows = -(-span // 128), -(-width // 128)
    piece = hidden_sum.shape[1]
    p_rows = -(-piece // 128)
    value_base = spots * q_rows
    rows_base = 2 * spots * q_rows
    hidden_base = rows_base + 6 * w_rows
    line[...] = jnp.zeros(line.shape, F32)
    fill(place * q_rows, jnp.sum(dqkv[:, 0:span].astype(F32), axis=0, keepdims=True))
    fill(
        value_base + place * q_rows,
        jnp.sum(dqkv[:, 2 * span : 3 * span].astype(F32), axis=0, keepdims=True),
    )
    for n in range(4):
        fill(rows_base + n * w_rows, row_sums[n : n + 1, :])
    fill(rows_base + 4 * w_rows, jnp.sum(grad * plain, axis=0, keepdims=True))
    fill(rows_base + 5 * w_rows, jnp.sum(grad, axis=0, keepdims=True))
    fill(hidden_base + (shard * inner + i) * p_rows, hidden_sum[...])
    line_rows = line_came.shape[1]

    def share_of(ref, device):
        return ref.at[pl.ds(pl.multiple_of(device * line_rows, line_rows), line_rows)]

    line_started = []
    for t, off in enumerate(offs):
        peer = moved(axes, sizes, off)
        device = flat(peer, axes, sizes)
        copy = remote(
            share_of(line, device), line_came.at[t], l_send.at[t], l_recv.at[t], peer
        )
        copy.start()
        line_started.append(copy)
    shrink.over_i()
    outw.over_o()
    for copy in line_started:
        copy.wait_recv()
    mine = pl.ds(pl.multiple_of(me * line_rows, line_rows), line_rows)
    line_out[mine, :] = line[mine, :] + jnp.sum(line_came[...], axis=0)
    count = len(offs)
    for t, off in enumerate(offs):
        peer = moved(axes, sizes, off)
        copy = remote(
            share_of(line_out, me),
            share_of(line_out, me),
            l_send.at[count + t],
            l_recv.at[count + t],
            peer,
        )
        copy.start()
        line_started.append(copy)
    outw.over_i()

    base = (share * place) // HEAD_DIM
    for slot in range(routed.shape[0]):
        block = base + slot
        owner = (block % HEADS) // heads

        @pl.when((block * HEAD_DIM < share * (place + 1)) & (owner != place))
        def _(slot=slot):
            remote(
                blocks.at[0], routed.at[slot], hop.at[0], land.at[slot], where(place)
            ).wait_recv()

    for t, off in enumerate(offs):
        peer = moved(axes, sizes, off, -1)
        block = share_of(line_out, flat(peer, axes, sizes))
        remote(block, block, l_send.at[count + t], l_recv.at[count + t], peer).wait_recv()

    def take(base, ref, row, start, size):
        for n in range(-(-size // 128)):
            low, high = n * 128, min(n * 128 + 128, size)
            ref[row : row + 1, start + low : start + high] = line_out[
                base + n : base + n + 1, 0 : high - low
            ]

    for c in range(spots):
        take(c * q_rows, query_out, 0, c * span, span)
        take(value_base + c * q_rows, value_out, 0, c * span, span)
    for n in range(6):
        take(rows_base + n * w_rows, rows_out, n, 0, width)
    for n in range(xs * ks * inner):
        take(hidden_base + n * p_rows, hidden_out, 0, n * piece, piece)

    @pl.when(away)
    def _():
        route.wait()

    expand_out[...] = expand_came[...].astype(F32)
    shrink.finish()
    outw.finish()
    each_sent(sent_block)
    for copy in line_started + q_copies + [q_over]:
        copy.wait_send()
    for t in range(chips):
        to_mate(t).wait_send()
    for t in range(1, chips):
        to_chip(t).wait_send()


def final_part(
    dqkv,
    columns,
    normed_low,
    shrink_kept,
    shrink_came,
    expand_parts,
    low_middle,
    att,
    own,
    grad_middle,
    gain,
    row_sums,
    hidden_sum,
    axes,
    sizes,
    heads,
    share,
    ident,
):
    outer, inner, ys, xs, ks = sizes
    spots = outer * inner * ys
    cell, piece = shrink_kept.shape[1:]
    rows, width = own.shape
    chips = outer * inner
    devices = spots * xs * ks
    group = inner * xs * ks
    span = heads * HEAD_DIM
    part_rows = width // (xs * ks)
    slots = max(
        (share * (c + 1) - 1) // HEAD_DIM - (share * c) // HEAD_DIM + 1 for c in range(spots)
    )
    line_rows = (
        2 * spots * -(-span // 128) + 6 * -(-width // 128) + xs * ks * inner * -(-piece // 128)
    )
    line_rows = 8 * -(-line_rows // (8 * devices))
    block = (rows, width)
    q_block = (3 * span, part_rows)
    out_rows = width // group
    return pl.pallas_call(
        functools.partial(final_kernel, axes, sizes, heads, share),
        out_shape=[
            jax.ShapeDtypeStruct(block, F32),
            jax.ShapeDtypeStruct((slots, HEAD_DIM, part_rows), BF16),
            jax.ShapeDtypeStruct((inner, cell, piece), BF16),
            jax.ShapeDtypeStruct((inner, cell, out_rows), BF16),
            jax.ShapeDtypeStruct((1, spots * span), F32),
            jax.ShapeDtypeStruct((1, spots * span), F32),
            jax.ShapeDtypeStruct((6, width), F32),
            jax.ShapeDtypeStruct((1, group * piece), F32),
            jax.ShapeDtypeStruct(expand_parts[0].shape, F32),
        ],
        in_specs=[VMEM] * 2 + [ANY] + [VMEM] * (9 + outer),
        out_specs=[VMEM] * 9,
        scratch_shapes=[
            pltpu.VMEM((chips, ys) + block, BF16),
            pltpu.VMEM((chips,) + block, BF16),
            pltpu.VMEM((chips - 1,) + block, BF16),
            pltpu.VMEM((min(1024, dqkv.shape[0]), width), BF16),
            pltpu.VMEM((xs, ks) + q_block, BF16),
            pltpu.VMEM((2,) + q_block, BF16),
            pltpu.VMEM(q_block, BF16),
            pltpu.VMEM(q_block, BF16),
            pltpu.VMEM((3 * heads, HEAD_DIM, part_rows), BF16),
            pltpu.VMEM((inner * xs, ks) + block, BF16),
            pltpu.VMEM((group, rows, out_rows), BF16),
            pltpu.VMEM((group, rows, out_rows), BF16),
            pltpu.VMEM((spots, cell, out_rows), BF16),
            pltpu.VMEM((devices * line_rows, 128), F32),
            pltpu.VMEM((devices - 1, line_rows, 128), F32),
            pltpu.VMEM((devices * line_rows, 128), F32),
            pltpu.SemaphoreType.DMA((2 * chips,)),
            pltpu.SemaphoreType.DMA((2 * chips,)),
            pltpu.SemaphoreType.DMA((3,)),
            pltpu.SemaphoreType.DMA((3,)),
            pltpu.SemaphoreType.DMA((6 * heads,)),
            pltpu.SemaphoreType.DMA((slots,)),
            pltpu.SemaphoreType.DMA((group,)),
            pltpu.SemaphoreType.DMA((group,)),
            pltpu.SemaphoreType.DMA((2 * devices,)),
            pltpu.SemaphoreType.DMA((2 * devices,)),
            *gather_scratch((("i", "x"), (inner, xs), "k")),
            pltpu.SemaphoreType.DMA,
            pltpu.VMEM(expand_parts[0].shape, BF16),
            pltpu.VMEM(expand_parts[0].shape, BF16),
            pltpu.SemaphoreType.DMA,
            pltpu.SemaphoreType.DMA,
            *owned_scratch(outer, cell, piece, False),
            *owned_scratch(outer, cell, out_rows),
        ],
        name="final%d" % ident,
        compiler_params=pltpu.CompilerParams(
            collective_id=ident, has_side_effects=True, vmem_limit_bytes=67_000_000
        ),
        cost_estimate=pl.CostEstimate(
            flops=12 * rows * spots * width * span,
            bytes_accessed=100 * rows * width * 2,
            transcendentals=0,
        ),
    )(
        dqkv,
        columns,
        normed_low,
        shrink_kept,
        shrink_came,
        expand_parts[0],
        low_middle,
        att,
        own,
        grad_middle,
        gain,
        row_sums,
        hidden_sum,
        *expand_parts[1:],
    )


def nt(left, right):
    return lax.dot_general(left, right, (((1,), (1,)), ((), ())), preferred_element_type=F32)


def nn(left, right):
    return lax.dot_general(left, right, (((1,), (0,)), ((), ())), preferred_element_type=F32)


def tn(left, right):
    return lax.dot_general(left, right, (((0,), (0,)), ((), ())), preferred_element_type=F32)


def rows_of(inv, ref, pair, low, high):
    first = pl.multiple_of(inv[2 * pair] * HEAD_DIM, HEAD_DIM)
    second = pl.multiple_of(inv[2 * pair + 1] * HEAD_DIM, HEAD_DIM)
    return jnp.concatenate(
        [ref[pl.ds(first, 64), low:high], ref[pl.ds(second, 64), low:high]], axis=0
    )


def put_rows(inv, ref, pair, low, high, values):
    first = pl.multiple_of(inv[2 * pair] * HEAD_DIM, HEAD_DIM)
    second = pl.multiple_of(inv[2 * pair + 1] * HEAD_DIM, HEAD_DIM)
    ref[pl.ds(first, 64), low:high] = values[:64]
    ref[pl.ds(second, 64), low:high] = values[64:]


def head_slice(values, part, heads, head):
    low = (part * heads + head) * HEAD_DIM
    return values[:, low : low + HEAD_DIM]


def diagonal(block):
    return lax.broadcasted_iota(jnp.int32, (block, block), 0) <= lax.broadcasted_iota(
        jnp.int32, (block, block), 1
    )


def attend_kernel(heads, block, inv, qkv, out, out_low, lse, qs, ks, vt, ot):
    length = qkv.shape[0]
    width = heads * HEAD_DIM

    def sort(pair, unused):
        at = pl.multiple_of(pair * 128, 128)
        values = rows_of(inv, qkv, pair, 0, 3 * width)
        for h in range(heads):
            qs[h, pl.ds(at, 128), :] = head_slice(values, 0, heads, h) * BF16(0.125)
            ks[h, pl.ds(at, 128), :] = head_slice(values, 1, heads, h)
            vt[h, :, pl.ds(at, 128)] = head_slice(values, 2, heads, h).astype(F32).T.astype(BF16)
        return unused

    lax.fori_loop(0, length // 128, sort, 0)
    allowed = diagonal(block)

    def row(qi, unused):
        q_at = pl.multiple_of(qi * block, block)

        def first(h):
            scores = nt(ks[h, pl.ds(q_at, block), :], qs[h, pl.ds(q_at, block), :])
            scores = jnp.where(allowed, scores, -1e30)
            high = jnp.max(scores, axis=0, keepdims=True)
            probs = jnp.exp(scores - high)
            return (
                high,
                jnp.sum(probs, axis=0, keepdims=True),
                nn(vt[h, :, pl.ds(q_at, block)], probs.astype(BF16)),
            )

        def column(kj, state):
            k_at = pl.multiple_of(kj * block, block)
            fresh_state = []
            for h in range(heads):
                high, weight, acc = state[h]
                scores = nt(ks[h, pl.ds(k_at, block), :], qs[h, pl.ds(q_at, block), :])
                fresh = jnp.maximum(high, jnp.max(scores, axis=0, keepdims=True))
                probs = jnp.exp(scores - fresh)
                fade = jnp.exp(high - fresh)
                fresh_state.append(
                    (
                        fresh,
                        weight * fade + jnp.sum(probs, axis=0, keepdims=True),
                        acc * fade + nn(vt[h, :, pl.ds(k_at, block)], probs.astype(BF16)),
                    )
                )
            return tuple(fresh_state)

        state = lax.fori_loop(0, qi, column, tuple(first(h) for h in range(heads)))
        for h in range(heads):
            high, weight, acc = state[h]
            ot[h, :, pl.ds(q_at, block)] = acc / weight
            lse[h : h + 1, pl.ds(q_at, block)] = high + jnp.log(weight)
        return unused

    lax.fori_loop(0, length // block, row, 0)

    def unsort(pair, unused):
        at = pl.multiple_of(pair * 128, 128)
        values = [ot[h, :, pl.ds(at, 128)].T for h in range(heads)]
        values = jnp.concatenate(values, axis=1)
        put_rows(inv, out, pair, 0, width, values)
        put_rows(inv, out_low, pair, 0, width, values.astype(BF16))
        return unused

    lax.fori_loop(0, length // 128, unsort, 0)


def attend(inv, qkv, heads):
    length = qkv.shape[0]
    width = heads * HEAD_DIM
    block = min(256, length)
    pairs = length * (length + block) // 2
    return pl.pallas_call(
        functools.partial(attend_kernel, heads, block),
        out_shape=(
            jax.ShapeDtypeStruct((length, width), F32),
            jax.ShapeDtypeStruct((length, width), BF16),
            jax.ShapeDtypeStruct((heads, length), F32),
        ),
        grid_spec=pltpu.PrefetchScalarGridSpec(
            num_scalar_prefetch=1,
            grid=(1,),
            in_specs=[pl.BlockSpec((length, 3 * width), lambda i, inv: (0, 0))],
            out_specs=(
                pl.BlockSpec((length, width), lambda i, inv: (0, 0)),
                pl.BlockSpec((length, width), lambda i, inv: (0, 0)),
                pl.BlockSpec((heads, length), lambda i, inv: (0, 0)),
            ),
            scratch_shapes=[
                pltpu.VMEM((heads, length, HEAD_DIM), BF16),
                pltpu.VMEM((heads, length, HEAD_DIM), BF16),
                pltpu.VMEM((heads, HEAD_DIM, length), BF16),
                pltpu.VMEM((heads, HEAD_DIM, length), F32),
            ],
        ),
        name="attend",
        cost_estimate=pl.CostEstimate(
            flops=4 * heads * pairs * HEAD_DIM * 4,
            bytes_accessed=length * width * 10,
            transcendentals=heads * pairs,
        ),
    )(inv, qkv)


def attend_back_kernel(
    heads, block, inv, qkv, grads, outs, lse, dqkv, qs, ks, vs, gs, kt, delta, dqt, dks, dvs
):
    length = qkv.shape[0]
    width = heads * HEAD_DIM
    count = length // block

    def sort(pair, unused):
        at = pl.multiple_of(pair * 128, 128)
        values = rows_of(inv, qkv, pair, 0, 3 * width)
        grad = rows_of(inv, grads, pair, 0, width)
        value = rows_of(inv, outs, pair, 0, width)
        product = (grad.astype(F32) * value).T
        for h in range(heads):
            qs[h, pl.ds(at, 128), :] = head_slice(values, 0, heads, h) * BF16(0.125)
            key = head_slice(values, 1, heads, h)
            ks[h, pl.ds(at, 128), :] = key
            kt[h, :, pl.ds(at, 128)] = key.astype(F32).T.astype(BF16)
            vs[h, pl.ds(at, 128), :] = head_slice(values, 2, heads, h)
            gs[h, pl.ds(at, 128), :] = head_slice(grad, 0, heads, h)
            delta[h : h + 1, pl.ds(at, 128)] = jnp.sum(
                product[h * HEAD_DIM : (h + 1) * HEAD_DIM], axis=0, keepdims=True
            )
            dqt[h, :, pl.ds(at, 128)] = jnp.zeros((HEAD_DIM, 128), F32)
        return unused

    lax.fori_loop(0, length // 128, sort, 0)
    allowed = diagonal(block)

    def column(kj, unused):
        k_at = pl.multiple_of(kj * block, block)

        def tile(h, q_at, masked):
            q = qs[h, pl.ds(q_at, block), :]
            g = gs[h, pl.ds(q_at, block), :]
            scores = nt(ks[h, pl.ds(k_at, block), :], q)
            probs = jnp.exp(scores - lse[h : h + 1, pl.ds(q_at, block)])
            if masked:
                probs = jnp.where(allowed, probs, 0.0)
            slopes = nt(vs[h, pl.ds(k_at, block), :], g)
            low = (probs * (slopes - delta[h : h + 1, pl.ds(q_at, block)])).astype(BF16)
            dqt[h, :, pl.ds(q_at, block)] += nn(kt[h, :, pl.ds(k_at, block)], low)
            return nn(low, q), nn(probs.astype(BF16), g)

        def row(qi, state):
            q_at = pl.multiple_of(qi * block, block)
            fresh = []
            for h in range(heads):
                dk, dv = tile(h, q_at, False)
                fresh.append((state[h][0] + dk, state[h][1] + dv))
            return tuple(fresh)

        state = tuple(tile(h, k_at, True) for h in range(heads))
        state = lax.fori_loop(kj + 1, count, row, state)
        for h in range(heads):
            dks[h, pl.ds(k_at, block), :] = state[h][0].astype(BF16)
            dvs[h, pl.ds(k_at, block), :] = state[h][1].astype(BF16)
        return unused

    lax.fori_loop(0, count, column, 0)

    def unsort(pair, unused):
        at = pl.multiple_of(pair * 128, 128)
        values = [(dqt[h, :, pl.ds(at, 128)].T * 0.125).astype(BF16) for h in range(heads)]
        values += [dks[h, pl.ds(at, 128), :] for h in range(heads)]
        values += [dvs[h, pl.ds(at, 128), :] for h in range(heads)]
        put_rows(inv, dqkv, pair, 0, 3 * width, jnp.concatenate(values, axis=1))
        return unused

    lax.fori_loop(0, length // 128, unsort, 0)


def attend_back(inv, qkv, grads, outs, lse, heads):
    length = qkv.shape[0]
    width = heads * HEAD_DIM
    block = min(256, length)
    pairs = length * (length + block) // 2
    row_shape = (heads, length, HEAD_DIM)
    return pl.pallas_call(
        functools.partial(attend_back_kernel, heads, block),
        out_shape=jax.ShapeDtypeStruct((length, 3 * width), BF16),
        grid_spec=pltpu.PrefetchScalarGridSpec(
            num_scalar_prefetch=1,
            grid=(1,),
            in_specs=[
                pl.BlockSpec((length, 3 * width), lambda i, inv: (0, 0)),
                pl.BlockSpec((length, width), lambda i, inv: (0, 0)),
                pl.BlockSpec((length, width), lambda i, inv: (0, 0)),
                pl.BlockSpec((heads, length), lambda i, inv: (0, 0)),
            ],
            out_specs=pl.BlockSpec((length, 3 * width), lambda i, inv: (0, 0)),
            scratch_shapes=[
                pltpu.VMEM(row_shape, BF16),
                pltpu.VMEM(row_shape, BF16),
                pltpu.VMEM(row_shape, BF16),
                pltpu.VMEM(row_shape, BF16),
                pltpu.VMEM((heads, HEAD_DIM, length), BF16),
                pltpu.VMEM((heads, length), F32),
                pltpu.VMEM((heads, HEAD_DIM, length), F32),
                pltpu.VMEM(row_shape, BF16),
                pltpu.VMEM(row_shape, BF16),
            ],
        ),
        name="attend_back",
        cost_estimate=pl.CostEstimate(
            flops=10 * heads * pairs * HEAD_DIM * 4,
            bytes_accessed=length * width * 20,
            transcendentals=heads * pairs,
        ),
    )(inv, qkv, grads, outs, lse)


def body(
    sizes,
    tokens,
    block_order,
    qkv_weight,
    query_bias,
    value_bias,
    out_weight,
    out_bias,
    expand_weight,
    expand_bias,
    shrink_weight,
    shrink_bias,
    first_gain,
    first_shift,
    second_gain,
    second_shift,
    cotangent,
):
    outer, inner, ys, xs, ks = (sizes[a] for a in ("o", "i", "y", "x", "k"))
    spots = outer * inner * ys
    shards = xs * ks
    rows, width = tokens.shape[1:]
    o, i, y = lax.axis_index("o"), lax.axis_index("i"), lax.axis_index("y")
    shard = lax.axis_index("x") * ks + lax.axis_index("k")
    place = (o * inner + i) * ys + y
    heads = -(-HEADS // spots)
    span = heads * HEAD_DIM
    padded = spots * span
    part = qkv_weight.shape[0]
    hidden = expand_weight.shape[1]
    piece = hidden // (shards * inner)
    every = (("o", "i", "y"), (outer, inner, ys))
    group = (("i", "x"), (inner, xs), "k")
    own = tokens[0]
    own_grad = cotangent[0]

    def columns(values, count):
        wide = values.reshape(values.shape[:-1] + (count, width))
        wide = jnp.pad(wide, [(0, 0)] * (wide.ndim - 1) + [(0, padded - width)])
        return lax.dynamic_slice_in_dim(wide, place * span, span, axis=wide.ndim - 1)

    qkv_bias = jnp.concatenate(
        [columns(query_bias, 1)[0], jnp.zeros((span,), F32), columns(value_bias, 1)[0]]
    )
    sizes_of = (outer, inner, ys, xs, ks)
    qkv, normed_low, qkv_columns, expand_columns = first_part(
        own,
        qkv_weight,
        expand_weight,
        [first_gain[None], first_shift[None], qkv_bias[None]],
        span,
        sizes_of,
        piece,
        0,
    )
    qkv_columns = qkv_columns.reshape(width, 3 * span)

    qkv, out_own = lax.optimization_barrier((qkv, out_weight))
    out_far = lax.ppermute(out_own, "x", [(0, 1), (1, 0)])
    expand_own_bias = lax.dynamic_slice_in_dim(
        expand_bias, (shard * inner + i) * piece, piece, axis=0
    )

    order_row = block_order[0]
    blocks = order_row.shape[0]
    inv = jnp.sum(
        jnp.where(
            order_row[:, None] == jnp.arange(blocks, dtype=jnp.int32)[None, :],
            jnp.arange(blocks, dtype=jnp.int32)[:, None],
            0,
        ),
        axis=0,
    ).astype(jnp.int32)
    attended, attended_bf, log_sum = attend(inv, qkv, heads)
    (
        attended_low,
        result,
        grad_middle,
        middle_low,
        row_sums,
        hidden_sums,
        grad_heads,
        shrink_kept,
        shrink_sent,
        *expand_parts,
    ) = middle_part(
        attended_bf.reshape(spots, rows, span),
        own,
        own_grad,
        out_own,
        out_far,
        expand_columns,
        shrink_weight,
        [
            v[None]
            for v in (out_bias, expand_own_bias, shrink_bias, second_gain, second_shift)
        ],
        every,
        group,
        1,
    )
    grad_heads = grad_heads.reshape(spots * rows, span)
    dqkv = attend_back(inv, qkv, grad_heads, attended, log_sum, heads)
    shrink_came = lax.ppermute(shrink_sent, "y", [(0, 1), (1, 0)])
    for step in range(1, outer):
        ring = [(d, (d + step) % outer) for d in range(outer)]
        expand_parts[step] = lax.ppermute(expand_parts[step], "o", ring)
    axes = ("o", "i", "y", "x", "k")
    share = 3 * width // spots
    (
        grad_inputs,
        routed,
        shrink_cells,
        outw_cells,
        query_sums,
        value_sums,
        row_totals,
        hidden_totals,
        grad_expand,
    ) = final_part(
        dqkv,
        qkv_columns,
        normed_low,
        shrink_kept,
        shrink_came,
        expand_parts,
        middle_low,
        attended_low,
        own,
        grad_middle,
        first_gain[None],
        row_sums,
        hidden_sums,
        axes,
        sizes_of,
        heads,
        share,
        2,
    )

    def upright(cells):
        return cells.transpose(0, 2, 1).reshape(-1, cells.shape[1]).astype(F32)

    start = share * place - HEAD_DIM * ((share * place) // HEAD_DIM)
    grad_qkv = lax.dynamic_slice_in_dim(routed.reshape(-1, part), start, share, axis=0)
    return (
        result[None],
        grad_inputs[None],
        grad_qkv.T.astype(F32),
        upright(outw_cells),
        grad_expand,
        upright(shrink_cells),
        query_sums[0, :width],
        value_sums[0, :width],
        row_totals[0],
        hidden_totals[0],
        row_totals[1],
        row_totals[4],
        row_totals[5],
        row_totals[2],
        row_totals[3],
    )


def solution(mesh):
    spots, shards = mesh.shape["ctx"], mesh.shape["fsdp"]
    sizes = {"o": spots // 4, "i": 2, "y": 2, "x": shards // 2, "k": 2}
    fine = Mesh(mesh.devices.reshape(tuple(sizes.values())), tuple(sizes))
    seq, pos = ("x", "k"), ("o", "i", "y")
    weight = P(seq, None)
    placed = (
        P(seq, pos, None),
        P(seq, None),
        weight,
        P(),
        P(),
        weight,
        P(),
        weight,
        P(),
        weight,
        P(),
        P(),
        P(),
        P(),
        P(),
        P(seq, pos, None),
    )
    given = (P(seq, pos, None),) * 2 + (P(seq, pos),) * 4 + (P(),) * 9
    return jax.shard_map(
        functools.partial(body, sizes),
        mesh=fine,
        in_specs=placed,
        out_specs=given,
        check_vma=False,
    )
```

```python
import functools
import itertools

import jax
import jax.numpy as jnp
from jax import lax
from jax.experimental import pallas as pl
from jax.experimental.pallas import tpu as pltpu
from jax.sharding import Mesh
from jax.sharding import PartitionSpec as P

HEADS = 25
HEAD_DIM = 64
EPSILON = 1e-05
MESH = pl.DeviceIdType.MESH
F32 = jnp.float32
BF16 = jnp.bfloat16
ANY = pl.BlockSpec(memory_space=pl.ANY)
VMEM = pl.BlockSpec(memory_space=pltpu.VMEM)


def offsets(sizes):
    return [o for o in itertools.product(*(range(s) for s in sizes)) if any(o)]


def moved(axes, sizes, offset, sign=1):
    return {
        a: lax.rem(lax.axis_index(a) + (o if sign > 0 else s - o), s)
        for a, s, o in zip(axes, sizes, offset)
    }


def flat(place, axes, sizes):
    index = 0
    for a, s in zip(axes, sizes):
        index = index * s + place[a]
    return index


def own_place(axes):
    return {a: lax.axis_index(a) for a in axes}


def greet(peers):
    barrier = pltpu.get_barrier_semaphore()
    for peer in peers:
        pl.semaphore_signal(barrier, inc=1, device_id=peer, device_id_type=MESH)
    pl.semaphore_wait(barrier, len(peers))


def remote(src, dst, send, recv, peer):
    return pltpu.make_async_remote_copy(
        src_ref=src,
        dst_ref=dst,
        send_sem=send,
        recv_sem=recv,
        device_id=peer,
        device_id_type=MESH,
    )


class Gather:
    def __init__(self, axes, sizes, pair, source, out, send, recv, local):
        self.axes, self.sizes = axes, sizes
        self.offs = offsets(sizes)
        self.side = lax.axis_index(pair)
        self.mate = {pair: 1 - self.side}
        self.source, self.out, self.send, self.recv, self.local = source, out, send, recv, local
        self.started = []

    def peers(self):
        return [moved(self.axes, self.sizes, o) for o in self.offs] + [self.mate]

    def mine(self):
        return self.out.at[flat(own_place(self.axes), self.axes, self.sizes), self.side]

    def start(self):
        pltpu.make_async_copy(self.source, self.mine(), self.local).start()
        last = len(self.offs)
        for t, peer in enumerate(self.peers()):
            copy = remote(self.source, self.mine(), self.send.at[t], self.recv.at[t], peer)
            copy.start()
            self.started.append(copy)

    def hand_on(self):
        last = len(self.offs)
        for t, off in enumerate(self.offs):
            came = flat(moved(self.axes, self.sizes, off, -1), self.axes, self.sizes)
            block = self.out.at[came, self.side]
            remote(self.source, block, self.send.at[t], self.recv.at[t], self.mate).wait_recv()
            slot = last + 1 + t
            copy = remote(block, block, self.send.at[slot], self.recv.at[slot], self.mate)
            copy.start()
            self.started.append(copy)

    def finish(self):
        last = len(self.offs)
        me = flat(own_place(self.axes), self.axes, self.sizes)
        pltpu.make_async_copy(self.source, self.mine(), self.local).wait()
        block = self.out.at[me, 1 - self.side]
        remote(self.source, block, self.send.at[last], self.recv.at[last], self.mate).wait_recv()
        for t, off in enumerate(self.offs):
            came = flat(moved(self.axes, self.sizes, off, -1), self.axes, self.sizes)
            slot = last + 1 + t
            block = self.out.at[came, 1 - self.side]
            remote(
                self.source, block, self.send.at[slot], self.recv.at[slot], self.mate
            ).wait_recv()
        for copy in self.started:
            copy.wait_send()


class Quad:
    def __init__(self, source, out, send, recv, local):
        self.i, self.x, self.k = (lax.axis_index(a) for a in ("i", "x", "k"))
        self.source, self.out, self.send, self.recv, self.local = source, out, send, recv, local
        self.i_mate, self.x_mate, self.k_mate = {"i": 1 - self.i}, {"x": 1 - self.x}, {"k": 1 - self.k}
        self.half = source.shape[0] // 2
        self.places = (
            2 * self.i + self.x,
            2 * self.i + 1 - self.x,
            2 * (1 - self.i) + self.x,
            2 * (1 - self.i) + 1 - self.x,
        )
        self.started = []

    def peers(self):
        return [self.i_mate, self.x_mate, self.k_mate]

    def copy(self, source, target, slot, peer):
        return remote(source, target, self.send.at[slot], self.recv.at[slot], peer)

    def go(self, source, target, slot, peer):
        copy = self.copy(source, target, slot, peer)
        copy.start()
        self.started.append(copy)

    def start(self):
        mine = self.out.at[self.places[0], self.k]
        pltpu.make_async_copy(self.source, mine, self.local).start()
        self.go(self.source, mine, 0, self.x_mate)
        self.go(self.source, mine, 1, self.i_mate)
        self.go(self.source, mine, 2, self.k_mate)

    def x_in(self):
        block = self.out.at[self.places[1], self.k]
        self.copy(self.source, block, 0, self.x_mate).wait_recv()
        part = block.at[pl.ds(0, self.half)]
        self.go(part, part, 4, self.i_mate)
        self.go(block, block, 3, self.k_mate)

    def i_in(self):
        block = self.out.at[self.places[2], self.k]
        self.copy(self.source, block, 1, self.i_mate).wait_recv()
        part = block.at[pl.ds(self.half, self.half)]
        self.go(part, part, 6, self.x_mate)
        self.go(block, block, 5, self.k_mate)

    def d_in(self):
        block = self.out.at[self.places[3], self.k]
        part = block.at[pl.ds(0, self.half)]
        self.copy(part, part, 4, self.i_mate).wait_recv()
        part = block.at[pl.ds(self.half, self.half)]
        self.copy(part, part, 6, self.x_mate).wait_recv()
        self.go(block, block, 7, self.k_mate)

    def across(self, place, slot):
        block = self.out.at[place, 1 - self.k]
        self.copy(self.source, block, slot, self.k_mate).wait_recv()

    def all_across(self):
        for place, slot in zip(self.places, (2, 3, 5, 7)):
            self.across(place, slot)

    def local_wait(self):
        mine = self.out.at[self.places[0], self.k]
        pltpu.make_async_copy(self.source, mine, self.local).wait()

    def finish(self):
        for copy in self.started:
            copy.wait_send()


def quad_scratch():
    return [
        pltpu.SemaphoreType.DMA((8,)),
        pltpu.SemaphoreType.DMA((8,)),
        pltpu.SemaphoreType.DMA,
    ]


def turned(block):
    return block.astype(F32).T.astype(block.dtype)


def gather_shape(block, spec):
    group = 1
    for s in spec[1]:
        group *= s
    return jax.ShapeDtypeStruct((group, 2) + block.shape, block.dtype)


def gather_scratch(spec):
    group = 1
    for s in spec[1]:
        group *= s
    return [
        pltpu.SemaphoreType.DMA((2 * group,)),
        pltpu.SemaphoreType.DMA((2 * group,)),
        pltpu.SemaphoreType.DMA,
    ]


def sent_estimate(size):
    return pl.CostEstimate(flops=0, bytes_accessed=20 * size, transcendentals=0)


class Line:
    def __init__(self, sizes, source, out, send, recv, local):
        self.outer, self.inner = sizes
        self.count = self.outer * self.inner
        self.at = lax.axis_index("o") * self.inner + lax.axis_index("i")
        self.y = lax.axis_index("y")
        self.mate = {"y": 1 - self.y}
        self.source, self.out, self.send, self.recv, self.local = source, out, send, recv, local

    def spot(self, at):
        return {"o": at // self.inner, "i": at % self.inner}

    def copies(self, at, here):
        block = self.out.at[at, self.y]
        source = self.source if here else block
        right, left = lax.rem(self.at + 1, self.count), lax.rem(
            self.at + self.count - 1, self.count
        )
        return [
            (
                (at <= self.at) & (self.at + 1 < self.count),
                remote(source, block, self.send.at[0, at], self.recv.at[0, at], self.spot(right)),
            ),
            (
                (at >= self.at) & (self.at > 0),
                remote(source, block, self.send.at[1, at], self.recv.at[0, at], self.spot(left)),
            ),
            (True, remote(source, block, self.send.at[2, at], self.recv.at[1, at], self.mate)),
        ]

    def each(self, at, here, act):
        for needed, copy in self.copies(at, here):
            if needed is True:
                act(copy)
            else:

                @pl.when(needed)
                def _(copy=copy):
                    act(copy)

    def start(self):
        pltpu.make_async_copy(
            self.source, self.out.at[self.at, self.y], self.local
        ).start()
        self.each(self.at, True, lambda copy: copy.start())

    def arrive(self, at):
        block = self.out.at[at, self.y]
        remote(self.source, block, self.send.at[0, at], self.recv.at[0, at], self.mate).wait_recv()
        self.each(at, False, lambda copy: copy.start())

    def across(self, at):
        block = self.out.at[at, 1 - self.y]
        remote(self.source, block, self.send.at[2, at], self.recv.at[1, at], self.mate).wait_recv()

    def finish(self):
        for at in range(self.count):
            self.each(at, False, lambda copy: copy.wait_send())


def first_kernel(
    sizes,
    own_turned,
    qkv_weight,
    weight,
    gain,
    shift,
    query_bias,
    value_bias,
    qkv,
    normed_out,
    all_columns,
    pieces,
    own,
    sequence,
    bias,
    qkv_whole,
    columns,
    columns_in,
    whole,
    cut,
    send,
    recv,
    local,
    head_send,
    head_recv,
    head_local,
    read,
    qkv_read,
    cut_send,
    cut_recv,
    cut_local,
):
    outer, inner, ys, xs, ks = sizes
    axes, shard_sizes = ("x", "k"), (xs, ks)
    offs = offsets(shard_sizes)
    line = Line((outer, inner), own, sequence, send, recv, local)
    heads = Gather(
        ("x",), (xs,), "k", columns, all_columns, head_send, head_recv, head_local
    )
    qkv_fetch = pltpu.make_async_copy(qkv_weight, qkv_whole, qkv_read)
    qkv_fetch.start()
    fetch = pltpu.make_async_copy(weight, whole, read)
    fetch.start()
    own[...] = turned(own_turned[...])
    peers = [moved(axes, shard_sizes, o) for o in offs] + [
        moved(("o", "i", "y"), (outer, inner, ys), o) for o in offsets((outer, inner, ys))
    ]
    greet(peers)
    line.start()
    qkv_fetch.wait()
    place = line.at * ys + line.y
    part, span = columns.shape[0], columns.shape[1] // 3
    width = qkv_whole.shape[1] // 3
    for spot in range(-(-width // span)):

        @pl.when(place == spot)
        def _(spot=spot):
            size = min(span, width - spot * span)
            for section in range(3):
                low = section * width + spot * span
                if size < span:
                    columns[:, section * span : (section + 1) * span] = jnp.zeros(
                        (part, span), BF16
                    )
                columns[:, section * span : section * span + size] = qkv_whole[:, low : low + size]
            bias[...] = jnp.zeros(bias.shape, F32)
            low = spot * span
            bias[:, 0:size] = query_bias[...].reshape(1, width)[:, low : low + size]
            bias[:, 2 * span : 2 * span + size] = value_bias[...].reshape(1, width)[
                :, low : low + size
            ]

    @pl.when(place * span >= width)
    def _():
        columns[...] = jnp.zeros(columns.shape, BF16)
        bias[...] = jnp.zeros(bias.shape, F32)

    heads.start()
    fetch.wait()
    cut_width = cut.shape[2]
    side = lax.axis_index("i")
    for half in range(2):

        @pl.when(side == half)
        def _():
            for f in range(cut.shape[0]):
                low = (2 * f + half) * cut_width
                cut[f] = whole[:, low : low + cut_width]

    me = flat(own_place(axes), axes, shard_sizes)
    here = pltpu.make_async_copy(cut.at[me], pieces.at[me], cut_local)
    here.start()
    started = []
    for t, off in enumerate(offs):
        peer = moved(axes, shard_sizes, off)
        there = flat(peer, axes, shard_sizes)
        copy = remote(cut.at[there], pieces.at[me], cut_send.at[t], cut_recv.at[t], peer)
        copy.start()
        started.append(copy)
    pltpu.make_async_copy(own, sequence.at[line.at, line.y], local).wait()
    for distance in range(1, line.count):
        for sign in (-1, 1):
            at = line.at + sign * distance

            @pl.when((at >= 0) & (at < line.count))
            def _(at=at):
                line.arrive(at)

        if distance == 1:
            heads.hand_on()

    heads.finish()
    load = pltpu.make_async_copy(all_columns, columns_in, qkv_read)
    load.start()
    load.wait()
    rows = own.shape[0]

    def project(at):
        values = sequence[at].reshape(ys * rows, width).astype(F32)
        plain, unused_scale = normed(values)
        low = (plain * gain[...].reshape(1, width) + shift[...].reshape(1, width)).astype(BF16)
        start = pl.multiple_of(at * ys * rows, ys * rows)
        normed_out[pl.ds(start, ys * rows), :] = low
        weights = columns_in[...].reshape(width, 3 * span)
        qkv[pl.ds(start, ys * rows), :] = (
            jnp.dot(low, weights, preferred_element_type=F32) + bias[...]
        ).astype(BF16)

    nearest = [sorted(range(line.count), key=lambda q: abs(q - p)) for p in range(line.count)]

    def step(n, unused):
        at = line.at
        for p in range(line.count):
            for m in range(1, line.count):
                at = jnp.where((line.at == p) & (n == m), nearest[p][m], at)
        line.across(at)
        project(at)
        return unused

    lax.fori_loop(0, line.count, step, 0)
    here.wait()
    for t, off in enumerate(offs):
        peer = moved(axes, shard_sizes, off, -1)
        came = flat(peer, axes, shard_sizes)
        remote(cut.at[came], pieces.at[came], cut_send.at[t], cut_recv.at[t], peer).wait_recv()
    for copy in started:
        copy.wait_send()
    line.finish()


def first_part(own_turned, qkv_weight, weight, vectors, span, sizes, piece, ident):
    outer, inner, ys, xs, ks = sizes
    shards, chips = xs * ks, outer * inner
    part = weight.shape[0]
    width, rows = own_turned.shape
    tokens = chips * ys * rows
    columns = jax.ShapeDtypeStruct((part, 3 * span), BF16)
    spec = (("x",), (xs,), "k")
    gathered = gather_shape(columns, spec)
    return pl.pallas_call(
        functools.partial(first_kernel, sizes),
        out_shape=[
            jax.ShapeDtypeStruct((tokens, 3 * span), BF16),
            jax.ShapeDtypeStruct((tokens, width), BF16),
            gathered,
            jax.ShapeDtypeStruct((shards, part, piece), BF16),
            jax.ShapeDtypeStruct((rows, width), BF16),
        ],
        in_specs=[VMEM, ANY, ANY] + [VMEM] * 4,
        out_specs=[VMEM, VMEM, ANY, ANY, VMEM],
        scratch_shapes=[
            pltpu.VMEM((chips, ys, rows, width), BF16),
            pltpu.VMEM((1, 3 * span), F32),
            pltpu.VMEM(qkv_weight.shape, BF16),
            pltpu.VMEM(columns.shape, BF16),
            pltpu.VMEM(gathered.shape, BF16),
            pltpu.VMEM(weight.shape, BF16),
            pltpu.VMEM((shards, part, piece), BF16),
            pltpu.SemaphoreType.DMA((3, chips)),
            pltpu.SemaphoreType.DMA((2, chips)),
            pltpu.SemaphoreType.DMA,
            *gather_scratch(spec),
            pltpu.SemaphoreType.DMA,
            pltpu.SemaphoreType.DMA,
            pltpu.SemaphoreType.DMA((shards,)),
            pltpu.SemaphoreType.DMA((shards,)),
            pltpu.SemaphoreType.DMA,
        ],
        name="first%d" % ident,
        compiler_params=pltpu.CompilerParams(
            collective_id=ident, has_side_effects=True, vmem_limit_bytes=67_000_000
        ),
        cost_estimate=pl.CostEstimate(
            flops=6 * tokens * width * span,
            bytes_accessed=40 * tokens * width,
            transcendentals=0,
        ),
    )(own_turned, qkv_weight, weight, *vectors)


def pieces_out(axes, sizes, source, out, send, recv):
    me = flat(own_place(axes), axes, sizes)
    started = []
    for t, off in enumerate(offsets(sizes)):
        peer = moved(axes, sizes, off)
        copy = remote(
            source.at[flat(peer, axes, sizes)], out.at[me], send.at[t], recv.at[t], peer
        )
        copy.start()
        started.append(copy)
    return started


def pieces_in(axes, sizes, source, out, send, recv, started):
    for t, off in enumerate(offsets(sizes)):
        peer = moved(axes, sizes, off, -1)
        came = flat(peer, axes, sizes)
        remote(source.at[came], out.at[came], send.at[t], recv.at[t], peer).wait_recv()
    for copy in started:
        copy.wait_send()


def normed(values):
    center = jnp.mean(values, axis=-1, keepdims=True)
    centred = values - center
    spread = jnp.mean(centred * centred, axis=-1, keepdims=True)
    scale = lax.rsqrt(spread + EPSILON)
    return centred * scale, scale


def norm_back(grad, gain, plain, scale):
    inner = grad * gain
    return scale * (
        inner
        - jnp.mean(inner, axis=-1, keepdims=True)
        - plain * jnp.mean(inner * plain, axis=-1, keepdims=True)
    )


def by_columns(left, right, cell, put):
    tokens = left.shape[0] * left.shape[1] * left.shape[2]
    wide = 400 // cell
    others = right[...].reshape(tokens, right.shape[-1])
    for c in range(left.shape[3] // 400):
        terms = tn(left[:, :, :, c * 400 : (c + 1) * 400].reshape(tokens, 400), others)
        for n in range(wide):
            put(c * wide + n, terms[n * cell : (n + 1) * cell].astype(BF16))


def middle_kernel(
    every,
    pieces,
    own,
    grad_turned,
    out_own,
    out_far,
    expand,
    shrink,
    out_bias,
    expand_bias_all,
    shrink_bias,
    gain,
    shift,
    att,
    result,
    grad_middle,
    low_middle,
    sums,
    hidden_sum,
    to_heads,
    shrink_kept,
    shrink_sent,
    *rest,
):
    outer = every[1][0]
    middle_body(every, pieces, own, grad_turned, out_own, out_far, expand, shrink, out_bias,
        expand_bias_all, shrink_bias, gain, shift, att, result, grad_middle, low_middle, sums,
        hidden_sum, to_heads, shrink_kept, shrink_sent, rest[:outer], *rest[outer:])


def middle_body(
    every, pieces, own, grad_turned, out_own, out_far, expand, shrink, out_bias,
    expand_bias_all, shrink_bias, gain, shift, att, result, grad_middle, low_middle, sums,
    hidden_sum, to_heads, shrink_kept, shrink_sent, expand_half,
    own_grad,
    expand_bias,
    came,
    out_w,
    expand_w,
    shrink_w,
    mid,
    c_own,
    c_all,
    e_all,
    gh,
    u_all,
    gz_all,
    part,
    first,
    summed,
    last,
    part_two,
    first_two,
    summed_two,
    last_two,
    cut,
    expand_terms,
    expand_came,
    send,
    recv,
    c_send,
    c_recv,
    c_local,
    e_send,
    e_recv,
    e_local,
    w_sem,
    w_send,
    w_recv,
    r_send,
    r_recv,
    s_send,
    s_recv,
    h_send,
    h_recv,
    y_send,
    y_recv,
):
    axes, sizes = every
    y = lax.axis_index("y")
    x, k, inner = lax.axis_index("x"), lax.axis_index("k"), lax.axis_index("i")
    mate = {"k": 1 - k}
    shard = 2 * x + k
    part_rows = out_own.shape[0]
    width = own.shape[1]
    rows = own.shape[0]
    piece = expand.shape[2]

    def chip(t):
        ti, tx = lax.rem(inner + t // 2, 2), lax.rem(x + t % 2, 2)
        return 2 * ti + tx, {"i": ti, "x": tx}

    loads = [
        pltpu.make_async_copy(out_own, out_w.at[pl.ds(shard * part_rows, part_rows)], w_sem.at[0]),
        pltpu.make_async_copy(
            out_far, out_w.at[pl.ds((shard ^ 2) * part_rows, part_rows)], w_sem.at[1]
        ),
        pltpu.make_async_copy(shrink.at[pl.ds(inner * piece, piece)], shrink_w, w_sem.at[2]),
    ]
    for f in range(expand.shape[0]):
        loads.append(
            pltpu.make_async_copy(
                expand.at[f], expand_w.at[pl.ds(f * part_rows, part_rows)], w_sem.at[3 + f]
            )
        )
    for copy in loads:
        copy.start()
    own_grad[...] = turned(grad_turned[...])
    greet([moved(axes, sizes, o) for o in offsets(sizes)] + [chip(t)[1] for t in range(1, 4)] + [mate])

    started = pieces_out(axes, sizes, pieces, came, send, recv)
    out_sent = []
    for n, (source, owner) in enumerate(((out_own, shard), (out_far, shard ^ 2))):
        copy = remote(
            source, out_w.at[pl.ds(owner * part_rows, part_rows)], w_send.at[n], w_recv.at[n], mate
        )
        copy.start()
        out_sent.append(copy)
    e_gather = Quad(own_grad, e_all, e_send, e_recv, e_local)
    e_gather.start()
    here = flat(own_place(axes), axes, sizes)
    came[here] = pieces[here]
    for n in range(expand_bias_all.shape[0] // piece):

        @pl.when(2 * shard + inner == n)
        def _(n=n):
            everything = expand_bias_all[...].reshape(1, expand_bias_all.shape[0])
            expand_bias[...] = everything[:, n * piece : (n + 1) * piece]

    e_gather.x_in()
    e_gather.i_in()
    pieces_in(axes, sizes, pieces, came, send, recv, started)
    span = came.shape[2]
    for d in range(came.shape[0]):
        low, high = d * span, min((d + 1) * span, width)
        if low < high:
            att[:, low:high] = came[d, :, : high - low]
    for copy in loads[:2]:
        copy.wait()
    for n, owner in enumerate((shard ^ 1, shard ^ 3)):
        remote(
            out_own,
            out_w.at[pl.ds(owner * part_rows, part_rows)],
            w_send.at[n],
            w_recv.at[n],
            mate,
        ).wait_recv()

    mid[...] = (
        own[...].astype(F32)
        + jnp.dot(att[...], out_w[...], preferred_element_type=F32)
        + out_bias[...].reshape(1, width)
    )
    plain, scale = normed(mid[...])
    gains = gain[...].reshape(1, width)
    c_own[...] = (plain * gains + shift[...].reshape(1, width)).astype(BF16)
    c_gather = Quad(c_own, c_all, c_send, c_recv, c_local)
    c_gather.start()
    e_gather.d_in()
    e_gather.local_wait()
    e_gather.all_across()
    for copy in loads[2:]:
        copy.wait()

    def both(ref, place):
        return ref[place].reshape(2 * rows, ref.shape[3])

    def slopes(t, unused):
        place, unused_peer = chip(t)
        gh[place] = nt(both(e_all, place), shrink_w[...])
        return unused

    lax.fori_loop(0, 4, slopes, 0)
    hidden_sum[...] = jnp.zeros(hidden_sum.shape, F32)

    def to_mate(t, source, target, sends, recvs):
        place, peer = chip(t)
        return remote(source.at[place, 1 - k], target.at[t], sends.at[t], recvs.at[t], mate)

    def to_chip(t, source, target, sends, recvs):
        place, peer = chip(t)
        return remote(
            source.at[t - 1], target.at[t - 1], sends.at[3 + t], recvs.at[3 + t], peer
        )

    def add_and_send(t, parts, firsts, sums_of, lasts, sends, recvs):
        place, peer = chip(t)
        to_mate(t, parts, firsts, sends, recvs).wait_recv()
        sums_of[t - 1] = (parts[place, k].astype(F32) + firsts[t].astype(F32)).astype(BF16)
        to_chip(t, sums_of, lasts, sends, recvs).start()

    c_gather.x_in()
    c_gather.i_in()
    c_gather.local_wait()

    def feed(step, unused):
        t = lax.rem(step + 1, 4)
        place, peer = chip(t)
        c_gather.across(place, jnp.where(t == 0, 2, jnp.where(t == 3, 7, 2 * t + 1)))
        expanded = jnp.dot(both(c_all, place), expand_w[...], preferred_element_type=F32)
        expanded = expanded + expand_bias[...]
        square = expanded * expanded
        bent = jnp.tanh(0.7978845608028654 * (expanded + 0.044715 * square * expanded))
        half = 0.5 * (1.0 + bent)
        u_all[place] = (expanded * half).astype(BF16)
        slope = half + 0.5 * expanded * (1.0 - bent * bent) * (
            0.7978845608028654 * (1.0 + 3 * 0.044715 * square)
        )
        low = (slope * gh[place]).astype(BF16)
        gz_all[place] = low
        hidden_sum[...] += jnp.sum(low.astype(F32), axis=0, keepdims=True)
        back = nt(low, expand_w[...]).astype(BF16)
        part[place] = back.reshape(2, rows, width)
        to_mate(t, part, first, r_send, r_recv).start()

        @pl.when(step == 0)
        def _():
            c_gather.d_in()

        @pl.when(step > 0)
        def _():
            add_and_send(step, part, first, summed, last, r_send, r_recv)

        return unused

    lax.fori_loop(0, 4, feed, 0)

    parts, cuts = expand.shape[0], expand_terms.shape[0] * 2 // expand.shape[0]
    cut_width = expand_terms.shape[3]
    for f in range(parts):
        terms = tn(
            c_all[:, :, :, f * part_rows : (f + 1) * part_rows].reshape(8 * rows, part_rows),
            gz_all[...].reshape(8 * rows, piece),
        )
        for c in range(cuts):
            index = lax.rem(f + 2 * k, parts) * cuts + c
            expand_terms[index // 2, index % 2] = terms[
                :, c * cut_width : (c + 1) * cut_width
            ].astype(BF16)
    y_mate = {"y": 1 - y}
    y_copies = [
        remote(
            expand_terms.at[n, 1 - y], expand_came.at[n], y_send.at[n], y_recv.at[n], y_mate
        )
        for n in range(expand_terms.shape[0])
    ]
    for copy in y_copies:
        copy.start()

    def gathered_sum(parts, firsts, lasts, sends, recvs):
        place, unused_peer = chip(0)
        to_mate(0, parts, firsts, sends, recvs).wait_recv()
        total = parts[place, k].astype(F32) + firsts[0].astype(F32)
        for t in range(1, 4):
            to_chip(t, firsts, lasts, sends, recvs).wait_recv()
            total = total + lasts[t - 1].astype(F32)
        return total

    grad = gathered_sum(part, first, last, r_send, r_recv)
    plain, scale = normed(mid[...])
    grad_mid = own_grad[...].astype(F32) + norm_back(grad, gains, plain, scale)
    grad_middle[...] = grad_mid
    low = grad_mid.astype(BF16)
    low_middle[...] = low
    sums[0:1, :] = jnp.sum(low.astype(F32), axis=0, keepdims=True)
    sums[1:2, :] = jnp.sum(own_grad[...].astype(F32), axis=0, keepdims=True)
    sums[2:3, :] = jnp.sum(grad * plain, axis=0, keepdims=True)
    sums[3:4, :] = jnp.sum(grad, axis=0, keepdims=True)
    back = nt(low, out_w[...]).astype(BF16)
    for d in range(cut.shape[0]):
        low_end, high = d * span, min((d + 1) * span, width)
        if high - low_end < span:
            cut[d] = jnp.zeros(cut.shape[1:], cut.dtype)
        if low_end < high:
            cut[d, :, : high - low_end] = back[:, low_end:high]
    head_started = pieces_out(axes, sizes, cut, to_heads, h_send, h_recv)

    def shrunk(t, unused):
        place, peer = chip(t)
        terms = jnp.dot(u_all[place], shrink_w[...], preferred_element_type=F32).astype(BF16)
        part_two[place] = terms.reshape(2, rows, width)
        to_mate(t, part_two, first_two, s_send, s_recv).start()
        return unused

    lax.fori_loop(0, 4, shrunk, 0)
    for t in range(1, 4):
        add_and_send(t, part_two, first_two, summed_two, last_two, s_send, s_recv)
    to_heads[here] = cut[here]

    def keep_or_send(spot, values):
        @pl.when(y == spot % 2)
        def _():
            shrink_kept[spot // 2] = values

        @pl.when(y != spot % 2)
        def _():
            shrink_sent[spot // 2] = values

    by_columns(e_all, u_all, shrink_kept.shape[1], keep_or_send)
    values = mid[...] + gathered_sum(part_two, first_two, last_two, s_send, s_recv)
    result[...] = (values + shrink_bias[...].reshape(1, width)).T.astype(BF16)
    pieces_in(axes, sizes, cut, to_heads, h_send, h_recv, head_started)
    for n, copy in enumerate(y_copies):
        copy.wait_recv()
        half = (expand_terms[n, y].astype(F32) + expand_came[n].astype(F32)).astype(BF16)
        for step, out in enumerate(expand_half):

            @pl.when(lax.rem(lax.axis_index("o") + step, len(expand_half)) == n)
            def _(out=out, half=half):
                out[...] = half


    for copy in out_sent:
        copy.wait_send()
    for gather in (e_gather, c_gather):
        for slot in (0, 1, 2, 3, 5, 7):
            gather.copy(c_own, c_own, slot, mate).wait_send()
        for slot in (4, 6):
            half = c_own.at[pl.ds(0, rows // 2)]
            gather.copy(half, half, slot, mate).wait_send()
    for t in range(4):
        to_mate(t, part, first, r_send, r_recv).wait_send()
        to_mate(t, part_two, first_two, s_send, s_recv).wait_send()
    for t in range(1, 4):
        to_chip(t, summed, last, r_send, r_recv).wait_send()
        to_chip(t, summed_two, last_two, s_send, s_recv).wait_send()
    for copy in y_copies:
        copy.wait_send()


def middle_part(
    pieces, own, grad_turned, out_own, out_far, expand, shrink, vectors, every, ident
):
    spots, rows, span = pieces.shape
    width = own.shape[1]
    piece = expand.shape[2]
    outer = every[1][0]
    cuts = outer * 2 // expand.shape[0]
    expand_cut = (outer, 2, expand.shape[1], piece // cuts)
    everyone = jax.ShapeDtypeStruct((4, 2, rows, width), BF16)
    hidden = jax.ShapeDtypeStruct((4, 2 * rows, piece), BF16)
    flat_f32 = jax.ShapeDtypeStruct((rows, width), F32)
    flat_low = jax.ShapeDtypeStruct((rows, width), BF16)

    def scatter_buffers():
        return [
            pltpu.VMEM(everyone.shape, BF16),
            pltpu.VMEM((4, rows, width), BF16),
            pltpu.VMEM((3, rows, width), BF16),
            pltpu.VMEM((3, rows, width), BF16),
        ]

    return pl.pallas_call(
        functools.partial(middle_kernel, every),
        out_shape=[
            flat_low,
            jax.ShapeDtypeStruct((width, rows), BF16),
            flat_f32,
            flat_low,
            jax.ShapeDtypeStruct((4, width), F32),
            jax.ShapeDtypeStruct((1, piece), F32),
            jax.ShapeDtypeStruct(pieces.shape, BF16),
            jax.ShapeDtypeStruct((spots // 2, width // spots, piece), BF16),
            jax.ShapeDtypeStruct((spots // 2, width // spots, piece), BF16),
        ]
        + [jax.ShapeDtypeStruct(expand_cut[2:], BF16)] * outer,
        in_specs=[VMEM] * 3 + [ANY] * 4 + [VMEM] * 5,
        out_specs=[VMEM] * (9 + outer),
        scratch_shapes=[
            pltpu.VMEM((rows, width), BF16),
            pltpu.VMEM((1, piece), F32),
            pltpu.VMEM(pieces.shape, BF16),
            pltpu.VMEM((width, width), BF16),
            pltpu.VMEM((width, piece), BF16),
            pltpu.VMEM((piece, width), BF16),
            pltpu.VMEM((rows, width), F32),
            pltpu.VMEM((rows, width), BF16),
            pltpu.VMEM(everyone.shape, BF16),
            pltpu.VMEM(everyone.shape, BF16),
            pltpu.VMEM(hidden.shape, F32),
            pltpu.VMEM(hidden.shape, BF16),
            pltpu.VMEM(hidden.shape, BF16),
            *scatter_buffers(),
            *scatter_buffers(),
            pltpu.VMEM(pieces.shape, BF16),
            pltpu.VMEM(expand_cut, BF16),
            pltpu.VMEM(expand_cut[:1] + expand_cut[2:], BF16),
            pltpu.SemaphoreType.DMA((spots,)),
            pltpu.SemaphoreType.DMA((spots,)),
            *quad_scratch(),
            *quad_scratch(),
            pltpu.SemaphoreType.DMA((7,)),
            pltpu.SemaphoreType.DMA((2,)),
            pltpu.SemaphoreType.DMA((2,)),
            pltpu.SemaphoreType.DMA((7,)),
            pltpu.SemaphoreType.DMA((7,)),
            pltpu.SemaphoreType.DMA((7,)),
            pltpu.SemaphoreType.DMA((7,)),
            pltpu.SemaphoreType.DMA((spots,)),
            pltpu.SemaphoreType.DMA((spots,)),
            pltpu.SemaphoreType.DMA(expand_cut[:1]),
            pltpu.SemaphoreType.DMA(expand_cut[:1]),
        ],
        name="middle%d" % ident,
        compiler_params=pltpu.CompilerParams(
            collective_id=ident, has_side_effects=True, vmem_limit_bytes=67_000_000
        ),
        cost_estimate=pl.CostEstimate(
            flops=8 * rows * 8 * width * piece,
            bytes_accessed=100 * rows * width * 2,
            transcendentals=8 * rows * piece,
        ),
    )(pieces, own, grad_turned, out_own, out_far, expand, shrink, *vectors)


class Owned:
    def __init__(
        self, outer, terms, out, upright, came, half, last, whole, swapped, y_sems, o_sems, i_sems
    ):
        self.outer, self.upright, self.swapped = outer, upright, swapped
        self.terms, self.out = terms, out
        self.came, self.half, self.last, self.whole = came, half, last, whole
        self.y_sems, self.o_sems, self.i_sems = y_sems, o_sems, i_sems
        self.o, self.i, self.y = (lax.axis_index(a) for a in ("o", "i", "y"))

    def come(self, kept, came):
        self.first = []
        for n in range(2 * self.outer):
            self.half[n // 2, n % 2] = (kept[n].astype(F32) + came[n].astype(F32)).astype(BF16)

    def start(self):
        mate = {"y": 1 - self.y}
        self.first = [
            remote(
                self.terms.at[2 * n + 1 - self.y],
                self.came.at[n],
                self.y_sems.at[0, n],
                self.y_sems.at[1, n],
                mate,
            )
            for n in range(2 * self.outer)
        ]
        for copy in self.first:
            copy.start()

    def over_o(self):
        for n, copy in enumerate(self.first):
            copy.wait_recv()
            self.half[n // 2, n % 2] = (
                self.terms[2 * n + self.y].astype(F32) + self.came[n].astype(F32)
            ).astype(BF16)
        self.send_o()

    def send_o(self):
        self.second = []
        for step in range(1, self.outer):
            there = lax.rem(self.o + step, self.outer)
            copy = remote(
                self.half.at[there],
                self.last.at[step - 1],
                self.o_sems.at[0, step],
                self.o_sems.at[1, step],
                {"o": there},
            )
            copy.start()
            self.second.append(copy)

    def over_i(self):
        total = self.half[self.o].astype(F32)
        for step, copy in enumerate(self.second):
            copy.wait_recv()
            total = total + self.last[step].astype(F32)
        self.whole[...] = total.astype(BF16)
        self.third = remote(
            self.whole.at[1 - self.i],
            self.swapped.at[self.i],
            self.i_sems.at[0],
            self.i_sems.at[1],
            {"i": 1 - self.i},
        )
        self.third.start()
        self.swapped[self.i] = self.whole[self.i]

    def finish(self):
        self.third.wait_recv()
        rows = self.swapped.shape[2]
        for n in range(2):
            values = self.swapped[n].astype(F32)
            if self.upright:
                self.out[n] = values
            else:
                self.out[:, n * rows : (n + 1) * rows] = values
        for copy in self.first + self.second + [self.third]:
            copy.wait_send()


def owned_scratch(outer, cell, rows, first=True):
    return [
        pltpu.VMEM((2 * outer if first else 1, cell, rows), BF16),
        pltpu.VMEM((outer, 2, cell, rows), BF16),
        pltpu.VMEM((max(outer - 1, 1), 2, cell, rows), BF16),
        pltpu.VMEM((2, cell, rows), BF16),
        pltpu.VMEM((2, cell, rows), BF16),
        pltpu.SemaphoreType.DMA((2, 2 * outer)),
        pltpu.SemaphoreType.DMA((2, outer)),
        pltpu.SemaphoreType.DMA((2,)),
    ]


def final_kernel(
    axes,
    sizes,
    heads,
    share,
    dqkv,
    columns,
    normed_low,
    shrink_kept,
    shrink_came,
    expand_kept,
    low_middle,
    att,
    own,
    grad_middle,
    gain,
    row_sums,
    hidden_sum,
    *rest,
):
    others = sizes[0] - 1
    final_body(axes, sizes, heads, share, dqkv, columns, normed_low, shrink_kept, shrink_came,
        [expand_kept, *rest[:others]], low_middle, att, own, grad_middle, gain, row_sums,
        hidden_sum, *rest[others:])


def final_body(
    axes, sizes, heads, share, dqkv, columns, normed_low, shrink_kept_far, shrink_came_far,
    expand_far, low_middle, att, own, grad_middle_far, gain, row_sums,
    hidden_sum,
    grad_inputs,
    routed,
    shrink_out,
    outw_out,
    query_out,
    value_out,
    rows_out,
    hidden_out,
    expand_out,
    shrink_kept,
    shrink_came,
    expand_parts,
    grad_middle,
    part,
    first,
    i_came,
    o_came,
    normed_part,
    q_part,
    q_first,
    q_sum,
    q_last,
    blocks,
    gy_all,
    att_cut,
    att_all,
    outw_terms,
    line,
    line_came,
    line_out,
    r_send,
    r_recv,
    q_send,
    q_recv,
    hop,
    land,
    a_send,
    a_recv,
    l_send,
    l_recv,
    g_send,
    g_recv,
    g_local,
    load_sem,
    late_sem,
    expand_sum,
    expand_came,
    e_send,
    e_recv,
    *owned,
):
    outer, inner, ys, xs, ks = sizes
    o, i, y, x, k = (lax.axis_index(a) for a in axes)
    offs = offsets(sizes)
    chips = outer * inner
    spots = chips * ys
    place = (o * inner + i) * ys + y
    shard = x * ks + k
    me = place * xs * ks + shard
    rows, width = own.shape
    span = heads * HEAD_DIM
    y_mate, k_mate, x_mate = {"y": 1 - y}, {"k": 1 - k}, {"x": 1 - x}
    shrink = Owned(outer, None, shrink_out, False, *owned[:8])
    outw = Owned(outer, outw_terms, outw_out, True, *owned[8:])

    def load_normed(n):
        some = normed_part.shape[0]
        return pltpu.make_async_copy(
            normed_low.at[pl.ds(n * some, some)], normed_part, load_sem
        )

    load_normed(0).start()
    late = [
        pltpu.make_async_copy(source, target, late_sem.at[n])
        for n, (source, target) in enumerate(
            [
                (shrink_kept_far, shrink_kept),
                (shrink_came_far, shrink_came),
                (grad_middle_far, grad_middle),
            ]
            + [(far, expand_parts.at[n]) for n, far in enumerate(expand_far)]
        )
    ]
    for copy in late:
        copy.start()
    greet([moved(axes, sizes, off) for off in offs])

    def spot_of(n):
        to = lax.rem(o + n % outer + 1, outer)
        ti = lax.rem(i + 1 + n // outer, inner)
        return to * inner + ti, to

    def to_mate(n):
        return remote(
            part.at[spot_of(n)[0], 1 - y], first.at[n], r_send.at[n], r_recv.at[n], y_mate
        )

    def to_i(s):
        slot = 2 * outer + s
        return remote(
            part.at[spot_of(s)[0], y], i_came.at[s], r_send.at[slot], r_recv.at[slot], {"i": 1 - i}
        )

    def to_o(s):
        slot = 3 * outer + s
        spot, to = spot_of(outer + s)
        return remote(part.at[spot, y], o_came.at[s], r_send.at[slot], r_recv.at[slot], {"o": to})

    def terms(n, unused):
        spot = spot_of(n)[0]
        at = pl.multiple_of(spot * 2 * rows, 2 * rows)
        values = nt(dqkv[pl.ds(at, 2 * rows), :], columns[...]).astype(BF16)
        part[spot] = values.reshape(2, rows, width)
        to_mate(n).start()
        return unused

    lax.fori_loop(0, chips, terms, 0)

    late[0].wait()
    late[1].wait()
    shrink.come(shrink_kept, shrink_came)
    shrink.send_o()

    group = (("i", "x", "k"), (inner, xs, ks))
    side = Quad(low_middle, gy_all, g_send, g_recv, g_local)
    side.start()
    cell = att_cut.shape[2]
    for half in range(inner):
        for f in range(xs * ks):
            low = (f * inner + half) * cell
            att_cut[half * xs * ks + f] = att[:, low : low + cell]
    att_started = pieces_out(*group, att_cut, att_all, a_send, a_recv)
    here = (i * xs + x) * ks + k
    att_all[here] = att_cut[here]

    quarter = q_part.shape[3]
    some = normed_part.shape[0]
    pieces = dqkv.shape[0] // some
    for section in range(3):
        low = section * span
        values = 0.0
        for n in range(pieces):
            if n or section == 0 or pieces > 1:
                copy = load_normed(n)
                if n or section:
                    copy.start()
                copy.wait()
            values = values + tn(
                dqkv[n * some : (n + 1) * some, low : low + span], normed_part[...]
            )
        for f in range(xs * ks):
            q_part[f // ks, f % ks, low : low + span, :] = values[
                :, f * quarter : (f + 1) * quarter
            ].astype(BF16)
    q_copies = [
        remote(q_part.at[1 - x, 1 - k], q_first.at[1], q_send.at[1], q_recv.at[1], k_mate),
        remote(q_part.at[x, 1 - k], q_first.at[0], q_send.at[0], q_recv.at[0], k_mate),
    ]
    for copy in q_copies:
        copy.start()

    for s in range(outer):
        to_mate(s).wait_recv()
        spot = spot_of(s)[0]
        part[spot, y] = (part[spot, y].astype(F32) + first[s].astype(F32)).astype(BF16)
        to_i(s).start()
    side.x_in()
    side.i_in()
    q_copies[0].wait_recv()
    q_sum[...] = (q_part[1 - x, k].astype(F32) + q_first[1].astype(F32)).astype(BF16)
    q_over = remote(q_sum, q_last, q_send.at[2], q_recv.at[2], x_mate)
    q_over.start()

    def inner_sum(s):
        to_mate(outer + s).wait_recv()
        to_i(s).wait_recv()
        spot = spot_of(outer + s)[0]
        return spot, (
            part[spot, y].astype(F32) + first[outer + s].astype(F32) + i_came[s].astype(F32)
        )

    for s in range(outer - 1):
        spot, total = inner_sum(s)
        part[spot, y] = total.astype(BF16)
        to_o(s).start()
    side.d_in()

    for copy in late[2:]:
        copy.wait()
    shards = xs * ks
    cuts = spots // (2 * shards)
    total = expand_parts[0].astype(F32)
    for n in range(1, outer):
        total = total + expand_parts[n].astype(F32)
    expand_sum[...] = total.astype(BF16)
    index = o * ys + y
    goal = shard * (spots // shards) + i * cuts + index % cuts
    goal_shard = lax.rem(index // cuts + 2 * k, shards)
    away = goal * shards + goal_shard != me
    route = remote(
        expand_sum,
        expand_came,
        e_send,
        e_recv,
        {
            "o": goal // (inner * ys),
            "i": (goal // ys) % inner,
            "y": goal % ys,
            "x": goal_shard // ks,
            "k": goal_shard % ks,
        },
    )

    @pl.when(away)
    def _():
        route.start()

    @pl.when(jnp.logical_not(away))
    def _():
        expand_came[...] = expand_sum[...]

    pieces_in(*group, att_cut, att_all, a_send, a_recv, att_started)
    side.local_wait()
    side.all_across()

    def put_terms(spot, values):
        outw_terms[spot] = values

    by_columns(gy_all, att_all, outw_terms.shape[1], put_terms)
    outw.start()

    q_copies[1].wait_recv()
    q_over.wait_recv()
    total = q_part[x, k].astype(F32) + q_first[0].astype(F32) + q_last[...].astype(F32)
    blocks[...] = total.astype(BF16).reshape(blocks.shape)

    def where(spot):
        return {
            "o": spot // (inner * ys),
            "i": (spot // ys) % inner,
            "y": spot % ys,
        }

    def each_sent(act):
        for section in range(3):
            for h in range(heads):
                head = place * heads + h
                block = section * HEADS + head
                low = (block * HEAD_DIM) // share
                high = (block * HEAD_DIM + HEAD_DIM - 1) // share
                index = section * heads + h
                for which, owner, needed in (
                    (0, low, head < HEADS),
                    (1, high, (head < HEADS) & (high != low)),
                ):

                    @pl.when(needed)
                    def _(which=which, owner=owner, block=block, index=index):
                        act(index, 2 * index + which, owner, block - (share * owner) // HEAD_DIM)

    def block_copy(index, slot, owner, target):
        return remote(
            blocks.at[index], routed.at[target], hop.at[slot], land.at[target], where(owner)
        )

    def send_block(index, slot, owner, target):
        @pl.when(owner != place)
        def _():
            block_copy(index, slot, owner, target).start()

        @pl.when(owner == place)
        def _():
            routed[target] = blocks[index]

    def sent_block(index, slot, owner, target):
        @pl.when(owner != place)
        def _():
            block_copy(index, slot, owner, target).wait_send()

    each_sent(send_block)

    spot, grad = inner_sum(outer - 1)
    for s in range(outer - 1):
        to_o(s).wait_recv()
        grad = grad + o_came[s].astype(F32)
    plain, scale = normed(own[...].astype(F32))
    gains = gain[...].reshape(1, width)
    grad_inputs[...] = (grad_middle[...] + norm_back(grad, gains, plain, scale)).T

    def fill(base, values):
        size = values.shape[1]
        for n in range(-(-size // 128)):
            low, high = n * 128, min(n * 128 + 128, size)
            line[pl.ds(base + n, 1), 0 : high - low] = values[:, low:high]

    q_rows, w_rows = -(-span // 128), -(-width // 128)
    piece = hidden_sum.shape[1]
    p_rows = -(-piece // 128)
    value_base = spots * q_rows
    rows_base = 2 * spots * q_rows
    hidden_base = rows_base + 6 * w_rows
    line[...] = jnp.zeros(line.shape, F32)
    fill(place * q_rows, jnp.sum(dqkv[:, 0:span].astype(F32), axis=0, keepdims=True))
    fill(
        value_base + place * q_rows,
        jnp.sum(dqkv[:, 2 * span : 3 * span].astype(F32), axis=0, keepdims=True),
    )
    for n in range(4):
        fill(rows_base + n * w_rows, row_sums[n : n + 1, :])
    fill(rows_base + 4 * w_rows, jnp.sum(grad * plain, axis=0, keepdims=True))
    fill(rows_base + 5 * w_rows, jnp.sum(grad, axis=0, keepdims=True))
    fill(hidden_base + (shard * inner + i) * p_rows, hidden_sum[...])
    line_rows = line_came.shape[1]

    def share_of(ref, device):
        return ref.at[pl.ds(pl.multiple_of(device * line_rows, line_rows), line_rows)]

    line_started = []
    for t, off in enumerate(offs):
        peer = moved(axes, sizes, off)
        device = flat(peer, axes, sizes)
        copy = remote(
            share_of(line, device), line_came.at[t], l_send.at[t], l_recv.at[t], peer
        )
        copy.start()
        line_started.append(copy)
    shrink.over_i()
    outw.over_o()
    for copy in line_started:
        copy.wait_recv()
    mine = pl.ds(pl.multiple_of(me * line_rows, line_rows), line_rows)
    line_out[mine, :] = line[mine, :] + jnp.sum(line_came[...], axis=0)
    count = len(offs)
    for t, off in enumerate(offs):
        peer = moved(axes, sizes, off)
        copy = remote(
            share_of(line_out, me),
            share_of(line_out, me),
            l_send.at[count + t],
            l_recv.at[count + t],
            peer,
        )
        copy.start()
        line_started.append(copy)
    outw.over_i()

    base = (share * place) // HEAD_DIM
    for slot in range(routed.shape[0]):
        block = base + slot
        owner = (block % HEADS) // heads

        @pl.when((block * HEAD_DIM < share * (place + 1)) & (owner != place))
        def _(slot=slot):
            remote(
                blocks.at[0], routed.at[slot], hop.at[0], land.at[slot], where(place)
            ).wait_recv()

    for t, off in enumerate(offs):
        peer = moved(axes, sizes, off, -1)
        block = share_of(line_out, flat(peer, axes, sizes))
        remote(block, block, l_send.at[count + t], l_recv.at[count + t], peer).wait_recv()

    def take(base, ref, row, start, size):
        for n in range(-(-size // 128)):
            low, high = n * 128, min(n * 128 + 128, size)
            ref[row : row + 1, start + low : start + high] = line_out[
                base + n : base + n + 1, 0 : high - low
            ]

    for c in range(spots):
        take(c * q_rows, query_out, 0, c * span, span)
        take(value_base + c * q_rows, value_out, 0, c * span, span)
    for n in range(6):
        take(rows_base + n * w_rows, rows_out, n, 0, width)
    for n in range(xs * ks * inner):
        take(hidden_base + n * p_rows, hidden_out, 0, n * piece, piece)

    @pl.when(away)
    def _():
        route.wait()

    expand_out[...] = expand_came[...].astype(F32)
    shrink.finish()
    outw.finish()
    each_sent(sent_block)
    for copy in line_started + q_copies + [q_over]:
        copy.wait_send()
    side.finish()
    for n in range(chips):
        to_mate(n).wait_send()
    for s in range(outer):
        to_i(s).wait_send()
    for s in range(outer - 1):
        to_o(s).wait_send()


def final_part(
    dqkv,
    columns,
    normed_low,
    shrink_kept,
    shrink_came,
    expand_parts,
    low_middle,
    att,
    own,
    grad_middle,
    gain,
    row_sums,
    hidden_sum,
    axes,
    sizes,
    heads,
    share,
    ident,
):
    outer, inner, ys, xs, ks = sizes
    spots = outer * inner * ys
    cell, piece = shrink_kept.shape[1:]
    rows, width = own.shape
    chips = outer * inner
    devices = spots * xs * ks
    group = inner * xs * ks
    span = heads * HEAD_DIM
    part_rows = width // (xs * ks)
    slots = max(
        (share * (c + 1) - 1) // HEAD_DIM - (share * c) // HEAD_DIM + 1 for c in range(spots)
    )
    line_rows = (
        2 * spots * -(-span // 128) + 6 * -(-width // 128) + xs * ks * inner * -(-piece // 128)
    )
    line_rows = 8 * -(-line_rows // (8 * devices))
    block = (rows, width)
    q_block = (3 * span, part_rows)
    out_rows = width // group
    return pl.pallas_call(
        functools.partial(final_kernel, axes, sizes, heads, share),
        out_shape=[
            jax.ShapeDtypeStruct(block[::-1], F32),
            jax.ShapeDtypeStruct((slots, HEAD_DIM, part_rows), BF16),
            jax.ShapeDtypeStruct((cell, inner * piece), F32),
            jax.ShapeDtypeStruct((inner, cell, out_rows), F32),
            jax.ShapeDtypeStruct((1, spots * span), F32),
            jax.ShapeDtypeStruct((1, spots * span), F32),
            jax.ShapeDtypeStruct((6, width), F32),
            jax.ShapeDtypeStruct((1, group * piece), F32),
            jax.ShapeDtypeStruct(expand_parts[0].shape, F32),
        ],
        in_specs=[VMEM] * 2 + [ANY] * 4 + [VMEM] * 3 + [ANY] + [VMEM] * 3 + [ANY] * (outer - 1),
        out_specs=[VMEM] * 9,
        scratch_shapes=[
            pltpu.VMEM(shrink_kept.shape, BF16),
            pltpu.VMEM(shrink_kept.shape, BF16),
            pltpu.VMEM((outer,) + expand_parts[0].shape, BF16),
            pltpu.VMEM(block, F32),
            pltpu.VMEM((chips, ys) + block, BF16),
            pltpu.VMEM((chips,) + block, BF16),
            pltpu.VMEM((outer,) + block, BF16),
            pltpu.VMEM((max(outer - 1, 1),) + block, BF16),
            pltpu.VMEM((min(1024, dqkv.shape[0]), width), BF16),
            pltpu.VMEM((xs, ks) + q_block, BF16),
            pltpu.VMEM((2,) + q_block, BF16),
            pltpu.VMEM(q_block, BF16),
            pltpu.VMEM(q_block, BF16),
            pltpu.VMEM((3 * heads, HEAD_DIM, part_rows), BF16),
            pltpu.VMEM((inner * xs, ks) + block, BF16),
            pltpu.VMEM((group, rows, out_rows), BF16),
            pltpu.VMEM((group, rows, out_rows), BF16),
            pltpu.VMEM((spots, cell, out_rows), BF16),
            pltpu.VMEM((devices * line_rows, 128), F32),
            pltpu.VMEM((devices - 1, line_rows, 128), F32),
            pltpu.VMEM((devices * line_rows, 128), F32),
            pltpu.SemaphoreType.DMA((4 * outer,)),
            pltpu.SemaphoreType.DMA((4 * outer,)),
            pltpu.SemaphoreType.DMA((3,)),
            pltpu.SemaphoreType.DMA((3,)),
            pltpu.SemaphoreType.DMA((6 * heads,)),
            pltpu.SemaphoreType.DMA((slots,)),
            pltpu.SemaphoreType.DMA((group,)),
            pltpu.SemaphoreType.DMA((group,)),
            pltpu.SemaphoreType.DMA((2 * devices,)),
            pltpu.SemaphoreType.DMA((2 * devices,)),
            *quad_scratch(),
            pltpu.SemaphoreType.DMA,
            pltpu.SemaphoreType.DMA((3 + outer,)),
            pltpu.VMEM(expand_parts[0].shape, BF16),
            pltpu.VMEM(expand_parts[0].shape, BF16),
            pltpu.SemaphoreType.DMA,
            pltpu.SemaphoreType.DMA,
            *owned_scratch(outer, cell, piece, False),
            *owned_scratch(outer, cell, out_rows),
        ],
        name="final%d" % ident,
        compiler_params=pltpu.CompilerParams(
            collective_id=ident, has_side_effects=True, vmem_limit_bytes=67_000_000
        ),
        cost_estimate=pl.CostEstimate(
            flops=12 * rows * spots * width * span,
            bytes_accessed=100 * rows * width * 2,
            transcendentals=0,
        ),
    )(
        dqkv,
        columns,
        normed_low,
        shrink_kept,
        shrink_came,
        expand_parts[0],
        low_middle,
        att,
        own,
        grad_middle,
        gain,
        row_sums,
        hidden_sum,
        *expand_parts[1:],
    )


def nt(left, right):
    return lax.dot_general(left, right, (((1,), (1,)), ((), ())), preferred_element_type=F32)


def nn(left, right):
    return lax.dot_general(left, right, (((1,), (0,)), ((), ())), preferred_element_type=F32)


def tn(left, right):
    return lax.dot_general(left, right, (((0,), (0,)), ((), ())), preferred_element_type=F32)


def rows_of(inv, ref, pair, low, high):
    first = pl.multiple_of(inv[2 * pair] * HEAD_DIM, HEAD_DIM)
    second = pl.multiple_of(inv[2 * pair + 1] * HEAD_DIM, HEAD_DIM)
    return jnp.concatenate(
        [ref[pl.ds(first, 64), low:high], ref[pl.ds(second, 64), low:high]], axis=0
    )


def put_rows(inv, ref, pair, low, high, values):
    first = pl.multiple_of(inv[2 * pair] * HEAD_DIM, HEAD_DIM)
    second = pl.multiple_of(inv[2 * pair + 1] * HEAD_DIM, HEAD_DIM)
    ref[pl.ds(first, 64), low:high] = values[:64]
    ref[pl.ds(second, 64), low:high] = values[64:]


def head_slice(values, part, heads, head):
    low = (part * heads + head) * HEAD_DIM
    return values[:, low : low + HEAD_DIM]


def diagonal(block):
    return lax.broadcasted_iota(jnp.int32, (block, block), 0) <= lax.broadcasted_iota(
        jnp.int32, (block, block), 1
    )


def attend_kernel(heads, block, inv, qkv, out, out_low, lse, qs, ks, vt, ot):
    length = qkv.shape[0]
    width = heads * HEAD_DIM

    def sort(pair, unused):
        at = pl.multiple_of(pair * 128, 128)
        values = rows_of(inv, qkv, pair, 0, 3 * width)
        for h in range(heads):
            qs[h, pl.ds(at, 128), :] = head_slice(values, 0, heads, h) * BF16(0.125)
            ks[h, pl.ds(at, 128), :] = head_slice(values, 1, heads, h)
            vt[h, :, pl.ds(at, 128)] = head_slice(values, 2, heads, h).astype(F32).T.astype(BF16)
        return unused

    lax.fori_loop(0, length // 128, sort, 0)
    allowed = diagonal(block)

    def row(qi, unused):
        q_at = pl.multiple_of(qi * block, block)

        def first(h):
            scores = nt(ks[h, pl.ds(q_at, block), :], qs[h, pl.ds(q_at, block), :])
            scores = jnp.where(allowed, scores, -1e30)
            high = jnp.max(scores, axis=0, keepdims=True)
            probs = jnp.exp(scores - high)
            return (
                high,
                jnp.sum(probs, axis=0, keepdims=True),
                nn(vt[h, :, pl.ds(q_at, block)], probs.astype(BF16)),
            )

        def column(kj, state):
            k_at = pl.multiple_of(kj * block, block)
            fresh_state = []
            for h in range(heads):
                high, weight, acc = state[h]
                scores = nt(ks[h, pl.ds(k_at, block), :], qs[h, pl.ds(q_at, block), :])
                fresh = jnp.maximum(high, jnp.max(scores, axis=0, keepdims=True))
                probs = jnp.exp(scores - fresh)
                fade = jnp.exp(high - fresh)
                fresh_state.append(
                    (
                        fresh,
                        weight * fade + jnp.sum(probs, axis=0, keepdims=True),
                        acc * fade + nn(vt[h, :, pl.ds(k_at, block)], probs.astype(BF16)),
                    )
                )
            return tuple(fresh_state)

        state = lax.fori_loop(0, qi, column, tuple(first(h) for h in range(heads)))
        for h in range(heads):
            high, weight, acc = state[h]
            ot[h, :, pl.ds(q_at, block)] = acc / weight
            lse[h : h + 1, pl.ds(q_at, block)] = high + jnp.log(weight)
        return unused

    lax.fori_loop(0, length // block, row, 0)

    def unsort(pair, unused):
        at = pl.multiple_of(pair * 128, 128)
        values = [ot[h, :, pl.ds(at, 128)].T for h in range(heads)]
        values = jnp.concatenate(values, axis=1)
        put_rows(inv, out, pair, 0, width, values)
        put_rows(inv, out_low, pair, 0, width, values.astype(BF16))
        return unused

    lax.fori_loop(0, length // 128, unsort, 0)


def attend(inv, qkv, heads):
    length = qkv.shape[0]
    width = heads * HEAD_DIM
    block = min(256, length)
    pairs = length * (length + block) // 2
    return pl.pallas_call(
        functools.partial(attend_kernel, heads, block),
        out_shape=(
            jax.ShapeDtypeStruct((length, width), F32),
            jax.ShapeDtypeStruct((length, width), BF16),
            jax.ShapeDtypeStruct((heads, length), F32),
        ),
        grid_spec=pltpu.PrefetchScalarGridSpec(
            num_scalar_prefetch=1,
            grid=(1,),
            in_specs=[pl.BlockSpec((length, 3 * width), lambda i, inv: (0, 0))],
            out_specs=(
                pl.BlockSpec((length, width), lambda i, inv: (0, 0)),
                pl.BlockSpec((length, width), lambda i, inv: (0, 0)),
                pl.BlockSpec((heads, length), lambda i, inv: (0, 0)),
            ),
            scratch_shapes=[
                pltpu.VMEM((heads, length, HEAD_DIM), BF16),
                pltpu.VMEM((heads, length, HEAD_DIM), BF16),
                pltpu.VMEM((heads, HEAD_DIM, length), BF16),
                pltpu.VMEM((heads, HEAD_DIM, length), F32),
            ],
        ),
        name="attend",
        cost_estimate=pl.CostEstimate(
            flops=4 * heads * pairs * HEAD_DIM * 4,
            bytes_accessed=length * width * 10,
            transcendentals=heads * pairs,
        ),
    )(inv, qkv)


def attend_back_kernel(
    heads, block, inv, qkv, grads, outs, lse, dqkv, qs, ks, vs, gs, kt, delta, dqt, dks, dvs
):
    length = qkv.shape[0]
    width = heads * HEAD_DIM
    count = length // block

    def sort(pair, unused):
        at = pl.multiple_of(pair * 128, 128)
        values = rows_of(inv, qkv, pair, 0, 3 * width)
        grad = rows_of(inv, grads, pair, 0, width)
        value = rows_of(inv, outs, pair, 0, width)
        product = (grad.astype(F32) * value).T
        for h in range(heads):
            qs[h, pl.ds(at, 128), :] = head_slice(values, 0, heads, h) * BF16(0.125)
            key = head_slice(values, 1, heads, h)
            ks[h, pl.ds(at, 128), :] = key
            kt[h, :, pl.ds(at, 128)] = key.astype(F32).T.astype(BF16)
            vs[h, pl.ds(at, 128), :] = head_slice(values, 2, heads, h)
            gs[h, pl.ds(at, 128), :] = head_slice(grad, 0, heads, h)
            delta[h : h + 1, pl.ds(at, 128)] = jnp.sum(
                product[h * HEAD_DIM : (h + 1) * HEAD_DIM], axis=0, keepdims=True
            )
            dqt[h, :, pl.ds(at, 128)] = jnp.zeros((HEAD_DIM, 128), F32)
        return unused

    lax.fori_loop(0, length // 128, sort, 0)
    allowed = diagonal(block)

    def column(kj, unused):
        k_at = pl.multiple_of(kj * block, block)

        def tile(h, q_at, masked):
            q = qs[h, pl.ds(q_at, block), :]
            g = gs[h, pl.ds(q_at, block), :]
            scores = nt(ks[h, pl.ds(k_at, block), :], q)
            probs = jnp.exp(scores - lse[h : h + 1, pl.ds(q_at, block)])
            if masked:
                probs = jnp.where(allowed, probs, 0.0)
            slopes = nt(vs[h, pl.ds(k_at, block), :], g)
            low = (probs * (slopes - delta[h : h + 1, pl.ds(q_at, block)])).astype(BF16)
            dqt[h, :, pl.ds(q_at, block)] += nn(kt[h, :, pl.ds(k_at, block)], low)
            return nn(low, q), nn(probs.astype(BF16), g)

        def row(qi, state):
            q_at = pl.multiple_of(qi * block, block)
            fresh = []
            for h in range(heads):
                dk, dv = tile(h, q_at, False)
                fresh.append((state[h][0] + dk, state[h][1] + dv))
            return tuple(fresh)

        state = tuple(tile(h, k_at, True) for h in range(heads))
        state = lax.fori_loop(kj + 1, count, row, state)
        for h in range(heads):
            dks[h, pl.ds(k_at, block), :] = state[h][0].astype(BF16)
            dvs[h, pl.ds(k_at, block), :] = state[h][1].astype(BF16)
        return unused

    lax.fori_loop(0, count, column, 0)

    def unsort(pair, unused):
        at = pl.multiple_of(pair * 128, 128)
        values = [(dqt[h, :, pl.ds(at, 128)].T * 0.125).astype(BF16) for h in range(heads)]
        values += [dks[h, pl.ds(at, 128), :] for h in range(heads)]
        values += [dvs[h, pl.ds(at, 128), :] for h in range(heads)]
        put_rows(inv, dqkv, pair, 0, 3 * width, jnp.concatenate(values, axis=1))
        return unused

    lax.fori_loop(0, length // 128, unsort, 0)


def attend_back(inv, qkv, grads, outs, lse, heads):
    length = qkv.shape[0]
    width = heads * HEAD_DIM
    block = min(256, length)
    pairs = length * (length + block) // 2
    row_shape = (heads, length, HEAD_DIM)
    return pl.pallas_call(
        functools.partial(attend_back_kernel, heads, block),
        out_shape=jax.ShapeDtypeStruct((length, 3 * width), BF16),
        grid_spec=pltpu.PrefetchScalarGridSpec(
            num_scalar_prefetch=1,
            grid=(1,),
            in_specs=[
                pl.BlockSpec((length, 3 * width), lambda i, inv: (0, 0)),
                pl.BlockSpec((length, width), lambda i, inv: (0, 0)),
                pl.BlockSpec((length, width), lambda i, inv: (0, 0)),
                pl.BlockSpec((heads, length), lambda i, inv: (0, 0)),
            ],
            out_specs=pl.BlockSpec((length, 3 * width), lambda i, inv: (0, 0)),
            scratch_shapes=[
                pltpu.VMEM(row_shape, BF16),
                pltpu.VMEM(row_shape, BF16),
                pltpu.VMEM(row_shape, BF16),
                pltpu.VMEM(row_shape, BF16),
                pltpu.VMEM((heads, HEAD_DIM, length), BF16),
                pltpu.VMEM((heads, length), F32),
                pltpu.VMEM((heads, HEAD_DIM, length), F32),
                pltpu.VMEM(row_shape, BF16),
                pltpu.VMEM(row_shape, BF16),
            ],
        ),
        name="attend_back",
        cost_estimate=pl.CostEstimate(
            flops=10 * heads * pairs * HEAD_DIM * 4,
            bytes_accessed=length * width * 20,
            transcendentals=heads * pairs,
        ),
    )(inv, qkv, grads, outs, lse)


def body(
    sizes,
    tokens,
    block_order,
    qkv_weight,
    query_bias,
    value_bias,
    out_weight,
    out_bias,
    expand_weight,
    expand_bias,
    shrink_weight,
    shrink_bias,
    first_gain,
    first_shift,
    second_gain,
    second_shift,
    cotangent,
):
    outer, inner, ys, xs, ks = (sizes[a] for a in ("o", "i", "y", "x", "k"))
    spots = outer * inner * ys
    shards = xs * ks
    rows, width = tokens.shape[1:]
    o, i, y = lax.axis_index("o"), lax.axis_index("i"), lax.axis_index("y")
    shard = lax.axis_index("x") * ks + lax.axis_index("k")
    place = (o * inner + i) * ys + y
    heads = -(-HEADS // spots)
    span = heads * HEAD_DIM
    padded = spots * span
    part = qkv_weight.shape[0]
    hidden = expand_weight.shape[1]
    piece = hidden // (shards * inner)
    every = (("o", "i", "y"), (outer, inner, ys))
    group = (("i", "x"), (inner, xs), "k")

    sizes_of = (outer, inner, ys, xs, ks)
    qkv, normed_low, qkv_columns, expand_columns, own = first_part(
        tokens[0].T,
        qkv_weight,
        expand_weight,
        [first_gain, first_shift, query_bias, value_bias],
        span,
        sizes_of,
        piece,
        0,
    )
    qkv_columns = qkv_columns.reshape(width, 3 * span)

    qkv, out_own = lax.optimization_barrier((qkv, out_weight))
    out_far = lax.ppermute(out_own, "x", [(0, 1), (1, 0)])

    order_row = block_order[0]
    blocks = order_row.shape[0]
    inv = jnp.sum(
        jnp.where(
            order_row[:, None] == jnp.arange(blocks, dtype=jnp.int32)[None, :],
            jnp.arange(blocks, dtype=jnp.int32)[:, None],
            0,
        ),
        axis=0,
    ).astype(jnp.int32)
    attended, attended_bf, log_sum = attend(inv, qkv, heads)
    (
        attended_low,
        result,
        grad_middle,
        middle_low,
        row_sums,
        hidden_sums,
        grad_heads,
        shrink_kept,
        shrink_sent,
        *expand_parts,
    ) = middle_part(
        attended_bf.reshape(spots, rows, span),
        own,
        cotangent[0].T,
        out_own,
        out_far,
        expand_columns,
        shrink_weight,
        [out_bias, expand_bias, shrink_bias, second_gain, second_shift],
        every,
        1,
    )
    grad_heads = grad_heads.reshape(spots * rows, span)
    dqkv = attend_back(inv, qkv, grad_heads, attended, log_sum, heads)
    shrink_came = lax.ppermute(shrink_sent, "y", [(0, 1), (1, 0)])
    for step in range(1, outer):
        ring = [(d, (d + step) % outer) for d in range(outer)]
        expand_parts[step] = lax.ppermute(expand_parts[step], "o", ring)
    axes = ("o", "i", "y", "x", "k")
    share = 3 * width // spots
    (
        grad_inputs,
        routed,
        shrink_cells,
        outw_cells,
        query_sums,
        value_sums,
        row_totals,
        hidden_totals,
        grad_expand,
    ) = final_part(
        dqkv,
        qkv_columns,
        normed_low,
        shrink_kept,
        shrink_came,
        expand_parts,
        middle_low,
        attended_low,
        own,
        grad_middle,
        first_gain,
        row_sums,
        hidden_sums,
        axes,
        sizes_of,
        heads,
        share,
        2,
    )

    start = share * place - HEAD_DIM * ((share * place) // HEAD_DIM)
    grad_qkv = lax.dynamic_slice_in_dim(routed.reshape(-1, part), start, share, axis=0)
    return (
        result.T[None],
        grad_inputs.T[None],
        grad_qkv.T.astype(F32),
        outw_cells.transpose(0, 2, 1).reshape(part, -1),
        grad_expand,
        shrink_cells.T,
        query_sums[0, :width],
        value_sums[0, :width],
        row_totals[0],
        hidden_totals[0],
        row_totals[1],
        row_totals[4],
        row_totals[5],
        row_totals[2],
        row_totals[3],
    )


def solution(mesh):
    spots, shards = mesh.shape["ctx"], mesh.shape["fsdp"]
    sizes = {"o": spots // 4, "i": 2, "y": 2, "x": shards // 2, "k": 2}
    fine = Mesh(mesh.devices.reshape(tuple(sizes.values())), tuple(sizes))
    seq, pos = ("x", "k"), ("o", "i", "y")
    weight = P(seq, None)
    placed = (
        P(seq, pos, None),
        P(seq, None),
        weight,
        P(),
        P(),
        weight,
        P(),
        weight,
        P(),
        weight,
        P(),
        P(),
        P(),
        P(),
        P(),
        P(seq, pos, None),
    )
    given = (P(seq, pos, None),) * 2 + (P(seq, pos),) * 4 + (P(),) * 9
    return jax.shard_map(
        functools.partial(body, sizes),
        mesh=fine,
        in_specs=placed,
        out_specs=given,
        check_vma=False,
    )
```
